32 devices in a mesh: gx: 4 (over x, core), gy: 4 (over z), zt: 2 (over y).
Axes of the slice: x: 2, y: 2, z: 4, core: 2. Of those that a mesh axis runs over, the one named last changes fastest.
Arguments:
- gauge_links: float32 [4, 2, 3, 3, 8, 32, 256], P(None, None, None, None, 'gx', 'gy', 'zt'), may hold values from -1 to 1, as said below
- momenta: float32 [4, 2, 3, 3, 8, 32, 256], P(None, None, None, None, 'gx', 'gy', 'zt'), may hold values from -4 to 4, as said below
Outputs:
- new_links: float32 [4, 2, 3, 3, 8, 32, 256], P(None, None, None, None, 'gx', 'gy', 'zt')
- new_momenta: float32 [4, 2, 3, 3, 8, 32, 256], P(None, None, None, None, 'gx', 'gy', 'zt')
- plaquette: float32 [], replicated
The draws below stay inside these ranges and needn't reach their ends.
Inputs may be any that keep to these rules, and one draw needn't show every extreme that they name: `gauge_links`: every link is a unitary 3 x 3 complex matrix. `momenta`: every momentum is an antihermitian traceless 3 x 3 complex matrix.
All inputs are finite; a program needn't handle non-finite values.
Results may differ from the reference program's by a relative error of at most 0.0001.
Values sent between devices are 32-bit elements; how exact they have to be, the bound alone decides.
A program may use at most 128 MiB of HBM per device.

```python
import jax
import jax.numpy as jnp

LT = 64
NX = 8
NY = 32
NZ = 4


def times_pair(first, second):
    return (first[0] * second[0] - first[1] * second[1], first[0] * second[1] + first[1] * second[0])


def unitary_from(real_gen, imag_gen):
    identity = jnp.eye(3, dtype=jnp.float32)[:, :, None, None, None, None]
    top_real = identity + 0.5 * real_gen
    top_imag = 0.5 * imag_gen
    low_real = identity - 0.5 * real_gen
    low_imag = -0.5 * imag_gen

    def element(row_index, column):
        return (low_real[row_index % 3, column % 3], low_imag[row_index % 3, column % 3])
    cofactor = []
    for row_index in range(3):
        line = []
        for column in range(3):
            first = times_pair(element(column + 1, row_index + 1), element(column + 2, row_index + 2))
            second = times_pair(element(column + 1, row_index + 2), element(column + 2, row_index + 1))
            line.append((first[0] - second[0], first[1] - second[1]))
        cofactor.append(line)
    determinant = times_pair(element(0, 0), cofactor[0][0])
    for middle in (1, 2):
        extra = times_pair(element(0, middle), cofactor[middle][0])
        determinant = (determinant[0] + extra[0], determinant[1] + extra[1])
    norm_square = determinant[0] * determinant[0] + determinant[1] * determinant[1]
    inverse_det = (determinant[0] / norm_square, -determinant[1] / norm_square)
    real_rows = []
    imag_rows = []
    for row_index in range(3):
        real_line = []
        imag_line = []
        for column in range(3):
            total_real = 0.0
            total_imag = 0.0
            for inner in range(3):
                entry = times_pair(cofactor[inner][column], inverse_det)
                value = times_pair((top_real[row_index, inner], top_imag[row_index, inner]), entry)
                total_real = total_real + value[0]
                total_imag = total_imag + value[1]
            real_line.append(total_real)
            imag_line.append(total_imag)
        real_rows.append(jnp.stack(real_line))
        imag_rows.append(jnp.stack(imag_line))
    return (jnp.stack(real_rows), jnp.stack(imag_rows))


def draw_gauge_links(key, part):
    key_x = jax.random.fold_in(key, 11)
    key_z = jax.random.fold_in(key, 12)
    key_noise = jax.random.fold_in(key, 13)
    order_x = jax.random.uniform(key_x, (NX,), jnp.float32)
    order_z = jax.random.uniform(key_z, (NZ,), jnp.float32)
    strength = 0.4 + 3.0 * order_x[:, None, None, None] * order_z[None, None, :, None]
    strength = jnp.broadcast_to(strength, (NX, NY, NZ, LT)).reshape(NX, NY, NZ * LT)
    shape = (2, 3, 3, 4, NX, NY, NZ * LT)
    noise = jax.random.normal(key_noise, shape, jnp.float32)
    identity = jnp.eye(3, dtype=jnp.float32)[:, :, None, None, None, None]
    real_gen = 0.5 * (noise[0] - jnp.swapaxes(noise[0], 0, 1)) * strength
    imag_sym = 0.5 * (noise[1] + jnp.swapaxes(noise[1], 0, 1))
    trace_imag = (imag_sym[0, 0] + imag_sym[1, 1] + imag_sym[2, 2]) / 3.0
    imag_gen = (imag_sym - trace_imag * identity) * strength
    real_link, imag_link = unitary_from(real_gen, imag_gen)
    result = jnp.stack([real_link, imag_link])
    result = jnp.moveaxis(result, 3, 0)
    return jnp.clip(result, -1.0, 1.0).astype(jnp.float32)


def draw_momenta(key, part):
    key_base = jax.random.fold_in(key, 21)
    shape = (4, 2, 3, 3, NX, NY, NZ * LT)
    base = jax.random.truncated_normal(key_base, -3.0, 3.0, shape, jnp.float32)
    identity = jnp.eye(3, dtype=jnp.float32)[:, :, None, None, None]
    real_part = 0.5 * (base[:, 0] - jnp.swapaxes(base[:, 0], 1, 2))
    imag_part = 0.5 * (base[:, 1] + jnp.swapaxes(base[:, 1], 1, 2))
    trace_imag = (imag_part[:, 0, 0] + imag_part[:, 1, 1] + imag_part[:, 2, 2]) / 3.0
    imag_part = imag_part - trace_imag[:, None, None] * identity
    return jnp.stack([real_part, imag_part], axis=1).astype(jnp.float32)


def setup_inputs(seed: int = 0) -> dict:
    keys = jax.random.split(jax.random.key(seed), 3)
    gauge_links = draw_gauge_links(jax.random.fold_in(keys[2], 71), 0)
    momenta = draw_momenta(jax.random.fold_in(keys[2], 71), 0)
    return dict(gauge_links=gauge_links, momenta=momenta)


kick_size = 0.25
step_size = 0.2


def matrix_product(left, right):
    real_part = 0.0
    imag_part = 0.0
    for inner in range(3):
        left_real = left[0][:, inner:inner + 1]
        left_imag = left[1][:, inner:inner + 1]
        right_real = right[0][inner:inner + 1]
        right_imag = right[1][inner:inner + 1]
        real_part = real_part + (left_real * right_real - left_imag * right_imag)
        imag_part = imag_part + (left_real * right_imag + left_imag * right_real)
    return jnp.stack([real_part, imag_part])


def adjoint(matrix):
    return jnp.stack([jnp.swapaxes(matrix[0], 0, 1), -jnp.swapaxes(matrix[1], 0, 1)])


def traceless_part(matrix):
    identity = jnp.eye(3, dtype=jnp.float32)[:, :, None, None, None]
    real_part = 0.5 * (matrix[0] - jnp.swapaxes(matrix[0], 0, 1))
    imag_part = 0.5 * (matrix[1] + jnp.swapaxes(matrix[1], 0, 1))
    trace_imag = (matrix[1][0, 0] + matrix[1][1, 1] + matrix[1][2, 2]) / 3.0
    return jnp.stack([real_part, imag_part - trace_imag * identity])


def complex_times(first, second):
    return (first[0] * second[0] - first[1] * second[1], first[0] * second[1] + first[1] * second[0])


def cayley(matrix):
    identity = jnp.eye(3, dtype=jnp.float32)[:, :, None, None, None]
    numerator = jnp.stack([identity + 0.5 * matrix[0], 0.5 * matrix[1]])
    denominator = jnp.stack([identity - 0.5 * matrix[0], -0.5 * matrix[1]])

    def element(row_index, column):
        return (denominator[0, row_index % 3, column % 3], denominator[1, row_index % 3, column % 3])

    cofactor = []
    for row_index in range(3):
        line = []
        for column in range(3):
            first = complex_times(element(column + 1, row_index + 1), element(column + 2, row_index + 2))
            second = complex_times(element(column + 1, row_index + 2), element(column + 2, row_index + 1))
            line.append((first[0] - second[0], first[1] - second[1]))
        cofactor.append(line)
    determinant = complex_times(element(0, 0), cofactor[0][0])
    for middle in (1, 2):
        extra = complex_times(element(0, middle), cofactor[middle][0])
        determinant = (determinant[0] + extra[0], determinant[1] + extra[1])
    norm_square = determinant[0] * determinant[0] + determinant[1] * determinant[1]
    inverse_det = (determinant[0] / norm_square, -determinant[1] / norm_square)
    real_rows = []
    imag_rows = []
    for row_index in range(3):
        values = [complex_times(cofactor[row_index][column], inverse_det) for column in range(3)]
        real_rows.append(jnp.stack([value[0] for value in values]))
        imag_rows.append(jnp.stack([value[1] for value in values]))
    inverse = jnp.stack([jnp.stack(real_rows), jnp.stack(imag_rows)])
    return matrix_product(numerator, inverse)


def roll_time(matrix, steps):
    shape = matrix.shape
    folded = matrix.reshape(shape[:-1] + (shape[-1] // LT, LT))
    return jnp.roll(folded, -steps, axis=-1).reshape(shape)


def displaced(matrix, direction, steps):
    if direction == 0:
        return jnp.roll(matrix, -steps, axis=-3)
    if direction == 1:
        return jnp.roll(matrix, -steps, axis=-2)
    if direction == 2:
        return jnp.roll(matrix, -steps * LT, axis=-1)
    return roll_time(matrix, steps)


def staple_sums(link_list):
    result = []
    for along in range(4):
        staple = None
        for across in range(4):
            if across == along:
                continue
            ahead_across = displaced(link_list[across], along, 1)
            upper_staple = matrix_product(matrix_product(ahead_across, adjoint(displaced(link_list[along], across, 1))), adjoint(link_list[across]))
            lower_staple = matrix_product(matrix_product(adjoint(ahead_across), adjoint(link_list[along])), link_list[across])
            term = upper_staple + displaced(lower_staple, across, -1)
            staple = term if staple is None else staple + term
        result.append(staple)
    return result


def reference(gauge_links, momenta):
    link_list = [gauge_links[index] for index in range(4)]
    first_staples = staple_sums(link_list)
    half_momenta = []
    new_list = []
    for along in range(4):
        gauge_force = traceless_part(matrix_product(link_list[along], first_staples[along]))
        half_step = momenta[along] - kick_size * gauge_force
        half_momenta.append(half_step)
        new_list.append(matrix_product(cayley(step_size * traceless_part(half_step)), link_list[along]))
    second_staples = staple_sums(new_list)
    final_momenta = []
    trace_total = jnp.float32(0.0)
    for along in range(4):
        loop_matrix = matrix_product(new_list[along], second_staples[along])
        final_momenta.append(half_momenta[along] - kick_size * traceless_part(loop_matrix))
        trace_total = trace_total + jnp.sum(loop_matrix[0][0, 0] + loop_matrix[0][1, 1] + loop_matrix[0][2, 2])
    plaquette = trace_total / (72.0 * NX * NY * NZ * LT)
    return (jnp.stack(new_list), jnp.stack(final_momenta), plaquette)
```

```python
import functools

import jax
import jax.numpy as jnp
from jax import lax
from jax.experimental import pallas as pl
from jax.experimental.pallas import tpu as pltpu
from jax.sharding import PartitionSpec as P

LT = 64
AXES = ("gx", "gy", "zt")
PAIRS = ((1, 3), (0, 3), (0, 1), (2, 3), (0, 2), (1, 2))
UPDATES = (3, 0, 2, 1)
MESH_ID = pl.DeviceIdType.MESH

kick_size = 0.25
step_size = 0.2


def mul(a, b):
    return a[0] * b[0] - a[1] * b[1], a[0] * b[1] + a[1] * b[0]


def mul_conj_second(a, b):
    return a[0] * b[0] + a[1] * b[1], a[1] * b[0] - a[0] * b[1]


def mul_conj_first(a, b):
    return a[0] * b[0] + a[1] * b[1], a[0] * b[1] - a[1] * b[0]


def add(a, b):
    return a[0] + b[0], a[1] + b[1]


def total(terms):
    result = terms[0]
    for term in terms[1:]:
        result = add(result, term)
    return result


def conj(a):
    return a[0], -a[1]


def pick(a, index):
    return a[0][index], a[1][index]


TINY = 1e-30
FAR = 1e15
CODED = 11


def project(first, rest):
    square = rest[0] * rest[0]
    for value in rest[1:]:
        square = square + value * value
    near = first >= 0.0
    low = jnp.where(near, 1.0 + first, square)
    factor = jnp.where(near, 1.0, 1.0 - first) / jnp.maximum(low, TINY)
    result = [value * factor for value in rest]
    result[0] = jnp.where(low < TINY, FAR, result[0])
    return result


def lift(values):
    square = values[0] * values[0]
    for value in values[1:]:
        square = square + value * value
    inverse = 1.0 / (1.0 + square)
    double = 2.0 * inverse
    return [(1.0 - square) * inverse] + [value * double for value in values]


def cross(a, b):
    result = []
    for i in range(3):
        j, k = (i + 1) % 3, (i + 2) % 3
        p, q = mul(a[j], b[k]), mul(a[k], b[j])
        result.append((p[0] - q[0], p[1] - q[1]))
    return result


def encode(rows):
    rows = [[pick(row, l) for l in range(3)] for row in rows]
    normal = cross(rows[0], rows[1])
    det = total([mul(rows[2][l], normal[l]) for l in range(3)])
    values = []
    for row in rows[:2]:
        flat = [part for entry in row for part in entry]
        values += project(flat[0], flat[1:])
    return values + project(det[0], [det[1]])


def decode(values):
    rows = []
    for start in (0, 5):
        flat = lift(values[start : start + 5])
        rows.append([(flat[2 * l], flat[2 * l + 1]) for l in range(3)])
    det = lift(values[10:])
    rows.append([mul_conj_second(det, entry) for entry in cross(rows[0], rows[1])])
    return rows


def kernel(
    sizes,
    volume,
    groups,
    links_in,
    mom_in,
    W,
    NM,
    plaq_out,
    V,
    MB,
    HB,
    TB,
    LB,
    YS,
    YR,
    YHS,
    YHR,
    ZS,
    ZR,
    ZHS,
    ZHR,
    ZL,
    YBS,
    YBR,
    ZBS,
    ZBR,
    TR,
    load_sem,
    fsend,
    frecv,
    bsend,
    brecv,
    tsend,
    trecv,
    *slots,
):
    coords = [lax.axis_index(axis) for axis in AXES]

    def device(offset):
        return tuple(
            lax.rem(coords[axis] + (offset[axis] % sizes[axis]), sizes[axis]) for axis in range(3)
        )

    def along(axis, distance):
        return tuple(distance if other == axis else 0 for other in range(3))

    loads = []
    for m in (3, 0, 1, 2):
        copy = pltpu.make_async_copy(links_in.at[m], V.at[m, :, :, :, 0:2], load_sem.at[m])
        copy.start()
        loads.append(copy)
    mom_load = pltpu.make_async_copy(mom_in, MB, load_sem.at[4])
    mom_load.start()

    barrier = pltpu.get_barrier_semaphore()
    partners = 0
    for axis in range(3):
        for k in range(1, sizes[axis]):
            pl.semaphore_signal(barrier, inc=1, device_id=device(along(axis, k)), device_id_type=MESH_ID)
            partners += 1

    shape3 = (1, 8, 128)
    lane = lax.broadcasted_iota(jnp.int32, shape3, 2)
    sub = lax.broadcasted_iota(jnp.int32, shape3, 1)
    t_index = lax.rem(lane, LT)
    half_lanes = lane.shape[-1] // 2
    low = lane < half_lanes
    t_last = t_index == LT - 1
    t_first = t_index == 0
    y_last = sub == 7
    y_first = sub == 0

    def choose(mask, a, b):
        return jnp.where(jnp.broadcast_to(mask, b.shape), jnp.broadcast_to(a, b.shape), b)

    pending = []

    def send(src, dst, offset, send_sem, recv_sem):
        copy = pltpu.make_async_remote_copy(
            src_ref=src,
            dst_ref=dst,
            send_sem=send_sem,
            recv_sem=recv_sem,
            device_id=device(offset),
            device_id_type=MESH_ID,
        )
        copy.start()
        pending.append(copy)
        return copy

    forward = {}
    backward = {}

    def forward_send(stage, d, m, src, dst):
        forward[stage, d, m] = send(
            src, dst, along(d, -1), fsend.at[stage, d, m], frecv.at[stage, d, m]
        )

    def send_link(m):
        for d in (2, 0, 1):
            if d == m:
                continue
            if d == 0:
                src, dst = V.at[m, :, :, :, 0], V.at[m, :, :, :, 2]
            elif d == 1:
                for r in range(2):
                    for i in range(3):
                        for x in range(2):
                            YS[m, r, i, :, x : x + 1] = V[m, r, i, :, x, 0:1, :]
                src, dst = YS.at[m], YR.at[0, m]
            else:
                rows = []
                for i in range(3):
                    parts = []
                    for r in range(2):
                        first = V[m, r, i, :, 0]
                        second = V[m, r, i, :, 1]
                        parts.append(choose(low, first, pltpu.roll(second, half_lanes, 2)))
                    rows.append(tuple(parts))
                for c, value in enumerate(encode(rows)):
                    ZS[m, c] = value
                src, dst = ZS.at[m], ZR.at[m]
            forward_send(0, d, m, src, dst)

    def send_half(m):
        for d in (2, 0, 1):
            if d == m:
                continue
            if d == 0:
                src, dst = HB.at[m, :, 0], HB.at[m, :, 2]
            elif d == 1:
                for x in range(2):
                    YHS[m, :, x : x + 1] = HB[m, :, x, 0:1, :]
                src, dst = YHS.at[m], YHR.at[m]
            else:
                first = HB[m, :, 0]
                second = HB[m, :, 1]
                ZHS[m] = choose(low, first, pltpu.roll(second, half_lanes, 2))
                src, dst = ZHS.at[m], ZHR.at[m]
            forward_send(1, d, m, src, dst)

    def send_back(stage, d, m):
        if d == 3:
            return
        if d == 0:
            src, dst = LB.at[stage, 0, m, :, 2], LB.at[stage, 0, m, :, 0]
        elif d == 1:
            for x in range(2):
                YBS[stage, m, :, x] = LB[stage, 1, m, :, x + 1, 7:8, :]
            src, dst = YBS.at[stage, m], YBR.at[stage, m]
        else:
            first = LB[stage, 2, m, :, 1]
            second = LB[stage, 2, m, :, 2]
            ZBS[stage, m] = choose(low, pltpu.roll(first, half_lanes, 2), second)
            src, dst = ZBS.at[stage, m], ZBR.at[stage, m]
        backward[stage, d, m] = send(src, dst, along(d, 1), bsend.at[stage, d, m], brecv.at[stage, d, m])

    def ahead(stage, buf, n, d, x):
        rows = []
        for k in range(3):
            parts = []
            for r in range(2):
                if d == 0:
                    parts.append(buf[n, r, k, :, x + 1])
                    continue
                value = buf[n, r, k, :, x]
                if d == 3:
                    parts.append(
                        choose(t_last, pltpu.roll(value, LT - 1, 2), pltpu.roll(value, 127, 2))
                    )
                elif d == 1:
                    row = YR[stage, n, r, k, :, pl.ds(x, 1)]
                    parts.append(choose(y_last, row, pltpu.roll(value, 7, 1)))
                else:
                    halo = pltpu.roll(ZL[stage, n, r, k], half_lanes * (1 - x), 2)
                    parts.append(choose(low, pltpu.roll(value, half_lanes, 2), halo))
            rows.append(tuple(parts))
        return rows

    def behind(stage, d, m, x):
        if d == 0:
            return LB[stage, 0, m, :, x]
        value = LB[stage, d, m, :, x + 1]
        if d == 1:
            return choose(y_first, YBR[stage, m, :, x], pltpu.roll(value, 1, 1))
        if d == 2:
            halo = pltpu.roll(ZBR[stage, m], half_lanes * x, 2)
            return choose(low, halo, pltpu.roll(value, half_lanes, 2))
        return choose(t_first, pltpu.roll(value, 128 - (LT - 1), 2), pltpu.roll(value, 1, 2))

    def conjugate(T, rows):
        d0, d1, d2, h01, h02, h12 = T
        full = [
            [d0, h01, h02],
            [(-h01[0], h01[1]), d1, h12],
            [(-h02[0], h02[1]), (-h12[0], h12[1]), d2],
        ]
        M = []
        for i in range(3):
            terms = []
            for k in range(3):
                if i == k:
                    terms.append((-(full[i][i] * rows[k][1]), full[i][i] * rows[k][0]))
                else:
                    terms.append(mul(full[i][k], rows[k]))
            M.append(total(terms))
        r0 = 0.0
        r1 = 0.0
        for k in range(3):
            r0 = r0 + (rows[k][0][0] * M[k][1][0] - rows[k][1][0] * M[k][0][0])
            r1 = r1 + (rows[k][0][1] * M[k][1][1] - rows[k][1][1] * M[k][0][1])
        tail = slice(1, 3)
        row0 = total(
            [mul_conj_first(pick(rows[k], 0), (M[k][0][tail], M[k][1][tail])) for k in range(3)]
        )
        r12 = total([mul_conj_first(pick(rows[k], 1), pick(M[k], 2)) for k in range(3)])
        return [r0, r1, row0[0][0], row0[1][0], row0[0][1], row0[1][1], r12[0], r12[1]]

    def pair_task(stage, buf, m, n, x):
        index = PAIRS.index((m, n))
        n_ahead = ahead(stage, buf, n, m, x)
        A = []
        for i in range(3):
            A.append(
                total(
                    [mul((buf[m, 0, i, k, x], buf[m, 1, i, k, x]), n_ahead[k]) for k in range(3)]
                )
            )
        m_ahead = ahead(stage, buf, m, n, x)
        columns = [(buf[n, 0, :, l, x], buf[n, 1, :, l, x]) for l in range(3)]
        Bt = []
        for k in range(3):
            Bt.append(total([mul(pick(m_ahead[l], k), columns[l]) for l in range(3)]))
        loop = []
        for i in range(3):
            loop.append(total([mul_conj_second(pick(A[i], k), Bt[k]) for k in range(3)]))
        i0, i1, i2 = loop[0][1][0], loop[1][1][1], loop[2][1][2]
        mean = (i0 + i1 + i2) * (2.0 / 3.0)
        d0 = 2.0 * i0 - mean
        d1 = 2.0 * i1 - mean
        d2 = -(d0 + d1)

        def off(i, j):
            a = pick(loop[i], j)
            b = pick(loop[j], i)
            return a[0] - b[0], a[1] + b[1]

        h01, h02, h12 = off(0, 1), off(0, 2), off(1, 2)
        values = [d0, d1, h01[0], h01[1], h02[0], h02[1], h12[0], h12[1]]
        for c in range(8):
            TB[index, c, x] = values[c]
        if stage == 1:
            trace = loop[0][0][0] + loop[1][0][1] + loop[2][0][2]
            TR[x] = trace if index == 0 else TR[x] + trace
        T = (d0, d1, d2, h01, h02, h12)
        for link, d in ((m, n), (n, m)):
            rows = [(buf[d, 0, k, :, x], buf[d, 1, k, :, x]) for k in range(3)]
            result = conjugate(T, rows)
            for c in range(8):
                LB[stage, d, link, c, x + 1] = result[c]

    def force(stage, m, x):
        result = None
        for n in range(4):
            if n == m:
                continue
            index = PAIRS.index((min(m, n), max(m, n)))
            term = TB[index, :, x] - behind(stage, n, m, x)
            if result is None:
                result = term if m < n else -term
            else:
                result = result + term if m < n else result - term
        return result

    places = ((1, 0, 0), (1, 1, 1), (0, 0, 1), (1, 0, 1), (0, 0, 2), (1, 0, 2), (0, 1, 2), (1, 1, 2))

    def half_update(m, x):
        F = force(0, m, x)
        for c, (r, i, j) in enumerate(places):
            HB[m, c, x] = MB[m, r, i, j, x] - (0.5 * kick_size) * F[c]

    def cayley(momentum, rows):
        half = [(0.5 * step_size) * value for value in momentum]
        d0, d1 = half[0], half[1]
        d2 = -(d0 + d1)
        h01, h02, h12 = (half[2], half[3]), (half[4], half[5]), (half[6], half[7])
        n01 = h01[0] * h01[0] + h01[1] * h01[1]
        n02 = h02[0] * h02[0] + h02[1] * h02[1]
        n12 = h12[0] * h12[0] + h12[1] * h12[1]
        k00 = d0 * d0 + n01 + n02
        k11 = d1 * d1 + n01 + n12
        k22 = d2 * d2 + n02 + n12
        one_c = 1.0 + 0.5 * (k00 + k11 + k22)
        h01h12 = mul(h01, h12)
        z_imag = h01h12[1] * h02[0] - h01h12[0] * h02[1]
        h = d0 * n12 + d2 * n01 + d1 * n02 - d0 * d1 * d2 - 2.0 * z_imag
        factor = 2.0 / (one_c * one_c + h * h)
        f = (one_c * factor, h * factor)
        s01 = mul_conj_second(h02, h12)
        k01 = (-(d0 + d1) * h01[1] - s01[0], (d0 + d1) * h01[0] - s01[1])
        k02 = (h01h12[0] - (d0 + d2) * h02[1], h01h12[1] + (d0 + d2) * h02[0])
        s12 = mul_conj_first(h01, h02)
        k12 = (-s12[0] - (d1 + d2) * h12[1], (d1 + d2) * h12[0] - s12[1])
        G = [[None] * 3 for _ in range(3)]
        for i, (k, d) in enumerate(((k00, d0), (k11, d1), (k22, d2))):
            G[i][i] = (one_c - k, d)
        for i, j, hh, kk in ((0, 1, h01, k01), (0, 2, h02, k02), (1, 2, h12, k12)):
            G[i][j] = add(hh, kk)
            G[j][i] = (kk[0] - hh[0], hh[1] - kk[1])
        result = []
        for i in range(3):
            E = []
            for k in range(3):
                value = mul(f, G[i][k])
                E.append((value[0] - 1.0, value[1]) if i == k else value)
            result.append(total([mul(E[k], rows[k]) for k in range(3)]))
        return result

    def link_update(m, x):
        rows = [(V[m, 0, k, :, x], V[m, 1, k, :, x]) for k in range(3)]
        new = cayley([HB[m, c, x] for c in range(8)], rows)
        for i in range(3):
            W[m, 0, i, :, x] = new[i][0]
            W[m, 1, i, :, x] = new[i][1]

    def halo_update(d, m):
        if d == 0:
            link_update(m, 2)
            return
        buf, momentum = (YR, YHR) if d == 1 else (ZL, ZHR)
        rows = [(buf[0, m, 0, k], buf[0, m, 1, k]) for k in range(3)]
        new = cayley([momentum[m, c] for c in range(8)], rows)
        for i in range(3):
            buf[1, m, 0, i] = new[i][0]
            buf[1, m, 1, i] = new[i][1]

    def halo_decode(m):
        rows = decode([ZR[m, c] for c in range(CODED)])
        for k in range(3):
            for r in range(2):
                for l in range(3):
                    ZL[0, m, r, k, l] = rows[k][l][r]

    def last_update(m, x):
        F = force(1, m, x)
        v = [HB[m, c, x] - (0.5 * kick_size) * F[c] for c in range(8)]
        zero = jnp.zeros_like(v[0])
        for i in range(3):
            NM[m, 0, i, i, x] = zero
        NM[m, 1, 0, 0, x] = v[0]
        NM[m, 1, 1, 1, x] = v[1]
        NM[m, 1, 2, 2, x] = -(v[0] + v[1])
        for i, j, c in ((0, 1, 2), (0, 2, 4), (1, 2, 6)):
            NM[m, 0, i, j, x] = v[c]
            NM[m, 0, j, i, x] = -v[c]
            NM[m, 1, i, j, x] = v[c + 1]
            NM[m, 1, j, i, x] = v[c + 1]

    def for_x(body):
        def step(x, carry):
            body(x)
            return carry

        lax.fori_loop(0, 2, step, 0)

    def pairs_of(stage, buf):
        for m, n in PAIRS:
            for link, d in ((n, m), (m, n)):
                if d == 3:
                    continue
                with jax.named_scope(f"wf{stage}_d{d}m{link}"):
                    forward[stage, d, link].wait_recv()
                if stage == 1:
                    halo_update(d, link)
                elif d == 2:
                    halo_decode(link)
            for_x(lambda x: pair_task(stage, buf, m, n, x))
            for link, d in ((m, n), (n, m)):
                send_back(stage, d, link)

    def wait_back(stage, m):
        for d in range(3):
            if d != m:
                backward[stage, d, m].wait_recv()

    for position, m in enumerate((3, 0, 1, 2)):
        loads[position].wait()
        if position == 0:
            with jax.named_scope("bar"):
                pl.semaphore_wait(barrier, partners)
        send_link(m)
    pairs_of(0, V)
    mom_load.wait()
    for m in UPDATES:
        with jax.named_scope(f"wb0_{m}"):
            wait_back(0, m)
        for_x(lambda x: half_update(m, x))
        send_half(m)
        for_x(lambda x: link_update(m, x))
    pairs_of(1, W)

    def offsets(group):
        result = [()]
        for axis in range(3):
            span = range(sizes[axis]) if axis in group else (0,)
            result = [head + (k,) for head in result for k in span]
        return [item for item in result if any(item)]

    def spread(index, value):
        buf = slots[index]
        position = 0
        for axis in groups[index]:
            position = position * sizes[axis] + coords[axis]
        buf[position] = jnp.sum(value, axis=0, keepdims=True)
        copies = []
        for k, offset in enumerate(offsets(groups[index])):
            copies.append(
                send(
                    buf.at[position],
                    buf.at[position],
                    offset,
                    tsend.at[index, k],
                    trecv.at[index, k],
                )
            )
        return copies

    def gathered(index, copies):
        for copy in copies:
            copy.wait_recv()
        value = slots[index][0]
        for k in range(1, slots[index].shape[0]):
            value = value + slots[index][k]
        return value

    def finish(m):
        with jax.named_scope(f"wb1_{m}"):
            wait_back(1, m)
        for_x(lambda x: last_update(m, x))

    value = TR[0] + TR[1]
    copies = spread(0, value)
    for position, m in enumerate(UPDATES):
        finish(m)
        if position + 1 < len(groups):
            value = gathered(position, copies)
            copies = spread(position + 1, value)
    with jax.named_scope("plaq"):
        lanes = gathered(len(groups) - 1, copies) * (4.0 / (72.0 * volume))
        plaq_out[...] = jnp.sum(lanes, axis=1, keepdims=True)
    for copy in pending:
        copy.wait_send()


def store_kernel(links, mom, plaq, links_out, mom_out, plaq_out, sem):
    copies = [pltpu.make_async_copy(plaq, plaq_out, sem.at[8])]
    for m in range(4):
        copies.append(
            pltpu.make_async_copy(links.at[m, :, :, :, 0:2], links_out.at[m], sem.at[m])
        )
        copies.append(pltpu.make_async_copy(mom.at[m], mom_out.at[m], sem.at[4 + m]))
    for copy in copies:
        copy.start()
    for copy in copies:
        copy.wait()


def per_device(gauge_links, momenta):
    block = gauge_links.shape
    assert block[-3:] == (2, 8, 2 * LT)
    sizes = tuple(lax.axis_size(axis) for axis in AXES)
    sites = block[-3] * block[-2] * block[-1]
    volume = sites * sizes[0] * sizes[1] * sizes[2]
    f32 = jnp.float32
    vm = lambda *shape: pltpu.VMEM(shape, f32)
    groups = ((0, 1, 2),) if sizes[0] * sizes[1] * sizes[2] <= 32 else ((0,), (1,), (2,))
    counts = []
    for group in groups:
        count = 1
        for axis in group:
            count *= sizes[axis]
        counts.append(count)
    dma = pltpu.SemaphoreType.DMA
    wide_links, momenta_vmem, plaquette = pl.pallas_call(
        functools.partial(kernel, sizes, volume, groups),
        out_shape=(
            vm(4, 2, 3, 3, 3, 8, 128),
            vm(*block),
            vm(1, 1),
        ),
        in_specs=[pl.BlockSpec(memory_space=pl.ANY)] * 2,
        out_specs=(
            pl.BlockSpec(memory_space=pltpu.VMEM),
            pl.BlockSpec(memory_space=pltpu.VMEM),
            pl.BlockSpec(memory_space=pltpu.VMEM),
        ),
        scratch_shapes=[
            vm(4, 2, 3, 3, 3, 8, 128),
            vm(*block),
            vm(4, 8, 3, 8, 128),
            vm(6, 8, 2, 8, 128),
            vm(2, 4, 4, 8, 3, 8, 128),
            vm(4, 2, 3, 3, 2, 128),
            vm(2, 4, 2, 3, 3, 2, 128),
            vm(4, 8, 2, 128),
            vm(4, 8, 2, 128),
            vm(4, CODED, 8, 128),
            vm(4, CODED, 8, 128),
            vm(4, 8, 8, 128),
            vm(4, 8, 8, 128),
            vm(2, 4, 2, 3, 3, 8, 128),
            vm(2, 4, 8, 2, 1, 128),
            vm(2, 4, 8, 2, 1, 128),
            vm(2, 4, 8, 8, 128),
            vm(2, 4, 8, 8, 128),
            vm(2, 8, 128),
            dma((5,)),
            dma((2, 3, 4)),
            dma((2, 3, 4)),
            dma((2, 3, 4)),
            dma((2, 3, 4)),
            dma((len(groups), max(counts))),
            dma((len(groups), max(counts))),
            *[vm(count, 1, 128) for count in counts],
        ],
        compiler_params=pltpu.CompilerParams(collective_id=0, has_side_effects=True),
        name="md_step",
    )(gauge_links, momenta)
    anywhere = pl.BlockSpec(memory_space=pl.ANY)
    in_vmem = pl.BlockSpec(memory_space=pltpu.VMEM)
    new_links, new_momenta, plaquette = pl.pallas_call(
        store_kernel,
        out_shape=(
            jax.ShapeDtypeStruct(block, f32),
            jax.ShapeDtypeStruct(block, f32),
            jax.ShapeDtypeStruct((1, 1), f32),
        ),
        in_specs=[in_vmem] * 3,
        out_specs=(anywhere,) * 3,
        scratch_shapes=[dma((9,))],
        name="store",
    )(
        pltpu.with_memory_space_constraint(wide_links, pltpu.VMEM),
        pltpu.with_memory_space_constraint(momenta_vmem, pltpu.VMEM),
        pltpu.with_memory_space_constraint(plaquette, pltpu.VMEM),
    )
    return new_links, new_momenta, plaquette.reshape(())


def solution(mesh):
    spec = P(None, None, None, None, "gx", "gy", "zt")
    return jax.shard_map(
        per_device,
        mesh=mesh,
        in_specs=(spec, spec),
        out_specs=(spec, spec, P()),
        check_vma=False,
    )
```

```python
import functools

import jax
import jax.numpy as jnp
from jax import lax
from jax.experimental import pallas as pl
from jax.experimental.pallas import tpu as pltpu
from jax.sharding import PartitionSpec as P

LT = 64
AXES = ("gx", "gy", "zt")
PAIRS = ((1, 3), (0, 3), (0, 1), (2, 3), (0, 2), (1, 2))
UPDATES = (3, 0, 2, 1)
MESH_ID = pl.DeviceIdType.MESH

kick_size = 0.25
step_size = 0.2


def mul(a, b):
    return a[0] * b[0] - a[1] * b[1], a[0] * b[1] + a[1] * b[0]


def mul_conj_second(a, b):
    return a[0] * b[0] + a[1] * b[1], a[1] * b[0] - a[0] * b[1]


def mul_conj_first(a, b):
    return a[0] * b[0] + a[1] * b[1], a[0] * b[1] - a[1] * b[0]


def add(a, b):
    return a[0] + b[0], a[1] + b[1]


def total(terms):
    result = terms[0]
    for term in terms[1:]:
        result = add(result, term)
    return result


def conj(a):
    return a[0], -a[1]


def pick(a, index):
    return a[0][index], a[1][index]


TINY = 1e-30
FAR = 1e15
CODED = 11


def project(first, rest):
    square = rest[0] * rest[0]
    for value in rest[1:]:
        square = square + value * value
    near = first >= 0.0
    low = jnp.where(near, 1.0 + first, square)
    factor = jnp.where(near, 1.0, 1.0 - first) / jnp.maximum(low, TINY)
    result = [value * factor for value in rest]
    result[0] = jnp.where(low < TINY, FAR, result[0])
    return result


def lift(values):
    square = values[0] * values[0]
    for value in values[1:]:
        square = square + value * value
    inverse = 1.0 / (1.0 + square)
    double = 2.0 * inverse
    return [(1.0 - square) * inverse] + [value * double for value in values]


def cross(a, b):
    result = []
    for i in range(3):
        j, k = (i + 1) % 3, (i + 2) % 3
        p, q = mul(a[j], b[k]), mul(a[k], b[j])
        result.append((p[0] - q[0], p[1] - q[1]))
    return result


def encode(rows):
    rows = [[pick(row, l) for l in range(3)] for row in rows]
    normal = cross(rows[0], rows[1])
    det = total([mul(rows[2][l], normal[l]) for l in range(3)])
    values = []
    for row in rows[:2]:
        flat = [part for entry in row for part in entry]
        values += project(flat[0], flat[1:])
    return values + project(det[0], [det[1]])


def decode(values):
    rows = []
    for start in (0, 5):
        flat = lift(values[start : start + 5])
        rows.append([(flat[2 * l], flat[2 * l + 1]) for l in range(3)])
    det = lift(values[10:])
    rows.append([mul_conj_second(det, entry) for entry in cross(rows[0], rows[1])])
    return rows


def kernel(
    sizes,
    volume,
    groups,
    links_in,
    mom_in,
    W,
    NM,
    plaq_out,
    V,
    MB,
    HB,
    TB,
    LB,
    YS,
    YR,
    YHS,
    YHR,
    ZS,
    ZR,
    ZHS,
    ZHR,
    ZL,
    YBS,
    YBR,
    ZBS,
    ZBR,
    TR,
    load_sem,
    fsend,
    frecv,
    bsend,
    brecv,
    tsend,
    trecv,
    *slots,
):
    coords = [lax.axis_index(axis) for axis in AXES]

    def device(offset):
        return tuple(
            lax.rem(coords[axis] + (offset[axis] % sizes[axis]), sizes[axis]) for axis in range(3)
        )

    def along(axis, distance):
        return tuple(distance if other == axis else 0 for other in range(3))

    loads = []
    for m in (3, 0, 1, 2):
        copy = pltpu.make_async_copy(links_in.at[m], V.at[m, :, :, :, 0:2], load_sem.at[m])
        copy.start()
        loads.append(copy)
    mom_load = pltpu.make_async_copy(mom_in, MB, load_sem.at[4])
    mom_load.start()

    barrier = pltpu.get_barrier_semaphore()
    partners = 0
    for axis in range(3):
        for k in range(1, sizes[axis]):
            pl.semaphore_signal(barrier, inc=1, device_id=device(along(axis, k)), device_id_type=MESH_ID)
            partners += 1

    shape3 = (1, 8, 128)
    lane = lax.broadcasted_iota(jnp.int32, shape3, 2)
    sub = lax.broadcasted_iota(jnp.int32, shape3, 1)
    t_index = lax.rem(lane, LT)
    half_lanes = lane.shape[-1] // 2
    low = lane < half_lanes
    t_last = t_index == LT - 1
    t_first = t_index == 0
    y_last = sub == 7
    y_first = sub == 0

    def choose(mask, a, b):
        return jnp.where(jnp.broadcast_to(mask, b.shape), jnp.broadcast_to(a, b.shape), b)

    pending = []

    def send(src, dst, offset, send_sem, recv_sem):
        copy = pltpu.make_async_remote_copy(
            src_ref=src,
            dst_ref=dst,
            send_sem=send_sem,
            recv_sem=recv_sem,
            device_id=device(offset),
            device_id_type=MESH_ID,
        )
        copy.start()
        pending.append(copy)
        return copy

    forward = {}
    backward = {}

    def forward_send(stage, d, m, src, dst):
        forward[stage, d, m] = send(
            src, dst, along(d, -1), fsend.at[stage, d, m], frecv.at[stage, d, m]
        )

    def send_link(m):
        for d in (2, 0, 1):
            if d == m:
                continue
            if d == 0:
                src, dst = V.at[m, :, :, :, 0], V.at[m, :, :, :, 2]
            elif d == 1:
                for r in range(2):
                    for i in range(3):
                        for x in range(2):
                            YS[m, r, i, :, x : x + 1] = V[m, r, i, :, x, 0:1, :]
                src, dst = YS.at[m], YR.at[0, m]
            else:
                rows = []
                for i in range(3):
                    parts = []
                    for r in range(2):
                        first = V[m, r, i, :, 0]
                        second = V[m, r, i, :, 1]
                        parts.append(choose(low, first, pltpu.roll(second, half_lanes, 2)))
                    rows.append(tuple(parts))
                for c, value in enumerate(encode(rows)):
                    ZS[m, c] = value
                src, dst = ZS.at[m], ZR.at[m]
            forward_send(0, d, m, src, dst)

    def send_half(m):
        for d in (2, 0, 1):
            if d == m:
                continue
            if d == 0:
                src, dst = HB.at[m, :, 0], HB.at[m, :, 2]
            elif d == 1:
                for x in range(2):
                    YHS[m, :, x : x + 1] = HB[m, :, x, 0:1, :]
                src, dst = YHS.at[m], YHR.at[m]
            else:
                first = HB[m, :, 0]
                second = HB[m, :, 1]
                ZHS[m] = choose(low, first, pltpu.roll(second, half_lanes, 2))
                src, dst = ZHS.at[m], ZHR.at[m]
            forward_send(1, d, m, src, dst)

    def send_back(stage, d, m):
        if d == 3:
            return
        if d == 0:
            src, dst = LB.at[stage, 0, m, :, 2], LB.at[stage, 0, m, :, 0]
        elif d == 1:
            for x in range(2):
                YBS[stage, m, :, x] = LB[stage, 1, m, :, x + 1, 7:8, :]
            src, dst = YBS.at[stage, m], YBR.at[stage, m]
        else:
            first = LB[stage, 2, m, :, 1]
            second = LB[stage, 2, m, :, 2]
            ZBS[stage, m] = choose(low, pltpu.roll(first, half_lanes, 2), second)
            src, dst = ZBS.at[stage, m], ZBR.at[stage, m]
        backward[stage, d, m] = send(src, dst, along(d, 1), bsend.at[stage, d, m], brecv.at[stage, d, m])

    def ahead(stage, buf, n, d, x):
        rows = []
        for k in range(3):
            parts = []
            for r in range(2):
                if d == 0:
                    parts.append(buf[n, r, k, :, x + 1])
                    continue
                value = buf[n, r, k, :, x]
                if d == 3:
                    parts.append(
                        choose(t_last, pltpu.roll(value, LT - 1, 2), pltpu.roll(value, 127, 2))
                    )
                elif d == 1:
                    row = YR[stage, n, r, k, :, pl.ds(x, 1)]
                    parts.append(choose(y_last, row, pltpu.roll(value, 7, 1)))
                else:
                    halo = pltpu.roll(ZL[stage, n, r, k], half_lanes * (1 - x), 2)
                    parts.append(choose(low, pltpu.roll(value, half_lanes, 2), halo))
            rows.append(tuple(parts))
        return rows

    def behind(stage, d, m, x):
        if d == 0:
            return LB[stage, 0, m, :, x]
        value = LB[stage, d, m, :, x + 1]
        if d == 1:
            return choose(y_first, YBR[stage, m, :, x], pltpu.roll(value, 1, 1))
        if d == 2:
            halo = pltpu.roll(ZBR[stage, m], half_lanes * x, 2)
            return choose(low, halo, pltpu.roll(value, half_lanes, 2))
        return choose(t_first, pltpu.roll(value, 128 - (LT - 1), 2), pltpu.roll(value, 1, 2))

    def conjugate(T, rows):
        d0, d1, d2, h01, h02, h12 = T
        full = [
            [d0, h01, h02],
            [(-h01[0], h01[1]), d1, h12],
            [(-h02[0], h02[1]), (-h12[0], h12[1]), d2],
        ]
        M = []
        for i in range(3):
            terms = []
            for k in range(3):
                if i == k:
                    terms.append((-(full[i][i] * rows[k][1]), full[i][i] * rows[k][0]))
                else:
                    terms.append(mul(full[i][k], rows[k]))
            M.append(total(terms))
        r0 = 0.0
        r1 = 0.0
        for k in range(3):
            r0 = r0 + (rows[k][0][0] * M[k][1][0] - rows[k][1][0] * M[k][0][0])
            r1 = r1 + (rows[k][0][1] * M[k][1][1] - rows[k][1][1] * M[k][0][1])
        tail = slice(1, 3)
        row0 = total(
            [mul_conj_first(pick(rows[k], 0), (M[k][0][tail], M[k][1][tail])) for k in range(3)]
        )
        r12 = total([mul_conj_first(pick(rows[k], 1), pick(M[k], 2)) for k in range(3)])
        return [r0, r1, row0[0][0], row0[1][0], row0[0][1], row0[1][1], r12[0], r12[1]]

    def pair_task(stage, buf, m, n, x):
        index = PAIRS.index((m, n))
        n_ahead = ahead(stage, buf, n, m, x)
        A = []
        for i in range(3):
            A.append(
                total(
                    [mul((buf[m, 0, i, k, x], buf[m, 1, i, k, x]), n_ahead[k]) for k in range(3)]
                )
            )
        m_ahead = ahead(stage, buf, m, n, x)
        columns = [(buf[n, 0, :, l, x], buf[n, 1, :, l, x]) for l in range(3)]
        Bt = []
        for k in range(3):
            Bt.append(total([mul(pick(m_ahead[l], k), columns[l]) for l in range(3)]))
        loop = []
        for i in range(3):
            loop.append(total([mul_conj_second(pick(A[i], k), Bt[k]) for k in range(3)]))
        i0, i1, i2 = loop[0][1][0], loop[1][1][1], loop[2][1][2]
        mean = (i0 + i1 + i2) * (2.0 / 3.0)
        d0 = 2.0 * i0 - mean
        d1 = 2.0 * i1 - mean
        d2 = -(d0 + d1)

        def off(i, j):
            a = pick(loop[i], j)
            b = pick(loop[j], i)
            return a[0] - b[0], a[1] + b[1]

        h01, h02, h12 = off(0, 1), off(0, 2), off(1, 2)
        values = [d0, d1, h01[0], h01[1], h02[0], h02[1], h12[0], h12[1]]
        for c in range(8):
            TB[index, c, x] = values[c]
        if stage == 1:
            trace = loop[0][0][0] + loop[1][0][1] + loop[2][0][2]
            TR[x] = trace if index == 0 else TR[x] + trace
        T = (d0, d1, d2, h01, h02, h12)
        for link, d in ((m, n), (n, m)):
            rows = [(buf[d, 0, k, :, x], buf[d, 1, k, :, x]) for k in range(3)]
            result = conjugate(T, rows)
            for c in range(8):
                LB[stage, d, link, c, x + 1] = result[c]

    def force(stage, m, x):
        result = None
        for n in range(4):
            if n == m:
                continue
            index = PAIRS.index((min(m, n), max(m, n)))
            term = TB[index, :, x] - behind(stage, n, m, x)
            if result is None:
                result = term if m < n else -term
            else:
                result = result + term if m < n else result - term
        return result

    places = ((1, 0, 0), (1, 1, 1), (0, 0, 1), (1, 0, 1), (0, 0, 2), (1, 0, 2), (0, 1, 2), (1, 1, 2))

    def half_update(m, x):
        F = force(0, m, x)
        for c, (r, i, j) in enumerate(places):
            HB[m, c, x] = MB[m, r, i, j, x] - (0.5 * kick_size) * F[c]

    def cayley(momentum, rows):
        half = [(0.5 * step_size) * value for value in momentum]
        d0, d1 = half[0], half[1]
        d2 = -(d0 + d1)
        h01, h02, h12 = (half[2], half[3]), (half[4], half[5]), (half[6], half[7])
        n01 = h01[0] * h01[0] + h01[1] * h01[1]
        n02 = h02[0] * h02[0] + h02[1] * h02[1]
        n12 = h12[0] * h12[0] + h12[1] * h12[1]
        k00 = d0 * d0 + n01 + n02
        k11 = d1 * d1 + n01 + n12
        k22 = d2 * d2 + n02 + n12
        one_c = 1.0 + 0.5 * (k00 + k11 + k22)
        h01h12 = mul(h01, h12)
        z_imag = h01h12[1] * h02[0] - h01h12[0] * h02[1]
        h = d0 * n12 + d2 * n01 + d1 * n02 - d0 * d1 * d2 - 2.0 * z_imag
        factor = 2.0 / (one_c * one_c + h * h)
        f = (one_c * factor, h * factor)
        s01 = mul_conj_second(h02, h12)
        k01 = (-(d0 + d1) * h01[1] - s01[0], (d0 + d1) * h01[0] - s01[1])
        k02 = (h01h12[0] - (d0 + d2) * h02[1], h01h12[1] + (d0 + d2) * h02[0])
        s12 = mul_conj_first(h01, h02)
        k12 = (-s12[0] - (d1 + d2) * h12[1], (d1 + d2) * h12[0] - s12[1])
        G = [[None] * 3 for _ in range(3)]
        for i, (k, d) in enumerate(((k00, d0), (k11, d1), (k22, d2))):
            G[i][i] = (one_c - k, d)
        for i, j, hh, kk in ((0, 1, h01, k01), (0, 2, h02, k02), (1, 2, h12, k12)):
            G[i][j] = add(hh, kk)
            G[j][i] = (kk[0] - hh[0], hh[1] - kk[1])
        result = []
        for i in range(3):
            E = []
            for k in range(3):
                value = mul(f, G[i][k])
                E.append((value[0] - 1.0, value[1]) if i == k else value)
            result.append(total([mul(E[k], rows[k]) for k in range(3)]))
        return result

    def link_update(m, x):
        rows = [(V[m, 0, k, :, x], V[m, 1, k, :, x]) for k in range(3)]
        new = cayley([HB[m, c, x] for c in range(8)], rows)
        for i in range(3):
            W[m, 0, i, :, x] = new[i][0]
            W[m, 1, i, :, x] = new[i][1]

    def halo_update(d, m):
        if d == 0:
            link_update(m, 2)
            return
        buf, momentum = (YR, YHR) if d == 1 else (ZL, ZHR)
        rows = [(buf[0, m, 0, k], buf[0, m, 1, k]) for k in range(3)]
        new = cayley([momentum[m, c] for c in range(8)], rows)
        for i in range(3):
            buf[1, m, 0, i] = new[i][0]
            buf[1, m, 1, i] = new[i][1]

    def halo_decode(m):
        rows = decode([ZR[m, c] for c in range(CODED)])
        for k in range(3):
            for r in range(2):
                for l in range(3):
                    ZL[0, m, r, k, l] = rows[k][l][r]

    def last_update(m, x):
        F = force(1, m, x)
        v = [HB[m, c, x] - (0.5 * kick_size) * F[c] for c in range(8)]
        zero = jnp.zeros_like(v[0])
        for i in range(3):
            NM[m, 0, i, i, x] = zero
        NM[m, 1, 0, 0, x] = v[0]
        NM[m, 1, 1, 1, x] = v[1]
        NM[m, 1, 2, 2, x] = -(v[0] + v[1])
        for i, j, c in ((0, 1, 2), (0, 2, 4), (1, 2, 6)):
            NM[m, 0, i, j, x] = v[c]
            NM[m, 0, j, i, x] = -v[c]
            NM[m, 1, i, j, x] = v[c + 1]
            NM[m, 1, j, i, x] = v[c + 1]

    def for_x(body):
        def step(x, carry):
            body(x)
            return carry

        lax.fori_loop(0, 2, step, 0)

    def pairs_of(stage, buf):
        for m, n in PAIRS:
            for link, d in ((n, m), (m, n)):
                if d == 3:
                    continue
                with jax.named_scope(f"wf{stage}_d{d}m{link}"):
                    forward[stage, d, link].wait_recv()
                if stage == 1:
                    halo_update(d, link)
                elif d == 2:
                    halo_decode(link)
            for_x(lambda x: pair_task(stage, buf, m, n, x))
            for link, d in ((m, n), (n, m)):
                send_back(stage, d, link)

    def wait_back(stage, m):
        for d in range(3):
            if d != m:
                backward[stage, d, m].wait_recv()

    for position, m in enumerate((3, 0, 1, 2)):
        loads[position].wait()
        if position == 0:
            with jax.named_scope("bar"):
                pl.semaphore_wait(barrier, partners)
        send_link(m)
    pairs_of(0, V)
    mom_load.wait()
    for m in UPDATES:
        with jax.named_scope(f"wb0_{m}"):
            wait_back(0, m)
        for_x(lambda x: half_update(m, x))
        send_half(m)
        for_x(lambda x: link_update(m, x))
    pairs_of(1, W)

    def offsets(group):
        result = [()]
        for axis in range(3):
            span = range(sizes[axis]) if axis in group else (0,)
            result = [head + (k,) for head in result for k in span]
        return [item for item in result if any(item)]

    def spread(index, value):
        buf = slots[index]
        position = 0
        for axis in groups[index]:
            position = position * sizes[axis] + coords[axis]
        buf[position] = jnp.sum(value, axis=0, keepdims=True)
        copies = []
        for k, offset in enumerate(offsets(groups[index])):
            copies.append(
                send(
                    buf.at[position],
                    buf.at[position],
                    offset,
                    tsend.at[index, k],
                    trecv.at[index, k],
                )
            )
        return copies

    def gathered(index, copies):
        for copy in copies:
            copy.wait_recv()
        value = slots[index][0]
        for k in range(1, slots[index].shape[0]):
            value = value + slots[index][k]
        return value

    def finish(m):
        with jax.named_scope(f"wb1_{m}"):
            wait_back(1, m)
        for_x(lambda x: last_update(m, x))

    value = TR[0] + TR[1]
    copies = spread(0, value)
    for position, m in enumerate(UPDATES):
        finish(m)
        if position + 1 < len(groups):
            value = gathered(position, copies)
            copies = spread(position + 1, value)
    with jax.named_scope("plaq"):
        lanes = gathered(len(groups) - 1, copies) * (4.0 / (72.0 * volume))
        plaq_out[...] = jnp.broadcast_to(jnp.sum(lanes, axis=1, keepdims=True), (8, 128))
    for copy in pending:
        copy.wait_send()


def store_kernel(links, mom, plaq, links_out, mom_out, plaq_out, sem):
    copies = [pltpu.make_async_copy(plaq.at[0:1], plaq_out, sem.at[8])]
    for m in range(4):
        copies.append(
            pltpu.make_async_copy(links.at[m, :, :, :, 0:2], links_out.at[m], sem.at[m])
        )
        copies.append(pltpu.make_async_copy(mom.at[m], mom_out.at[m], sem.at[4 + m]))
    for copy in copies:
        copy.start()
    for copy in copies:
        copy.wait()


def per_device(gauge_links, momenta):
    block = gauge_links.shape
    assert block[-3:] == (2, 8, 2 * LT)
    sizes = tuple(lax.axis_size(axis) for axis in AXES)
    sites = block[-3] * block[-2] * block[-1]
    volume = sites * sizes[0] * sizes[1] * sizes[2]
    f32 = jnp.float32
    vm = lambda *shape: pltpu.VMEM(shape, f32)
    groups = ((0, 1, 2),) if sizes[0] * sizes[1] * sizes[2] <= 32 else ((0,), (1,), (2,))
    counts = []
    for group in groups:
        count = 1
        for axis in group:
            count *= sizes[axis]
        counts.append(count)
    dma = pltpu.SemaphoreType.DMA
    wide_links, momenta_vmem, plaquette = pl.pallas_call(
        functools.partial(kernel, sizes, volume, groups),
        out_shape=(
            vm(4, 2, 3, 3, 3, 8, 128),
            vm(*block),
            vm(8, 128),
        ),
        in_specs=[pl.BlockSpec(memory_space=pl.ANY)] * 2,
        out_specs=(
            pl.BlockSpec(memory_space=pltpu.VMEM),
            pl.BlockSpec(memory_space=pltpu.VMEM),
            pl.BlockSpec(memory_space=pltpu.VMEM),
        ),
        scratch_shapes=[
            vm(4, 2, 3, 3, 3, 8, 128),
            vm(*block),
            vm(4, 8, 3, 8, 128),
            vm(6, 8, 2, 8, 128),
            vm(2, 4, 4, 8, 3, 8, 128),
            vm(4, 2, 3, 3, 2, 128),
            vm(2, 4, 2, 3, 3, 2, 128),
            vm(4, 8, 2, 128),
            vm(4, 8, 2, 128),
            vm(4, CODED, 8, 128),
            vm(4, CODED, 8, 128),
            vm(4, 8, 8, 128),
            vm(4, 8, 8, 128),
            vm(2, 4, 2, 3, 3, 8, 128),
            vm(2, 4, 8, 2, 1, 128),
            vm(2, 4, 8, 2, 1, 128),
            vm(2, 4, 8, 8, 128),
            vm(2, 4, 8, 8, 128),
            vm(2, 8, 128),
            dma((5,)),
            dma((2, 3, 4)),
            dma((2, 3, 4)),
            dma((2, 3, 4)),
            dma((2, 3, 4)),
            dma((len(groups), max(counts))),
            dma((len(groups), max(counts))),
            *[vm(count, 1, 128) for count in counts],
        ],
        compiler_params=pltpu.CompilerParams(collective_id=0, has_side_effects=True),
        name="md_step",
    )(gauge_links, momenta)
    anywhere = pl.BlockSpec(memory_space=pl.ANY)
    in_vmem = pl.BlockSpec(memory_space=pltpu.VMEM)
    new_links, new_momenta, plaquette = pl.pallas_call(
        store_kernel,
        out_shape=(
            jax.ShapeDtypeStruct(block, f32),
            jax.ShapeDtypeStruct(block, f32),
            jax.ShapeDtypeStruct((1, 128), f32),
        ),
        in_specs=[in_vmem] * 3,
        out_specs=(anywhere,) * 3,
        scratch_shapes=[dma((9,))],
        name="store",
    )(
        pltpu.with_memory_space_constraint(wide_links, pltpu.VMEM),
        pltpu.with_memory_space_constraint(momenta_vmem, pltpu.VMEM),
        pltpu.with_memory_space_constraint(plaquette, pltpu.VMEM),
    )
    return new_links, new_momenta, plaquette[0, 0]


def solution(mesh):
    spec = P(None, None, None, None, "gx", "gy", "zt")
    return jax.shard_map(
        per_device,
        mesh=mesh,
        in_specs=(spec, spec),
        out_specs=(spec, spec, P()),
        check_vma=False,
    )
```

```python
import functools

import jax
import jax.numpy as jnp
from jax import lax
from jax.experimental import pallas as pl
from jax.experimental.pallas import tpu as pltpu
from jax.sharding import PartitionSpec as P

LT = 64
AXES = ("gx", "gy", "zt")
PAIRS = ((1, 3), (0, 3), (0, 1), (2, 3), (0, 2), (1, 2))
UPDATES = (3, 0, 2, 1)
MESH_ID = pl.DeviceIdType.MESH

kick_size = 0.25
step_size = 0.2


def mul(a, b):
    return a[0] * b[0] - a[1] * b[1], a[0] * b[1] + a[1] * b[0]


def mul_conj_second(a, b):
    return a[0] * b[0] + a[1] * b[1], a[1] * b[0] - a[0] * b[1]


def mul_conj_first(a, b):
    return a[0] * b[0] + a[1] * b[1], a[0] * b[1] - a[1] * b[0]


def add(a, b):
    return a[0] + b[0], a[1] + b[1]


def total(terms):
    result = terms[0]
    for term in terms[1:]:
        result = add(result, term)
    return result


def conj(a):
    return a[0], -a[1]


def pick(a, index):
    return a[0][index], a[1][index]


TINY = 1e-30
FAR = 1e15
CODED = 11


def project(first, rest):
    square = rest[0] * rest[0]
    for value in rest[1:]:
        square = square + value * value
    near = first >= 0.0
    low = jnp.where(near, 1.0 + first, square)
    factor = jnp.where(near, 1.0, 1.0 - first) / jnp.maximum(low, TINY)
    result = [value * factor for value in rest]
    result[0] = jnp.where(low < TINY, FAR, result[0])
    return result


def lift(values):
    square = values[0] * values[0]
    for value in values[1:]:
        square = square + value * value
    inverse = 1.0 / (1.0 + square)
    double = 2.0 * inverse
    return [(1.0 - square) * inverse] + [value * double for value in values]


def cross(a, b):
    result = []
    for i in range(3):
        j, k = (i + 1) % 3, (i + 2) % 3
        p, q = mul(a[j], b[k]), mul(a[k], b[j])
        result.append((p[0] - q[0], p[1] - q[1]))
    return result


def encode(rows):
    rows = [[pick(row, l) for l in range(3)] for row in rows]
    normal = cross(rows[0], rows[1])
    det = total([mul(rows[2][l], normal[l]) for l in range(3)])
    values = []
    for row in rows[:2]:
        flat = [part for entry in row for part in entry]
        values += project(flat[0], flat[1:])
    return values + project(det[0], [det[1]])


def decode(values):
    rows = []
    for start in (0, 5):
        flat = lift(values[start : start + 5])
        rows.append([(flat[2 * l], flat[2 * l + 1]) for l in range(3)])
    det = lift(values[10:])
    rows.append([mul_conj_second(det, entry) for entry in cross(rows[0], rows[1])])
    return rows


def kernel(
    sizes,
    volume,
    groups,
    links_in,
    mom_in,
    W,
    NM,
    plaq_out,
    V,
    MB,
    HB,
    TB,
    LB,
    YS,
    YR,
    YHS,
    YHR,
    ZS,
    ZR,
    ZHS,
    ZHR,
    ZL,
    YBS,
    YBR,
    ZBS,
    ZBR,
    TR,
    load_sem,
    send_sem,
    frecv,
    brecv,
    trecv,
    lines,
    *slots,
):
    coords = [lax.axis_index(axis) for axis in AXES]

    def device(offset):
        return tuple(
            lax.rem(coords[axis] + (offset[axis] % sizes[axis]), sizes[axis]) for axis in range(3)
        )

    def along(axis, distance):
        return tuple(distance if other == axis else 0 for other in range(3))

    loads = []
    for m in (3, 0, 1, 2):
        copy = pltpu.make_async_copy(links_in.at[m], V.at[m, :, :, :, 0:2], load_sem.at[m])
        copy.start()
        loads.append(copy)
    mom_load = pltpu.make_async_copy(mom_in, MB, load_sem.at[4])
    mom_load.start()

    barrier = pltpu.get_barrier_semaphore()
    partners = 0
    for axis in range(3):
        for k in range(1, sizes[axis]):
            pl.semaphore_signal(barrier, inc=1, device_id=device(along(axis, k)), device_id_type=MESH_ID)
            partners += 1

    shape3 = (1, 8, 128)
    lane = lax.broadcasted_iota(jnp.int32, shape3, 2)
    sub = lax.broadcasted_iota(jnp.int32, shape3, 1)
    t_index = lax.rem(lane, LT)
    half_lanes = lane.shape[-1] // 2
    low = lane < half_lanes
    t_last = t_index == LT - 1
    t_first = t_index == 0
    y_last = sub == 7
    y_first = sub == 0

    def choose(mask, a, b):
        return jnp.where(jnp.broadcast_to(mask, b.shape), jnp.broadcast_to(a, b.shape), b)

    pending = []

    def send(src, dst, offset, recv_sem):
        copy = pltpu.make_async_remote_copy(
            src_ref=src,
            dst_ref=dst,
            send_sem=send_sem.at[0],
            recv_sem=recv_sem,
            device_id=device(offset),
            device_id_type=MESH_ID,
        )
        copy.start()
        pending.append(rows_of(src))
        return copy

    def rows_of(ref):
        size = 1
        for extent in ref.shape:
            size *= extent
        return size // 128

    def wait_rows(count, sem):
        part = lines.at[0:count]
        pltpu.make_async_copy(part, part, sem).wait()

    lane_of = {}
    for d in range(3):
        for m in range(4):
            if d != m:
                lane_of[d, m] = len(lane_of)
    forward = {}
    backward = {}

    def forward_send(stage, d, m, src, dst):
        forward[stage, d, m] = send(
            src, dst, along(d, -1), frecv.at[lane_of[d, m]]
        )

    def send_link(m):
        for d in (2, 0, 1):
            if d == m:
                continue
            if d == 0:
                src, dst = V.at[m, :, :, :, 0], V.at[m, :, :, :, 2]
            elif d == 1:
                for r in range(2):
                    for i in range(3):
                        for x in range(2):
                            YS[m, r, i, :, x : x + 1] = V[m, r, i, :, x, 0:1, :]
                src, dst = YS.at[m], YR.at[0, m]
            else:
                rows = []
                for i in range(3):
                    parts = []
                    for r in range(2):
                        first = V[m, r, i, :, 0]
                        second = V[m, r, i, :, 1]
                        parts.append(choose(low, first, pltpu.roll(second, half_lanes, 2)))
                    rows.append(tuple(parts))
                for c, value in enumerate(encode(rows)):
                    ZS[m, c] = value
                src, dst = ZS.at[m], ZR.at[m]
            forward_send(0, d, m, src, dst)

    def send_half(m):
        for d in (2, 0, 1):
            if d == m:
                continue
            if d == 0:
                src, dst = HB.at[m, :, 0], HB.at[m, :, 2]
            elif d == 1:
                for x in range(2):
                    YHS[m, :, x : x + 1] = HB[m, :, x, 0:1, :]
                src, dst = YHS.at[m], YHR.at[m]
            else:
                first = HB[m, :, 0]
                second = HB[m, :, 1]
                ZHS[m] = choose(low, first, pltpu.roll(second, half_lanes, 2))
                src, dst = ZHS.at[m], ZHR.at[m]
            forward_send(1, d, m, src, dst)

    def send_back(stage, d, m):
        if d == 3:
            return
        if d == 0:
            src, dst = LB.at[stage, 0, m, :, 2], LB.at[stage, 0, m, :, 0]
        elif d == 1:
            for x in range(2):
                YBS[stage, m, :, x] = LB[stage, 1, m, :, x + 1, 7:8, :]
            src, dst = YBS.at[stage, m], YBR.at[stage, m]
        else:
            first = LB[stage, 2, m, :, 1]
            second = LB[stage, 2, m, :, 2]
            ZBS[stage, m] = choose(low, pltpu.roll(first, half_lanes, 2), second)
            src, dst = ZBS.at[stage, m], ZBR.at[stage, m]
        send(src, dst, along(d, 1), brecv.at[m])
        backward[stage, m] = backward.get((stage, m), 0) + rows_of(src)

    def ahead(stage, buf, n, d, x):
        rows = []
        for k in range(3):
            parts = []
            for r in range(2):
                if d == 0:
                    parts.append(buf[n, r, k, :, x + 1])
                    continue
                value = buf[n, r, k, :, x]
                if d == 3:
                    parts.append(
                        choose(t_last, pltpu.roll(value, LT - 1, 2), pltpu.roll(value, 127, 2))
                    )
                elif d == 1:
                    row = YR[stage, n, r, k, :, pl.ds(x, 1)]
                    parts.append(choose(y_last, row, pltpu.roll(value, 7, 1)))
                else:
                    halo = pltpu.roll(ZL[stage, n, r, k], half_lanes * (1 - x), 2)
                    parts.append(choose(low, pltpu.roll(value, half_lanes, 2), halo))
            rows.append(tuple(parts))
        return rows

    def behind(stage, d, m, x):
        if d == 0:
            return LB[stage, 0, m, :, x]
        value = LB[stage, d, m, :, x + 1]
        if d == 1:
            return choose(y_first, YBR[stage, m, :, x], pltpu.roll(value, 1, 1))
        if d == 2:
            halo = pltpu.roll(ZBR[stage, m], half_lanes * x, 2)
            return choose(low, halo, pltpu.roll(value, half_lanes, 2))
        return choose(t_first, pltpu.roll(value, 128 - (LT - 1), 2), pltpu.roll(value, 1, 2))

    def conjugate(T, rows):
        d0, d1, d2, h01, h02, h12 = T
        full = [
            [d0, h01, h02],
            [(-h01[0], h01[1]), d1, h12],
            [(-h02[0], h02[1]), (-h12[0], h12[1]), d2],
        ]
        M = []
        for i in range(3):
            terms = []
            for k in range(3):
                if i == k:
                    terms.append((-(full[i][i] * rows[k][1]), full[i][i] * rows[k][0]))
                else:
                    terms.append(mul(full[i][k], rows[k]))
            M.append(total(terms))
        r0 = 0.0
        r1 = 0.0
        for k in range(3):
            r0 = r0 + (rows[k][0][0] * M[k][1][0] - rows[k][1][0] * M[k][0][0])
            r1 = r1 + (rows[k][0][1] * M[k][1][1] - rows[k][1][1] * M[k][0][1])
        tail = slice(1, 3)
        row0 = total(
            [mul_conj_first(pick(rows[k], 0), (M[k][0][tail], M[k][1][tail])) for k in range(3)]
        )
        r12 = total([mul_conj_first(pick(rows[k], 1), pick(M[k], 2)) for k in range(3)])
        return [r0, r1, row0[0][0], row0[1][0], row0[0][1], row0[1][1], r12[0], r12[1]]

    def pair_task(stage, buf, m, n, x):
        index = PAIRS.index((m, n))
        n_ahead = ahead(stage, buf, n, m, x)
        A = []
        for i in range(3):
            A.append(
                total(
                    [mul((buf[m, 0, i, k, x], buf[m, 1, i, k, x]), n_ahead[k]) for k in range(3)]
                )
            )
        m_ahead = ahead(stage, buf, m, n, x)
        columns = [(buf[n, 0, :, l, x], buf[n, 1, :, l, x]) for l in range(3)]
        Bt = []
        for k in range(3):
            Bt.append(total([mul(pick(m_ahead[l], k), columns[l]) for l in range(3)]))
        loop = []
        for i in range(3):
            loop.append(total([mul_conj_second(pick(A[i], k), Bt[k]) for k in range(3)]))
        i0, i1, i2 = loop[0][1][0], loop[1][1][1], loop[2][1][2]
        mean = (i0 + i1 + i2) * (2.0 / 3.0)
        d0 = 2.0 * i0 - mean
        d1 = 2.0 * i1 - mean
        d2 = -(d0 + d1)

        def off(i, j):
            a = pick(loop[i], j)
            b = pick(loop[j], i)
            return a[0] - b[0], a[1] + b[1]

        h01, h02, h12 = off(0, 1), off(0, 2), off(1, 2)
        values = [d0, d1, h01[0], h01[1], h02[0], h02[1], h12[0], h12[1]]
        for c in range(8):
            TB[index, c, x] = values[c]
        if stage == 1:
            trace = loop[0][0][0] + loop[1][0][1] + loop[2][0][2]
            TR[x] = trace if index == 0 else TR[x] + trace
        T = (d0, d1, d2, h01, h02, h12)
        for link, d in ((m, n), (n, m)):
            rows = [(buf[d, 0, k, :, x], buf[d, 1, k, :, x]) for k in range(3)]
            result = conjugate(T, rows)
            for c in range(8):
                LB[stage, d, link, c, x + 1] = result[c]

    def force(stage, m, x):
        result = None
        for n in range(4):
            if n == m:
                continue
            index = PAIRS.index((min(m, n), max(m, n)))
            term = TB[index, :, x] - behind(stage, n, m, x)
            if result is None:
                result = term if m < n else -term
            else:
                result = result + term if m < n else result - term
        return result

    places = ((1, 0, 0), (1, 1, 1), (0, 0, 1), (1, 0, 1), (0, 0, 2), (1, 0, 2), (0, 1, 2), (1, 1, 2))

    def half_update(m, x):
        F = force(0, m, x)
        for c, (r, i, j) in enumerate(places):
            HB[m, c, x] = MB[m, r, i, j, x] - (0.5 * kick_size) * F[c]

    def cayley(momentum, rows):
        half = [(0.5 * step_size) * value for value in momentum]
        d0, d1 = half[0], half[1]
        d2 = -(d0 + d1)
        h01, h02, h12 = (half[2], half[3]), (half[4], half[5]), (half[6], half[7])
        n01 = h01[0] * h01[0] + h01[1] * h01[1]
        n02 = h02[0] * h02[0] + h02[1] * h02[1]
        n12 = h12[0] * h12[0] + h12[1] * h12[1]
        k00 = d0 * d0 + n01 + n02
        k11 = d1 * d1 + n01 + n12
        k22 = d2 * d2 + n02 + n12
        one_c = 1.0 + 0.5 * (k00 + k11 + k22)
        h01h12 = mul(h01, h12)
        z_imag = h01h12[1] * h02[0] - h01h12[0] * h02[1]
        h = d0 * n12 + d2 * n01 + d1 * n02 - d0 * d1 * d2 - 2.0 * z_imag
        factor = 2.0 / (one_c * one_c + h * h)
        f = (one_c * factor, h * factor)
        s01 = mul_conj_second(h02, h12)
        k01 = (-(d0 + d1) * h01[1] - s01[0], (d0 + d1) * h01[0] - s01[1])
        k02 = (h01h12[0] - (d0 + d2) * h02[1], h01h12[1] + (d0 + d2) * h02[0])
        s12 = mul_conj_first(h01, h02)
        k12 = (-s12[0] - (d1 + d2) * h12[1], (d1 + d2) * h12[0] - s12[1])
        G = [[None] * 3 for _ in range(3)]
        for i, (k, d) in enumerate(((k00, d0), (k11, d1), (k22, d2))):
            G[i][i] = (one_c - k, d)
        for i, j, hh, kk in ((0, 1, h01, k01), (0, 2, h02, k02), (1, 2, h12, k12)):
            G[i][j] = add(hh, kk)
            G[j][i] = (kk[0] - hh[0], hh[1] - kk[1])
        result = []
        for i in range(3):
            E = []
            for k in range(3):
                value = mul(f, G[i][k])
                E.append((value[0] - 1.0, value[1]) if i == k else value)
            result.append(total([mul(E[k], rows[k]) for k in range(3)]))
        return result

    def link_update(m, x):
        rows = [(V[m, 0, k, :, x], V[m, 1, k, :, x]) for k in range(3)]
        new = cayley([HB[m, c, x] for c in range(8)], rows)
        for i in range(3):
            W[m, 0, i, :, x] = new[i][0]
            W[m, 1, i, :, x] = new[i][1]

    def halo_update(d, m):
        if d == 0:
            link_update(m, 2)
            return
        buf, momentum = (YR, YHR) if d == 1 else (ZL, ZHR)
        rows = [(buf[0, m, 0, k], buf[0, m, 1, k]) for k in range(3)]
        new = cayley([momentum[m, c] for c in range(8)], rows)
        for i in range(3):
            buf[1, m, 0, i] = new[i][0]
            buf[1, m, 1, i] = new[i][1]

    def halo_decode(m):
        rows = decode([ZR[m, c] for c in range(CODED)])
        for k in range(3):
            for r in range(2):
                for l in range(3):
                    ZL[0, m, r, k, l] = rows[k][l][r]

    def last_update(m, x):
        F = force(1, m, x)
        v = [HB[m, c, x] - (0.5 * kick_size) * F[c] for c in range(8)]
        zero = jnp.zeros_like(v[0])
        for i in range(3):
            NM[m, 0, i, i, x] = zero
        NM[m, 1, 0, 0, x] = v[0]
        NM[m, 1, 1, 1, x] = v[1]
        NM[m, 1, 2, 2, x] = -(v[0] + v[1])
        for i, j, c in ((0, 1, 2), (0, 2, 4), (1, 2, 6)):
            NM[m, 0, i, j, x] = v[c]
            NM[m, 0, j, i, x] = -v[c]
            NM[m, 1, i, j, x] = v[c + 1]
            NM[m, 1, j, i, x] = v[c + 1]

    def for_x(body):
        for x in range(2):
            body(x)

    def pairs_of(stage, buf):
        for m, n in PAIRS:
            for link, d in ((n, m), (m, n)):
                if d == 3:
                    continue
                with jax.named_scope(f"wf{stage}_d{d}m{link}"):
                    forward[stage, d, link].wait_recv()
                if stage == 1:
                    halo_update(d, link)
                elif d == 2:
                    halo_decode(link)
            for_x(lambda x: pair_task(stage, buf, m, n, x))
            for link, d in ((m, n), (n, m)):
                send_back(stage, d, link)

    def wait_back(stage, m):
        wait_rows(backward[stage, m], brecv.at[m])

    for position, m in enumerate((3, 0, 1, 2)):
        loads[position].wait()
        if position == 0:
            with jax.named_scope("bar"):
                pl.semaphore_wait(barrier, partners)
        send_link(m)
    pairs_of(0, V)
    mom_load.wait()
    for m in UPDATES:
        with jax.named_scope(f"wb0_{m}"):
            wait_back(0, m)
        for_x(lambda x: half_update(m, x))
        send_half(m)
        for_x(lambda x: link_update(m, x))
    pairs_of(1, W)

    def offsets(group):
        result = [()]
        for axis in range(3):
            span = range(sizes[axis]) if axis in group else (0,)
            result = [head + (k,) for head in result for k in span]
        return [item for item in result if any(item)]

    def spread(index, value):
        buf = slots[index]
        position = 0
        for axis in groups[index]:
            position = position * sizes[axis] + coords[axis]
        buf[position] = jnp.sum(value, axis=0, keepdims=True)
        for offset in offsets(groups[index]):
            send(buf.at[position], buf.at[position], offset, trecv.at[index])

    def gathered(index):
        wait_rows(slots[index].shape[0] - 1, trecv.at[index])
        value = slots[index][0]
        for k in range(1, slots[index].shape[0]):
            value = value + slots[index][k]
        return value

    def finish(m):
        with jax.named_scope(f"wb1_{m}"):
            wait_back(1, m)
        for_x(lambda x: last_update(m, x))

    value = TR[0] + TR[1]
    spread(0, value)
    for position, m in enumerate(UPDATES):
        finish(m)
        if position + 1 < len(groups):
            value = gathered(position)
            spread(position + 1, value)
    with jax.named_scope("plaq"):
        lanes = gathered(len(groups) - 1) * (4.0 / (72.0 * volume))
        plaq_out[...] = jnp.broadcast_to(jnp.sum(lanes, axis=1, keepdims=True), (8, 128))
    wait_rows(sum(pending), send_sem.at[0])


def store_kernel(links, mom, plaq, links_out, mom_out, plaq_out, sem):
    copies = [
        pltpu.make_async_copy(links.at[:, :, :, :, 0:2], links_out, sem.at[0]),
        pltpu.make_async_copy(mom, mom_out, sem.at[1]),
        pltpu.make_async_copy(plaq.at[0:1], plaq_out, sem.at[2]),
    ]
    for copy in copies:
        copy.start()
    for copy in copies:
        copy.wait()


def per_device(gauge_links, momenta):
    block = gauge_links.shape
    assert block[-3:] == (2, 8, 2 * LT)
    sizes = tuple(lax.axis_size(axis) for axis in AXES)
    sites = block[-3] * block[-2] * block[-1]
    volume = sites * sizes[0] * sizes[1] * sizes[2]
    f32 = jnp.float32
    vm = lambda *shape: pltpu.VMEM(shape, f32)
    groups = ((0, 1, 2),) if sizes[0] * sizes[1] * sizes[2] <= 32 else ((0,), (1,), (2,))
    counts = []
    for group in groups:
        count = 1
        for axis in group:
            count *= sizes[axis]
        counts.append(count)
    dma = pltpu.SemaphoreType.DMA
    wide_links, momenta_vmem, plaquette = pl.pallas_call(
        functools.partial(kernel, sizes, volume, groups),
        out_shape=(
            vm(4, 2, 3, 3, 3, 8, 128),
            vm(*block),
            vm(8, 128),
        ),
        in_specs=[pl.BlockSpec(memory_space=pl.ANY)] * 2,
        out_specs=(
            pl.BlockSpec(memory_space=pltpu.VMEM),
            pl.BlockSpec(memory_space=pltpu.VMEM),
            pl.BlockSpec(memory_space=pltpu.VMEM),
        ),
        scratch_shapes=[
            vm(4, 2, 3, 3, 3, 8, 128),
            vm(*block),
            vm(4, 8, 3, 8, 128),
            vm(6, 8, 2, 8, 128),
            vm(2, 4, 4, 8, 3, 8, 128),
            vm(4, 2, 3, 3, 2, 128),
            vm(2, 4, 2, 3, 3, 2, 128),
            vm(4, 8, 2, 128),
            vm(4, 8, 2, 128),
            vm(4, CODED, 8, 128),
            vm(4, CODED, 8, 128),
            vm(4, 8, 8, 128),
            vm(4, 8, 8, 128),
            vm(2, 4, 2, 3, 3, 8, 128),
            vm(2, 4, 8, 2, 1, 128),
            vm(2, 4, 8, 2, 1, 128),
            vm(2, 4, 8, 8, 128),
            vm(2, 4, 8, 8, 128),
            vm(2, 8, 128),
            dma((5,)),
            dma((1,)),
            dma((9,)),
            dma((4,)),
            dma((len(groups),)),
            vm(8192, 1, 128),
            *[vm(count, 1, 128) for count in counts],
        ],
        compiler_params=pltpu.CompilerParams(collective_id=0, has_side_effects=True),
        name="md_step",
    )(gauge_links, momenta)
    anywhere = pl.BlockSpec(memory_space=pl.ANY)
    in_vmem = pl.BlockSpec(memory_space=pltpu.VMEM)
    new_links, new_momenta, plaquette = pl.pallas_call(
        store_kernel,
        out_shape=(
            jax.ShapeDtypeStruct(block, f32),
            jax.ShapeDtypeStruct(block, f32),
            jax.ShapeDtypeStruct((1, 128), f32),
        ),
        in_specs=[in_vmem] * 3,
        out_specs=(anywhere,) * 3,
        scratch_shapes=[dma((3,))],
        name="store",
    )(
        pltpu.with_memory_space_constraint(wide_links, pltpu.VMEM),
        pltpu.with_memory_space_constraint(momenta_vmem, pltpu.VMEM),
        pltpu.with_memory_space_constraint(plaquette, pltpu.VMEM),
    )
    return new_links, new_momenta, plaquette[0, 0]


def solution(mesh):
    spec = P(None, None, None, None, "gx", "gy", "zt")
    return jax.shard_map(
        per_device,
        mesh=mesh,
        in_specs=(spec, spec),
        out_specs=(spec, spec, P()),
        check_vma=False,
    )
```

```python
import functools

import jax
import jax.numpy as jnp
from jax import lax
from jax.experimental import pallas as pl
from jax.experimental.pallas import tpu as pltpu
from jax.sharding import PartitionSpec as P

LT = 64
AXES = ("gx", "gy", "zt")
PAIRS = ((1, 3), (0, 3), (0, 1), (2, 3), (0, 2), (1, 2))
ORDERS = (
    ((0, 3), (2, 3), (1, 3), (0, 1), (1, 2), (0, 2)),
    ((0, 3), (1, 3), (2, 3), (0, 2), (0, 1), (1, 2)),
)
EARLY = 1
UPDATES = (3, 0, 2, 1)
MESH_ID = pl.DeviceIdType.MESH

kick_size = 0.25
step_size = 0.2


def mul(a, b):
    return a[0] * b[0] - a[1] * b[1], a[0] * b[1] + a[1] * b[0]


def mul_conj_second(a, b):
    return a[0] * b[0] + a[1] * b[1], a[1] * b[0] - a[0] * b[1]


def mul_conj_first(a, b):
    return a[0] * b[0] + a[1] * b[1], a[0] * b[1] - a[1] * b[0]


def add(a, b):
    return a[0] + b[0], a[1] + b[1]


def total(terms):
    result = terms[0]
    for term in terms[1:]:
        result = add(result, term)
    return result


def conj(a):
    return a[0], -a[1]


def pick(a, index):
    return a[0][index], a[1][index]


TINY = 1e-30
FAR = 1e15
CODED = 11


def project(first, rest):
    square = rest[0] * rest[0]
    for value in rest[1:]:
        square = square + value * value
    near = first >= 0.0
    low = jnp.where(near, 1.0 + first, square)
    factor = jnp.where(near, 1.0, 1.0 - first) / jnp.maximum(low, TINY)
    result = [value * factor for value in rest]
    result[0] = jnp.where(low < TINY, FAR, result[0])
    return result


def lift(values):
    square = values[0] * values[0]
    for value in values[1:]:
        square = square + value * value
    inverse = 1.0 / (1.0 + square)
    double = 2.0 * inverse
    return [(1.0 - square) * inverse] + [value * double for value in values]


def cross(a, b):
    result = []
    for i in range(3):
        j, k = (i + 1) % 3, (i + 2) % 3
        p, q = mul(a[j], b[k]), mul(a[k], b[j])
        result.append((p[0] - q[0], p[1] - q[1]))
    return result


def encode(rows):
    rows = [[pick(row, l) for l in range(3)] for row in rows]
    normal = cross(rows[0], rows[1])
    det = total([mul(rows[2][l], normal[l]) for l in range(3)])
    values = []
    for row in rows[:2]:
        flat = [part for entry in row for part in entry]
        values += project(flat[0], flat[1:])
    return values + project(det[0], [det[1]])


def decode(values):
    rows = []
    for start in (0, 5):
        flat = lift(values[start : start + 5])
        rows.append([(flat[2 * l], flat[2 * l + 1]) for l in range(3)])
    det = lift(values[10:])
    rows.append([mul_conj_second(det, entry) for entry in cross(rows[0], rows[1])])
    return rows


def kernel(
    sizes,
    volume,
    groups,
    links_in,
    mom_in,
    W,
    NM,
    plaq_out,
    V,
    MB,
    HB,
    TB,
    LB,
    YS,
    YR,
    YHS,
    YHR,
    ZS,
    ZR,
    ZHS,
    ZHR,
    ZL,
    YBS,
    YBR,
    ZBS,
    ZBR,
    TR,
    load_sem,
    send_sem,
    frecv,
    brecv,
    trecv,
    lines,
    *slots,
):
    coords = [lax.axis_index(axis) for axis in AXES]

    def device(offset):
        return tuple(
            lax.rem(coords[axis] + (offset[axis] % sizes[axis]), sizes[axis]) for axis in range(3)
        )

    def along(axis, distance):
        return tuple(distance if other == axis else 0 for other in range(3))

    loads = []
    for m in (3, 0, 1, 2):
        copy = pltpu.make_async_copy(links_in.at[m], V.at[m, :, :, :, 0:2], load_sem.at[m])
        copy.start()
        loads.append(copy)
    mom_load = pltpu.make_async_copy(mom_in, MB, load_sem.at[4])
    mom_load.start()

    barrier = pltpu.get_barrier_semaphore()
    partners = 0
    for axis in range(3):
        for k in range(1, sizes[axis]):
            pl.semaphore_signal(barrier, inc=1, device_id=device(along(axis, k)), device_id_type=MESH_ID)
            partners += 1

    shape3 = (1, 8, 128)
    lane = lax.broadcasted_iota(jnp.int32, shape3, 2)
    sub = lax.broadcasted_iota(jnp.int32, shape3, 1)
    t_index = lax.rem(lane, LT)
    half_lanes = lane.shape[-1] // 2
    low = lane < half_lanes
    t_last = t_index == LT - 1
    t_first = t_index == 0
    y_last = sub == 7
    y_first = sub == 0

    def choose(mask, a, b):
        return jnp.where(jnp.broadcast_to(mask, b.shape), jnp.broadcast_to(a, b.shape), b)

    pending = []

    def send(src, dst, offset, recv_sem):
        copy = pltpu.make_async_remote_copy(
            src_ref=src,
            dst_ref=dst,
            send_sem=send_sem.at[0],
            recv_sem=recv_sem,
            device_id=device(offset),
            device_id_type=MESH_ID,
        )
        copy.start()
        pending.append(rows_of(src))
        return copy

    def rows_of(ref):
        size = 1
        for extent in ref.shape:
            size *= extent
        return size // 128

    def wait_rows(count, sem):
        part = lines.at[0:count]
        pltpu.make_async_copy(part, part, sem).wait()

    lane_of = {}
    for d in range(3):
        for m in range(4):
            if d != m:
                lane_of[d, m] = len(lane_of)
    forward = {}
    backward = {}

    def forward_send(stage, d, m, src, dst):
        forward[stage, d, m] = send(
            src, dst, along(d, -1), frecv.at[lane_of[d, m]]
        )

    def pack_y(m):
        for r in range(2):
            for i in range(3):
                for x in range(2):
                    YS[m, r, i, :, x : x + 1] = V[m, r, i, :, x, 0:1, :]

    def pack_z(m):
        rows = []
        for i in range(3):
            parts = []
            for r in range(2):
                first = V[m, r, i, :, 0]
                second = V[m, r, i, :, 1]
                parts.append(choose(low, first, pltpu.roll(second, half_lanes, 2)))
            rows.append(tuple(parts))
        for c, value in enumerate(encode(rows)):
            ZS[m, c] = value

    def send_link(d, m):
        if d == 0:
            src, dst = V.at[m, :, :, :, 0], V.at[m, :, :, :, 2]
        elif d == 1:
            src, dst = YS.at[m], YR.at[0, m]
        else:
            src, dst = ZS.at[m], ZR.at[m]
        forward_send(0, d, m, src, dst)

    def send_half(m):
        for d in (1, 2, 0):
            if d == m:
                continue
            if d == 0:
                src, dst = HB.at[m, :, 0], HB.at[m, :, 2]
            elif d == 1:
                for x in range(2):
                    YHS[m, :, x : x + 1] = HB[m, :, x, 0:1, :]
                src, dst = YHS.at[m], YHR.at[m]
            else:
                first = HB[m, :, 0]
                second = HB[m, :, 1]
                ZHS[m] = choose(low, first, pltpu.roll(second, half_lanes, 2))
                src, dst = ZHS.at[m], ZHR.at[m]
            forward_send(1, d, m, src, dst)

    def send_back(stage, d, m):
        if d == 3:
            return
        if d == 0:
            src, dst = LB.at[stage, 0, m, :, 2], LB.at[stage, 0, m, :, 0]
        elif d == 1:
            for x in range(2):
                YBS[stage, m, :, x] = LB[stage, 1, m, :, x + 1, 7:8, :]
            src, dst = YBS.at[stage, m], YBR.at[stage, m]
        else:
            first = LB[stage, 2, m, :, 1]
            second = LB[stage, 2, m, :, 2]
            ZBS[stage, m] = choose(low, pltpu.roll(first, half_lanes, 2), second)
            src, dst = ZBS.at[stage, m], ZBR.at[stage, m]
        send(src, dst, along(d, 1), brecv.at[m])
        backward[stage, m] = backward.get((stage, m), 0) + rows_of(src)

    def ahead(stage, buf, n, d, x):
        rows = []
        for k in range(3):
            parts = []
            for r in range(2):
                if d == 0:
                    parts.append(buf[n, r, k, :, x + 1])
                    continue
                value = buf[n, r, k, :, x]
                if d == 3:
                    parts.append(
                        choose(t_last, pltpu.roll(value, LT - 1, 2), pltpu.roll(value, 127, 2))
                    )
                elif d == 1:
                    row = YR[stage, n, r, k, :, pl.ds(x, 1)]
                    parts.append(choose(y_last, row, pltpu.roll(value, 7, 1)))
                else:
                    halo = pltpu.roll(ZL[stage, n, r, k], half_lanes * (1 - x), 2)
                    parts.append(choose(low, pltpu.roll(value, half_lanes, 2), halo))
            rows.append(tuple(parts))
        return rows

    def behind(stage, d, m, x):
        if d == 0:
            return LB[stage, 0, m, :, x]
        value = LB[stage, d, m, :, x + 1]
        if d == 1:
            return choose(y_first, YBR[stage, m, :, x], pltpu.roll(value, 1, 1))
        if d == 2:
            halo = pltpu.roll(ZBR[stage, m], half_lanes * x, 2)
            return choose(low, halo, pltpu.roll(value, half_lanes, 2))
        return choose(t_first, pltpu.roll(value, 128 - (LT - 1), 2), pltpu.roll(value, 1, 2))

    def conjugate(T, rows):
        d0, d1, d2, h01, h02, h12 = T
        full = [
            [d0, h01, h02],
            [(-h01[0], h01[1]), d1, h12],
            [(-h02[0], h02[1]), (-h12[0], h12[1]), d2],
        ]
        M = []
        for i in range(3):
            terms = []
            for k in range(3):
                if i == k:
                    terms.append((-(full[i][i] * rows[k][1]), full[i][i] * rows[k][0]))
                else:
                    terms.append(mul(full[i][k], rows[k]))
            M.append(total(terms))
        r0 = 0.0
        r1 = 0.0
        for k in range(3):
            r0 = r0 + (rows[k][0][0] * M[k][1][0] - rows[k][1][0] * M[k][0][0])
            r1 = r1 + (rows[k][0][1] * M[k][1][1] - rows[k][1][1] * M[k][0][1])
        tail = slice(1, 3)
        row0 = total(
            [mul_conj_first(pick(rows[k], 0), (M[k][0][tail], M[k][1][tail])) for k in range(3)]
        )
        r12 = total([mul_conj_first(pick(rows[k], 1), pick(M[k], 2)) for k in range(3)])
        return [r0, r1, row0[0][0], row0[1][0], row0[0][1], row0[1][1], r12[0], r12[1]]

    def loop_task(stage, buf, m, n, x):
        index = PAIRS.index((m, n))
        n_ahead = ahead(stage, buf, n, m, x)
        A = []
        for i in range(3):
            A.append(
                total(
                    [mul((buf[m, 0, i, k, x], buf[m, 1, i, k, x]), n_ahead[k]) for k in range(3)]
                )
            )
        m_ahead = ahead(stage, buf, m, n, x)
        columns = [(buf[n, 0, :, l, x], buf[n, 1, :, l, x]) for l in range(3)]
        Bt = []
        for k in range(3):
            Bt.append(total([mul(pick(m_ahead[l], k), columns[l]) for l in range(3)]))
        loop = []
        for i in range(3):
            loop.append(total([mul_conj_second(pick(A[i], k), Bt[k]) for k in range(3)]))
        i0, i1, i2 = loop[0][1][0], loop[1][1][1], loop[2][1][2]
        mean = (i0 + i1 + i2) * (2.0 / 3.0)
        d0 = 2.0 * i0 - mean
        d1 = 2.0 * i1 - mean
        d2 = -(d0 + d1)

        def off(i, j):
            a = pick(loop[i], j)
            b = pick(loop[j], i)
            return a[0] - b[0], a[1] + b[1]

        h01, h02, h12 = off(0, 1), off(0, 2), off(1, 2)
        values = [d0, d1, h01[0], h01[1], h02[0], h02[1], h12[0], h12[1]]
        for c in range(8):
            TB[index, c, x] = values[c]
        if stage == 1:
            trace = loop[0][0][0] + loop[1][0][1] + loop[2][0][2]
            TR[x] = trace if (m, n) == ORDERS[1][0] else TR[x] + trace
        return values

    def staple_task(stage, buf, m, n, x, values=None):
        if values is None:
            index = PAIRS.index((m, n))
            values = [TB[index, c, x] for c in range(8)]
        d0, d1 = values[0], values[1]
        T = (d0, d1, -(d0 + d1), tuple(values[2:4]), tuple(values[4:6]), tuple(values[6:8]))
        for link, d in ((m, n), (n, m)):
            rows = [(buf[d, 0, k, :, x], buf[d, 1, k, :, x]) for k in range(3)]
            result = conjugate(T, rows)
            for c in range(8):
                LB[stage, d, link, c, x + 1] = result[c]

    def force(stage, m, x):
        result = None
        for n in range(4):
            if n == m:
                continue
            index = PAIRS.index((min(m, n), max(m, n)))
            term = TB[index, :, x] - behind(stage, n, m, x)
            if result is None:
                result = term if m < n else -term
            else:
                result = result + term if m < n else result - term
        return result

    places = ((1, 0, 0), (1, 1, 1), (0, 0, 1), (1, 0, 1), (0, 0, 2), (1, 0, 2), (0, 1, 2), (1, 1, 2))

    def half_update(m, x):
        F = force(0, m, x)
        for c, (r, i, j) in enumerate(places):
            HB[m, c, x] = MB[m, r, i, j, x] - (0.5 * kick_size) * F[c]

    def cayley(momentum, rows):
        half = [(0.5 * step_size) * value for value in momentum]
        d0, d1 = half[0], half[1]
        d2 = -(d0 + d1)
        h01, h02, h12 = (half[2], half[3]), (half[4], half[5]), (half[6], half[7])
        n01 = h01[0] * h01[0] + h01[1] * h01[1]
        n02 = h02[0] * h02[0] + h02[1] * h02[1]
        n12 = h12[0] * h12[0] + h12[1] * h12[1]
        k00 = d0 * d0 + n01 + n02
        k11 = d1 * d1 + n01 + n12
        k22 = d2 * d2 + n02 + n12
        one_c = 1.0 + 0.5 * (k00 + k11 + k22)
        h01h12 = mul(h01, h12)
        z_imag = h01h12[1] * h02[0] - h01h12[0] * h02[1]
        h = d0 * n12 + d2 * n01 + d1 * n02 - d0 * d1 * d2 - 2.0 * z_imag
        factor = 2.0 / (one_c * one_c + h * h)
        f = (one_c * factor, h * factor)
        s01 = mul_conj_second(h02, h12)
        k01 = (-(d0 + d1) * h01[1] - s01[0], (d0 + d1) * h01[0] - s01[1])
        k02 = (h01h12[0] - (d0 + d2) * h02[1], h01h12[1] + (d0 + d2) * h02[0])
        s12 = mul_conj_first(h01, h02)
        k12 = (-s12[0] - (d1 + d2) * h12[1], (d1 + d2) * h12[0] - s12[1])
        G = [[None] * 3 for _ in range(3)]
        for i, (k, d) in enumerate(((k00, d0), (k11, d1), (k22, d2))):
            G[i][i] = (one_c - k, d)
        for i, j, hh, kk in ((0, 1, h01, k01), (0, 2, h02, k02), (1, 2, h12, k12)):
            G[i][j] = add(hh, kk)
            G[j][i] = (kk[0] - hh[0], hh[1] - kk[1])
        result = []
        for i in range(3):
            E = []
            for k in range(3):
                value = mul(f, G[i][k])
                E.append((value[0] - 1.0, value[1]) if i == k else value)
            result.append(total([mul(E[k], rows[k]) for k in range(3)]))
        return result

    def link_update(m, x):
        rows = [(V[m, 0, k, :, x], V[m, 1, k, :, x]) for k in range(3)]
        new = cayley([HB[m, c, x] for c in range(8)], rows)
        for i in range(3):
            W[m, 0, i, :, x] = new[i][0]
            W[m, 1, i, :, x] = new[i][1]

    def halo_update(d, m):
        if d == 0:
            link_update(m, 2)
            return
        buf, momentum = (YR, YHR) if d == 1 else (ZL, ZHR)
        rows = [(buf[0, m, 0, k], buf[0, m, 1, k]) for k in range(3)]
        new = cayley([momentum[m, c] for c in range(8)], rows)
        for i in range(3):
            buf[1, m, 0, i] = new[i][0]
            buf[1, m, 1, i] = new[i][1]

    def halo_decode(m):
        rows = decode([ZR[m, c] for c in range(CODED)])
        for k in range(3):
            for r in range(2):
                for l in range(3):
                    ZL[0, m, r, k, l] = rows[k][l][r]

    def last_update(m, x):
        F = force(1, m, x)
        v = [HB[m, c, x] - (0.5 * kick_size) * F[c] for c in range(8)]
        zero = jnp.zeros_like(v[0])
        for i in range(3):
            NM[m, 0, i, i, x] = zero
        NM[m, 1, 0, 0, x] = v[0]
        NM[m, 1, 1, 1, x] = v[1]
        NM[m, 1, 2, 2, x] = -(v[0] + v[1])
        for i, j, c in ((0, 1, 2), (0, 2, 4), (1, 2, 6)):
            NM[m, 0, i, j, x] = v[c]
            NM[m, 0, j, i, x] = -v[c]
            NM[m, 1, i, j, x] = v[c + 1]
            NM[m, 1, j, i, x] = v[c + 1]

    def for_x(body):
        for x in range(2):
            body(x)

    def wait_ahead(stage, m, n):
        for link, d in ((n, m), (m, n)):
            if d == 3:
                continue
            with jax.named_scope(f"wf{stage}_d{d}m{link}"):
                forward[stage, d, link].wait_recv()
            if stage == 1:
                halo_update(d, link)
            elif d == 2:
                halo_decode(link)

    def send_pair(stage, m, n):
        for link, d in ((m, n), (n, m)):
            send_back(stage, d, link)

    def whole_pair(stage, buf, m, n):
        wait_ahead(stage, m, n)
        for_x(lambda x: staple_task(stage, buf, m, n, x, loop_task(stage, buf, m, n, x)))
        send_pair(stage, m, n)

    def wait_back(stage, m):
        wait_rows(backward[stage, m], brecv.at[m])

    for copy in loads:
        copy.wait()
    for m in (3, 0, 2):
        pack_y(m)
    with jax.named_scope("bar"):
        pl.semaphore_wait(barrier, partners)
    for d, m in ((1, 3), (0, 3), (1, 0), (1, 2)):
        send_link(d, m)
    pack_z(3)
    for d, m in ((2, 3), (0, 1), (0, 2)):
        send_link(d, m)
    for m in (1, 0):
        pack_z(m)
        send_link(2, m)
    for m, n in ORDERS[0]:
        whole_pair(0, V, m, n)
    mom_load.wait()
    for m in UPDATES:
        with jax.named_scope(f"wb0_{m}"):
            wait_back(0, m)
        for_x(lambda x: half_update(m, x))
        send_half(m)
        if m == UPDATES[2]:
            for_x(lambda x: link_update(UPDATES[0], x))
    for m in UPDATES[1:]:
        for_x(lambda x: link_update(m, x))
    for m, n in ORDERS[1][:EARLY]:
        whole_pair(1, W, m, n)
    for m, n in ORDERS[1][EARLY:]:
        wait_ahead(1, m, n)
        for_x(lambda x: loop_task(1, W, m, n, x))

    def offsets(group):
        result = [()]
        for axis in range(3):
            span = range(sizes[axis]) if axis in group else (0,)
            result = [head + (k,) for head in result for k in span]
        return [item for item in result if any(item)]

    def spread(index, value):
        buf = slots[index]
        position = 0
        for axis in groups[index]:
            position = position * sizes[axis] + coords[axis]
        buf[position] = jnp.sum(value, axis=0, keepdims=True)
        for offset in offsets(groups[index]):
            send(buf.at[position], buf.at[position], offset, trecv.at[index])

    def gathered(index):
        wait_rows(slots[index].shape[0] - 1, trecv.at[index])
        value = slots[index][0]
        for k in range(1, slots[index].shape[0]):
            value = value + slots[index][k]
        return value

    def finish(m):
        with jax.named_scope(f"wb1_{m}"):
            wait_back(1, m)
        for_x(lambda x: last_update(m, x))

    value = TR[0] + TR[1]
    spread(0, value)
    for m, n in ORDERS[1][EARLY:]:
        for_x(lambda x: staple_task(1, W, m, n, x))
        send_pair(1, m, n)
    for position, m in enumerate(UPDATES):
        finish(m)
        if position + 1 < len(groups):
            value = gathered(position)
            spread(position + 1, value)
    with jax.named_scope("plaq"):
        lanes = gathered(len(groups) - 1) * (4.0 / (72.0 * volume))
        plaq_out[...] = jnp.broadcast_to(jnp.sum(lanes, axis=1, keepdims=True), (8, 128))
    wait_rows(sum(pending), send_sem.at[0])


def store_kernel(links, mom, plaq, links_out, mom_out, plaq_out, sem):
    copies = [
        pltpu.make_async_copy(links.at[:, :, :, :, 0:2], links_out, sem.at[0]),
        pltpu.make_async_copy(mom, mom_out, sem.at[1]),
        pltpu.make_async_copy(plaq.at[0:1], plaq_out, sem.at[2]),
    ]
    for copy in copies:
        copy.start()
    for copy in copies:
        copy.wait()


def per_device(gauge_links, momenta):
    block = gauge_links.shape
    assert block[-3:] == (2, 8, 2 * LT)
    sizes = tuple(lax.axis_size(axis) for axis in AXES)
    sites = block[-3] * block[-2] * block[-1]
    volume = sites * sizes[0] * sizes[1] * sizes[2]
    f32 = jnp.float32
    vm = lambda *shape: pltpu.VMEM(shape, f32)
    groups = ((0, 1, 2),) if sizes[0] * sizes[1] * sizes[2] <= 32 else ((0,), (1,), (2,))
    counts = []
    for group in groups:
        count = 1
        for axis in group:
            count *= sizes[axis]
        counts.append(count)
    dma = pltpu.SemaphoreType.DMA
    wide_links, momenta_vmem, plaquette = pl.pallas_call(
        functools.partial(kernel, sizes, volume, groups),
        out_shape=(
            vm(4, 2, 3, 3, 3, 8, 128),
            vm(*block),
            vm(8, 128),
        ),
        in_specs=[pl.BlockSpec(memory_space=pl.ANY)] * 2,
        out_specs=(
            pl.BlockSpec(memory_space=pltpu.VMEM),
            pl.BlockSpec(memory_space=pltpu.VMEM),
            pl.BlockSpec(memory_space=pltpu.VMEM),
        ),
        scratch_shapes=[
            vm(4, 2, 3, 3, 3, 8, 128),
            vm(*block),
            vm(4, 8, 3, 8, 128),
            vm(6, 8, 2, 8, 128),
            vm(2, 4, 4, 8, 3, 8, 128),
            vm(4, 2, 3, 3, 2, 128),
            vm(2, 4, 2, 3, 3, 2, 128),
            vm(4, 8, 2, 128),
            vm(4, 8, 2, 128),
            vm(4, CODED, 8, 128),
            vm(4, CODED, 8, 128),
            vm(4, 8, 8, 128),
            vm(4, 8, 8, 128),
            vm(2, 4, 2, 3, 3, 8, 128),
            vm(2, 4, 8, 2, 1, 128),
            vm(2, 4, 8, 2, 1, 128),
            vm(2, 4, 8, 8, 128),
            vm(2, 4, 8, 8, 128),
            vm(2, 8, 128),
            dma((5,)),
            dma((1,)),
            dma((9,)),
            dma((4,)),
            dma((len(groups),)),
            vm(8192, 1, 128),
            *[vm(count, 1, 128) for count in counts],
        ],
        compiler_params=pltpu.CompilerParams(collective_id=0, has_side_effects=True),
        name="md_step",
    )(gauge_links, momenta)
    anywhere = pl.BlockSpec(memory_space=pl.ANY)
    in_vmem = pl.BlockSpec(memory_space=pltpu.VMEM)
    new_links, new_momenta, plaquette = pl.pallas_call(
        store_kernel,
        out_shape=(
            jax.ShapeDtypeStruct(block, f32),
            jax.ShapeDtypeStruct(block, f32),
            jax.ShapeDtypeStruct((1, 128), f32),
        ),
        in_specs=[in_vmem] * 3,
        out_specs=(anywhere,) * 3,
        scratch_shapes=[dma((3,))],
        name="store",
    )(
        pltpu.with_memory_space_constraint(wide_links, pltpu.VMEM),
        pltpu.with_memory_space_constraint(momenta_vmem, pltpu.VMEM),
        pltpu.with_memory_space_constraint(plaquette, pltpu.VMEM),
    )
    return new_links, new_momenta, plaquette[0, 0]


def solution(mesh):
    spec = P(None, None, None, None, "gx", "gy", "zt")
    return jax.shard_map(
        per_device,
        mesh=mesh,
        in_specs=(spec, spec),
        out_specs=(spec, spec, P()),
        check_vma=False,
    )
```

```python
import functools

import jax
import jax.numpy as jnp
from jax import lax
from jax.experimental import pallas as pl
from jax.experimental.pallas import tpu as pltpu
from jax.sharding import PartitionSpec as P

LT = 64
AXES = ("gx", "gy", "zt")
PAIRS = ((1, 3), (0, 3), (0, 1), (2, 3), (0, 2), (1, 2))
ORDERS = (
    ((1, 3), (0, 3), (0, 1), (2, 3), (1, 2), (0, 2)),
    ((1, 3), (2, 3), (0, 3), (0, 2), (0, 1), (1, 2)),
)
EARLY = 2
EDGE = (3, 0, 2)
LOADS = (3, 1, 0, 2)
Z_LINKS = (3, 0, 1)
SENDS = ((0, 3), (2, 3), (1, 3), (2, 1), (0, 1), (2, 0), (1, 0), (0, 2), (1, 2))
UPDATES = (3, 0, 1, 2)
MESH_ID = pl.DeviceIdType.MESH

kick_size = 0.25
step_size = 0.2


def mul(a, b):
    return a[0] * b[0] - a[1] * b[1], a[0] * b[1] + a[1] * b[0]


def mul_conj_second(a, b):
    return a[0] * b[0] + a[1] * b[1], a[1] * b[0] - a[0] * b[1]


def mul_conj_first(a, b):
    return a[0] * b[0] + a[1] * b[1], a[0] * b[1] - a[1] * b[0]


def add(a, b):
    return a[0] + b[0], a[1] + b[1]


def total(terms):
    result = terms[0]
    for term in terms[1:]:
        result = add(result, term)
    return result


def conj(a):
    return a[0], -a[1]


def pick(a, index):
    return a[0][index], a[1][index]


TINY = 1e-30
FAR = 1e15
CODED = 11
LANES = 15
CODED_X = (1, 2)


def project(first, rest):
    square = rest[0] * rest[0]
    for value in rest[1:]:
        square = square + value * value
    near = first >= 0.0
    low = jnp.where(near, 1.0 + first, square)
    factor = jnp.where(near, 1.0, 1.0 - first) / jnp.maximum(low, TINY)
    result = [value * factor for value in rest]
    result[0] = jnp.where(low < TINY, FAR, result[0])
    return result


def lift(values):
    square = values[0] * values[0]
    for value in values[1:]:
        square = square + value * value
    inverse = 1.0 / (1.0 + square)
    double = 2.0 * inverse
    return [(1.0 - square) * inverse] + [value * double for value in values]


def cross(a, b):
    result = []
    for i in range(3):
        j, k = (i + 1) % 3, (i + 2) % 3
        p, q = mul(a[j], b[k]), mul(a[k], b[j])
        result.append((p[0] - q[0], p[1] - q[1]))
    return result


def encode(rows):
    rows = [[pick(row, l) for l in range(3)] for row in rows]
    normal = cross(rows[0], rows[1])
    det = total([mul(rows[2][l], normal[l]) for l in range(3)])
    values = []
    for row in rows[:2]:
        flat = [part for entry in row for part in entry]
        values += project(flat[0], flat[1:])
    return values + project(det[0], [det[1]])


def decode(values):
    rows = []
    for start in (0, 5):
        flat = lift(values[start : start + 5])
        rows.append([(flat[2 * l], flat[2 * l + 1]) for l in range(3)])
    det = lift(values[10:])
    rows.append([mul_conj_second(det, entry) for entry in cross(rows[0], rows[1])])
    return rows


def kernel(
    sizes,
    volume,
    groups,
    links_in,
    mom_in,
    W,
    NM,
    plaq_out,
    V,
    MB,
    HB,
    TB,
    LB,
    XS,
    XR,
    EM,
    EN,
    YHS,
    EX,
    EP,
    EH,
    EK,
    ET,
    ZS,
    ZR,
    ZHS,
    ZHR,
    ZL,
    YBR,
    ZBS,
    ZBR,
    TR,
    load_sem,
    send_sem,
    frecv,
    brecv,
    trecv,
    lines,
    *slots,
):
    coords = [lax.axis_index(axis) for axis in AXES]

    def device(offset):
        return tuple(
            lax.rem(coords[axis] + (offset[axis] % sizes[axis]), sizes[axis]) for axis in range(3)
        )

    def along(axis, distance):
        return tuple(distance if other == axis else 0 for other in range(3))

    loads = []
    for m in LOADS:
        copy = pltpu.make_async_copy(links_in.at[m], V.at[m, :, :, :, 0:2], load_sem.at[m])
        copy.start()
        loads.append(copy)
    mom_load = pltpu.make_async_copy(mom_in, MB, load_sem.at[4])
    mom_load.start()

    barrier = pltpu.get_barrier_semaphore()
    partners = 0
    for axis in range(3):
        for k in range(1, sizes[axis]):
            pl.semaphore_signal(barrier, inc=1, device_id=device(along(axis, k)), device_id_type=MESH_ID)
            partners += 1

    shape3 = (1, 8, 128)
    lane = lax.broadcasted_iota(jnp.int32, shape3, 2)
    sub = lax.broadcasted_iota(jnp.int32, shape3, 1)
    sub2 = lax.broadcasted_iota(jnp.int32, shape3[1:], 0)
    t_index = lax.rem(lane, LT)
    half_lanes = lane.shape[-1] // 2
    low = lane < half_lanes
    low_row = lax.broadcasted_iota(jnp.int32, (1, 1, 128), 2) < half_lanes
    t_last = t_index == LT - 1
    t_first = t_index == 0
    y_first = sub == 0

    def choose(mask, a, b):
        return jnp.where(jnp.broadcast_to(mask, b.shape), jnp.broadcast_to(a, b.shape), b)

    pending = []

    def send(src, dst, offset, recv_sem):
        copy = pltpu.make_async_remote_copy(
            src_ref=src,
            dst_ref=dst,
            send_sem=send_sem.at[0],
            recv_sem=recv_sem,
            device_id=device(offset),
            device_id_type=MESH_ID,
        )
        copy.start()
        pending.append(rows_of(src))
        return copy

    def rows_of(ref):
        size = 1
        for extent in ref.shape:
            size *= extent
        return size // 128

    def wait_rows(count, sem):
        part = lines.at[0:count]
        pltpu.make_async_copy(part, part, sem).wait()

    lane_of = {}
    for d in range(3):
        for m in range(4):
            if d != m:
                lane_of[0, d, m] = len(set(lane_of.values()))
                lane_of[1, d, m] = lane_of[0, d, m] + (d > 0)
    forward = {}
    backward = {}

    def forward_send(stage, d, m, src, dst):
        send(src, dst, along(d, -1), frecv.at[lane_of[stage, d, m]])
        forward[stage, d, m] = forward.get((stage, d, m), 0) + rows_of(src)

    def wait_forward(stage, d, m):
        with jax.named_scope(f"wf{stage}_d{d}m{m}"):
            wait_rows(forward[stage, d, m], frecv.at[lane_of[stage, d, m]])

    def edge_row(m, x):
        row = 2 * EDGE.index(m) + x
        return slice(row, row + 1)

    def store_code(buf, m, rows):
        for c, value in enumerate(encode(rows)):
            buf[m, c] = value

    def pack_z(m):
        rows = []
        for i in range(3):
            parts = []
            for r in range(2):
                first = V[m, r, i, :, 0]
                second = V[m, r, i, :, 1]
                parts.append(choose(low, first, pltpu.roll(second, half_lanes, 2)))
            rows.append(tuple(parts))
        store_code(ZS, m, rows)

    def send_link(d, m):
        if d == 1:
            for x in range(2):
                forward_send(0, 1, m, V.at[m, :, :, :, x, 0:1], EH.at[:, :, :, edge_row(m, x)])
        elif d == 2:
            pack_z(m)
            forward_send(0, 2, m, ZS.at[m], ZR.at[m])
        elif m in CODED_X:
            store_code(XS, m, [(V[m, 0, k, :, 0], V[m, 1, k, :, 0]) for k in range(3)])
            forward_send(0, 0, m, XS.at[m], XR.at[m])
        else:
            forward_send(0, 0, m, V.at[m, :, :, :, 0], V.at[m, :, :, :, 2])

    def share(d, m):
        return (0.5 * kick_size) if m < d else (-0.5 * kick_size)

    def add_x(m):
        if m != 0:
            wait_back(0, m, (0,))
            HB[m, :, 0] = HB[m, :, 0] + share(0, m) * LB[0, 0, m, :, 0]

    def add_y(m):
        if m != 1:
            if m == 2:
                wait_back(0, m, (1,))
            for x in range(2):
                HB[m, :, x, 0:1] = HB[m, :, x, 0:1] + share(1, m) * YBR[0, m, :, x]

    def add_z(m):
        if m == 2:
            return
        wait_back(0, m, (2,))
        for x in range(2):
            halo = pltpu.roll(ZBR[0, m], half_lanes * x, 2) if x else ZBR[0, m]
            HB[m, :, x] = HB[m, :, x] + choose(low, share(2, m) * halo, jnp.zeros_like(halo))

    def send_half_z(m):
        ZHS[m] = choose(low, HB[m, :, 0], pltpu.roll(HB[m, :, 1], half_lanes, 2))
        if m != 1:
            wait_back(0, m, (1,))
            first, second = YBR[0, m, :, 0], YBR[0, m, :, 1]
            row = choose(low_row, first, pltpu.roll(second, half_lanes, 2))
            ZHS[m, :, 0:1] = ZHS[m, :, 0:1] + share(1, m) * row
        forward_send(1, 2, m, ZHS.at[m], ZHR.at[m])

    def send_half_y(m):
        if m != 1:
            for x in range(2):
                YHS[m, :, x] = HB[m, :, x, 0:1]
                forward_send(1, 1, m, YHS.at[m, :, x], EK.at[:, edge_row(m, x)])

    def send_half_x(m):
        if m != 0:
            forward_send(1, 0, m, HB.at[m, :, 0], HB.at[m, :, 2])

    def send_back(stage, d, m):
        if d == 3:
            return
        if d == 0:
            copies = [(LB.at[stage, 0, m, :, 2], LB.at[stage, 0, m, :, 0])]
        elif d == 1:
            copies = [(ET.at[stage, 1, :, edge_row(m, x)], YBR.at[stage, m, :, x]) for x in range(2)]
        else:
            first = LB[stage, 2, m, :, 1]
            second = LB[stage, 2, m, :, 2]
            ZBS[stage, m] = choose(low, pltpu.roll(first, half_lanes, 2), second)
            copies = [(ZBS.at[stage, m], ZBR.at[stage, m])]
        for src, dst in copies:
            send(src, dst, along(d, 1), brecv.at[lane_of[stage, d, m]])
            backward[stage, d, m] = backward.get((stage, d, m), 0) + rows_of(src)

    def ahead(stage, buf, n, d, x):
        rows = []
        for k in range(3):
            parts = []
            for r in range(2):
                if d == 0:
                    parts.append(buf[n, r, k, :, x + 1])
                    continue
                value = buf[n, r, k, :, x]
                if d == 3:
                    parts.append(
                        choose(t_last, pltpu.roll(value, LT - 1, 2), pltpu.roll(value, 127, 2))
                    )
                elif d == 1:
                    parts.append(pltpu.roll(value, 7, 1))
                else:
                    halo = pltpu.roll(ZL[stage, n, r, k], half_lanes * (1 - x), 2)
                    parts.append(choose(low, pltpu.roll(value, half_lanes, 2), halo))
            rows.append(tuple(parts))
        return rows

    def behind(stage, d, m, x):
        if d == 0:
            return LB[stage, 0, m, :, x]
        value = LB[stage, d, m, :, x + 1]
        if d == 1:
            return choose(y_first, YBR[stage, m, :, x], pltpu.roll(value, 1, 1))
        if d == 2:
            halo = pltpu.roll(ZBR[stage, m], half_lanes * x, 2)
            return choose(low, halo, pltpu.roll(value, half_lanes, 2))
        return choose(t_first, pltpu.roll(value, 128 - (LT - 1), 2), pltpu.roll(value, 1, 2))

    def conjugate(T, rows):
        d0, d1, d2, h01, h02, h12 = T
        full = [
            [d0, h01, h02],
            [(-h01[0], h01[1]), d1, h12],
            [(-h02[0], h02[1]), (-h12[0], h12[1]), d2],
        ]
        M = []
        for i in range(3):
            terms = []
            for k in range(3):
                if i == k:
                    terms.append((-(full[i][i] * rows[k][1]), full[i][i] * rows[k][0]))
                else:
                    terms.append(mul(full[i][k], rows[k]))
            M.append(total(terms))
        r0 = 0.0
        r1 = 0.0
        for k in range(3):
            r0 = r0 + (rows[k][0][0] * M[k][1][0] - rows[k][1][0] * M[k][0][0])
            r1 = r1 + (rows[k][0][1] * M[k][1][1] - rows[k][1][1] * M[k][0][1])
        tail = slice(1, 3)
        row0 = total(
            [mul_conj_first(pick(rows[k], 0), (M[k][0][tail], M[k][1][tail])) for k in range(3)]
        )
        r12 = total([mul_conj_first(pick(rows[k], 1), pick(M[k], 2)) for k in range(3)])
        return [r0, r1, row0[0][0], row0[1][0], row0[0][1], row0[1][1], r12[0], r12[1]]

    def close(A, m_ahead, columns):
        Bt = []
        for k in range(3):
            Bt.append(total([mul(pick(m_ahead[l], k), columns[l]) for l in range(3)]))
        loop = []
        for i in range(3):
            loop.append(total([mul_conj_second(pick(A[i], k), Bt[k]) for k in range(3)]))
        i0, i1, i2 = loop[0][1][0], loop[1][1][1], loop[2][1][2]
        mean = (i0 + i1 + i2) * (2.0 / 3.0)
        d0 = 2.0 * i0 - mean
        d1 = 2.0 * i1 - mean

        def off(i, j):
            a = pick(loop[i], j)
            b = pick(loop[j], i)
            return a[0] - b[0], a[1] + b[1]

        h01, h02, h12 = off(0, 1), off(0, 2), off(1, 2)
        values = [d0, d1, h01[0], h01[1], h02[0], h02[1], h12[0], h12[1]]
        return values, loop[0][0][0] + loop[1][0][1] + loop[2][0][2]

    def loop_task(stage, buf, m, n, x):
        index = PAIRS.index((m, n))
        n_ahead = ahead(stage, buf, n, m, x)
        A = []
        for i in range(3):
            A.append(
                total(
                    [mul((buf[m, 0, i, k, x], buf[m, 1, i, k, x]), n_ahead[k]) for k in range(3)]
                )
            )
        m_ahead = ahead(stage, buf, m, n, x)
        columns = [(buf[n, 0, :, l, x], buf[n, 1, :, l, x]) for l in range(3)]
        values, trace = close(A, m_ahead, columns)
        for c in range(8):
            TB[index, c, x] = values[c]
        if stage == 1:
            if 1 in (m, n):
                trace = jnp.where(sub2 == 7, 0.0, trace)
            TR[x] = trace if (m, n) == ORDERS[1][0] else TR[x] + trace
        return values

    def algebra(values):
        d0, d1 = values[0], values[1]
        return (d0, d1, -(d0 + d1), tuple(values[2:4]), tuple(values[4:6]), tuple(values[6:8]))

    def edge_rows(stage, buf):
        for r in range(2):
            for k in range(3):
                for s, m in enumerate(EDGE):
                    for x in range(2):
                        row = slice(2 * s + x, 2 * s + x + 1)
                        EM[r, k, :, row] = buf[m, r, k, :, x, 7:8, :]
                        EN[r, k, :, row] = buf[1, r, k, :, x, 7:8, :]
                for x in range(2):
                    EX[r, k, :, 2 + x : 3 + x] = buf[1, r, k, :, x + 1, 7:8, :]
                    EX[r, k, :, 4 + x : 5 + x] = ZL[stage, 1, r, k, :, 7:8]
        n_ahead = []
        for k in range(3):
            parts = []
            for r in range(2):
                own, other = EN[r, k], EX[r, k]
                t_ahead = choose(t_last, pltpu.roll(own, LT - 1, 2), pltpu.roll(own, 127, 2))
                halo = choose(sub == 4, pltpu.roll(other, half_lanes, 2), other)
                z_ahead = choose(low, pltpu.roll(own, half_lanes, 2), halo)
                parts.append(choose(sub < 2, t_ahead, choose(sub < 4, other, z_ahead)))
            n_ahead.append(tuple(parts))
        for i in range(3):
            value = total([mul((EM[0, i, k], EM[1, i, k]), n_ahead[k]) for k in range(3)])
            EP[0, i], EP[1, i] = value

    def edge_loops(stage):
        for m in EDGE:
            wait_forward(stage, 1, m)
        m_ahead = [(EH[0, k], EH[1, k]) for k in range(3)]
        if stage == 1:
            scale = jnp.where((sub2 < 2) | (sub2 > 3), share(1, 3), share(1, 0))
            m_ahead = cayley([EK[c] + scale * ET[0, 1, c] for c in range(8)], m_ahead)
        A = [(EP[0, i], EP[1, i]) for i in range(3)]
        columns = [(EN[0, :, l], EN[1, :, l]) for l in range(3)]
        values, trace = close(A, m_ahead, columns)
        if stage == 1:
            TR[0] = TR[0] + jnp.where(sub2 < 6, trace, 0.0)
        sign = jnp.where((sub2 < 2) | (sub2 > 3), -1.0, 1.0)
        for c in range(8):
            ET[stage, 0, c] = sign * values[c]

    def edge_staples(stage):
        T = algebra([ET[stage, 0, c] for c in range(8)])
        for slot, buf in ((1, EN), (2, EM)):
            result = conjugate(T, [(buf[0, k], buf[1, k]) for k in range(3)])
            for c in range(8):
                ET[stage, slot, c] = result[c]
        for m in EDGE:
            send_back(stage, 1, m)

    def edge_merge(stage):
        for m in EDGE:
            index = PAIRS.index((min(m, 1), max(m, 1)))
            for x in range(2):
                TB[index, :, x, 7:8] = ET[stage, 0, :, edge_row(m, x)]
                LB[stage, m, 1, :, x + 1, 7:8] = ET[stage, 2, :, edge_row(m, x)]
        for d in (2, 0):
            send_back(stage, d, 1)

    def staple_task(stage, buf, m, n, x, values=None):
        if values is None:
            index = PAIRS.index((m, n))
            values = [TB[index, c, x] for c in range(8)]
        T = algebra(values)
        for link, d in ((m, n), (n, m)):
            rows = [(buf[d, 0, k, :, x], buf[d, 1, k, :, x]) for k in range(3)]
            result = conjugate(T, rows)
            for c in range(8):
                LB[stage, d, link, c, x + 1] = result[c]

    def force(stage, m, x, directions=(0, 1, 2, 3)):
        result = None
        for n in range(4):
            if n == m:
                continue
            index = PAIRS.index((min(m, n), max(m, n)))
            term = TB[index, :, x]
            if n in directions:
                term = term - behind(stage, n, m, x)
            if result is None:
                result = term if m < n else -term
            else:
                result = result + term if m < n else result - term
        return result

    places = ((1, 0, 0), (1, 1, 1), (0, 0, 1), (1, 0, 1), (0, 0, 2), (1, 0, 2), (0, 1, 2), (1, 1, 2))

    def half_update(m, x):
        F = None
        for n in range(4):
            if n == m:
                continue
            term = TB[PAIRS.index((min(m, n), max(m, n))), :, x]
            if n == 0 and x:
                term = term - LB[0, 0, m, :, x]
            elif n != 0:
                value = LB[0, n, m, :, x + 1]
                if n == 1:
                    back = choose(y_first, jnp.zeros_like(value), pltpu.roll(value, 1, 1))
                elif n == 2:
                    back = choose(low, jnp.zeros_like(value), pltpu.roll(value, half_lanes, 2))
                else:
                    back = behind(0, 3, m, x)
                term = term - back
            term = term if m < n else -term
            F = term if F is None else F + term
        for c, (r, i, j) in enumerate(places):
            HB[m, c, x] = MB[m, r, i, j, x] - (0.5 * kick_size) * F[c]

    def cayley(momentum, rows):
        half = [(0.5 * step_size) * value for value in momentum]
        d0, d1 = half[0], half[1]
        d2 = -(d0 + d1)
        h01, h02, h12 = (half[2], half[3]), (half[4], half[5]), (half[6], half[7])
        n01 = h01[0] * h01[0] + h01[1] * h01[1]
        n02 = h02[0] * h02[0] + h02[1] * h02[1]
        n12 = h12[0] * h12[0] + h12[1] * h12[1]
        k00 = d0 * d0 + n01 + n02
        k11 = d1 * d1 + n01 + n12
        k22 = d2 * d2 + n02 + n12
        one_c = 1.0 + 0.5 * (k00 + k11 + k22)
        h01h12 = mul(h01, h12)
        z_imag = h01h12[1] * h02[0] - h01h12[0] * h02[1]
        h = d0 * n12 + d2 * n01 + d1 * n02 - d0 * d1 * d2 - 2.0 * z_imag
        factor = 2.0 / (one_c * one_c + h * h)
        f = (one_c * factor, h * factor)
        s01 = mul_conj_second(h02, h12)
        k01 = (-(d0 + d1) * h01[1] - s01[0], (d0 + d1) * h01[0] - s01[1])
        k02 = (h01h12[0] - (d0 + d2) * h02[1], h01h12[1] + (d0 + d2) * h02[0])
        s12 = mul_conj_first(h01, h02)
        k12 = (-s12[0] - (d1 + d2) * h12[1], (d1 + d2) * h12[0] - s12[1])
        G = [[None] * 3 for _ in range(3)]
        for i, (k, d) in enumerate(((k00, d0), (k11, d1), (k22, d2))):
            G[i][i] = (one_c - k, d)
        for i, j, hh, kk in ((0, 1, h01, k01), (0, 2, h02, k02), (1, 2, h12, k12)):
            G[i][j] = add(hh, kk)
            G[j][i] = (kk[0] - hh[0], hh[1] - kk[1])
        result = []
        for i in range(3):
            E = []
            for k in range(3):
                value = mul(f, G[i][k])
                E.append((value[0] - 1.0, value[1]) if i == k else value)
            result.append(total([mul(E[k], rows[k]) for k in range(3)]))
        return result

    def link_update(m, x):
        rows = [(V[m, 0, k, :, x], V[m, 1, k, :, x]) for k in range(3)]
        new = cayley([HB[m, c, x] for c in range(8)], rows)
        for i in range(3):
            W[m, 0, i, :, x] = new[i][0]
            W[m, 1, i, :, x] = new[i][1]

    def halo_update(d, m):
        if d == 0:
            link_update(m, 2)
            return
        rows = [(ZL[0, m, 0, k], ZL[0, m, 1, k]) for k in range(3)]
        scale = share(2, m)
        new = cayley([ZHR[m, c] + scale * ZBS[0, m, c] for c in range(8)], rows)
        for i in range(3):
            ZL[1, m, 0, i] = new[i][0]
            ZL[1, m, 1, i] = new[i][1]

    def halo_decode(m):
        rows = decode([ZR[m, c] for c in range(CODED)])
        for k in range(3):
            for r in range(2):
                for l in range(3):
                    ZL[0, m, r, k, l] = rows[k][l][r]

    def last_update(m, x):
        F = force(1, m, x)
        v = [HB[m, c, x] - (0.5 * kick_size) * F[c] for c in range(8)]
        zero = jnp.zeros_like(v[0])
        for i in range(3):
            NM[m, 0, i, i, x] = zero
        NM[m, 1, 0, 0, x] = v[0]
        NM[m, 1, 1, 1, x] = v[1]
        NM[m, 1, 2, 2, x] = -(v[0] + v[1])
        for i, j, c in ((0, 1, 2), (0, 2, 4), (1, 2, 6)):
            NM[m, 0, i, j, x] = v[c]
            NM[m, 0, j, i, x] = -v[c]
            NM[m, 1, i, j, x] = v[c + 1]
            NM[m, 1, j, i, x] = v[c + 1]

    def for_x(body):
        for x in range(2):
            body(x)

    def wait_ahead(stage, m, n):
        for link, d in ((n, m), (m, n)):
            if d in (1, 3):
                continue
            wait_forward(stage, d, link)
            if stage == 1:
                halo_update(d, link)
            elif d == 2:
                halo_decode(link)
            elif link in CODED_X:
                rows = decode([XR[link, c] for c in range(CODED)])
                for k in range(3):
                    for r in range(2):
                        for l in range(3):
                            V[link, r, k, l, 2] = rows[k][l][r]

    def send_pair(stage, m, n):
        if 1 in (m, n):
            return
        for link, d in ((m, n), (n, m)):
            send_back(stage, d, link)

    def whole_pair(stage, buf, m, n):
        wait_ahead(stage, m, n)
        for_x(lambda x: staple_task(stage, buf, m, n, x, loop_task(stage, buf, m, n, x)))
        send_pair(stage, m, n)

    def wait_back(stage, m, directions=(0, 1, 2)):
        for d in directions:
            if d != m:
                with jax.named_scope(f"wb{stage}_d{d}m{m}"):
                    wait_rows(backward[stage, d, m], brecv.at[lane_of[stage, d, m]])

    waits = {m: position for position, m in enumerate(LOADS)}
    loads[waits.pop(3)].wait()
    with jax.named_scope("bar"):
        pl.semaphore_wait(barrier, partners)
    send_link(*SENDS[0])
    for d, m in SENDS[1:]:
        if m in waits and d != 1:
            loads[waits.pop(m)].wait()
        send_link(d, m)
    for m, n in ORDERS[0]:
        whole_pair(0, V, m, n)
        if (m, n) == (1, 2):
            edge_rows(0, V)
            edge_loops(0)
            edge_staples(0)
            edge_merge(0)
    mom_load.wait()
    for m in UPDATES:
        for_x(lambda x: half_update(m, x))

    for m in Z_LINKS:
        add_x(m)
        send_half_z(m)
    for m in UPDATES:
        if m == 2:
            add_x(m)
        add_z(m)
        send_half_y(m)
        add_y(m)
        send_half_x(m)
    for m in UPDATES:
        for_x(lambda x: link_update(m, x))
    for m, n in ORDERS[1][:EARLY]:
        whole_pair(1, W, m, n)
    for m, n in ORDERS[1][EARLY:]:
        wait_ahead(1, m, n)
        for_x(lambda x: loop_task(1, W, m, n, x))
    edge_rows(1, W)
    edge_loops(1)

    def offsets(group):
        result = [()]
        for axis in range(3):
            span = range(sizes[axis]) if axis in group else (0,)
            result = [head + (k,) for head in result for k in span]
        return [item for item in result if any(item)]

    def spread(index, value):
        buf = slots[index]
        position = 0
        for axis in groups[index]:
            position = position * sizes[axis] + coords[axis]
        buf[position] = jnp.sum(value, axis=0, keepdims=True)
        for offset in offsets(groups[index]):
            send(buf.at[position], buf.at[position], offset, trecv.at[index])

    def gathered(index):
        wait_rows(slots[index].shape[0] - 1, trecv.at[index])
        value = slots[index][0]
        for k in range(1, slots[index].shape[0]):
            value = value + slots[index][k]
        return value

    def finish(m):
        wait_back(1, m)
        for_x(lambda x: last_update(m, x))

    value = TR[0] + TR[1]
    spread(0, value)
    edge_staples(1)
    for m, n in ORDERS[1][EARLY:]:
        for_x(lambda x: staple_task(1, W, m, n, x))
        send_pair(1, m, n)
    edge_merge(1)
    for position, m in enumerate(UPDATES):
        finish(m)
        if position + 1 < len(groups):
            value = gathered(position)
            spread(position + 1, value)
    with jax.named_scope("plaq"):
        lanes = gathered(len(groups) - 1) * (4.0 / (72.0 * volume))
        plaq_out[...] = jnp.broadcast_to(jnp.sum(lanes, axis=1, keepdims=True), (8, 128))
    wait_rows(sum(pending), send_sem.at[0])


def store_kernel(links, mom, plaq, links_out, mom_out, plaq_out, sem):
    copies = [
        pltpu.make_async_copy(links.at[:, :, :, :, 0:2], links_out, sem.at[0]),
        pltpu.make_async_copy(mom, mom_out, sem.at[1]),
        pltpu.make_async_copy(plaq.at[0:1], plaq_out, sem.at[2]),
    ]
    for copy in copies:
        copy.start()
    for copy in copies:
        copy.wait()


def per_device(gauge_links, momenta):
    block = gauge_links.shape
    assert block[-3:] == (2, 8, 2 * LT)
    sizes = tuple(lax.axis_size(axis) for axis in AXES)
    sites = block[-3] * block[-2] * block[-1]
    volume = sites * sizes[0] * sizes[1] * sizes[2]
    f32 = jnp.float32
    vm = lambda *shape: pltpu.VMEM(shape, f32)
    groups = ((0, 1, 2),) if sizes[0] * sizes[1] * sizes[2] <= 32 else ((0,), (1,), (2,))
    counts = []
    for group in groups:
        count = 1
        for axis in group:
            count *= sizes[axis]
        counts.append(count)
    dma = pltpu.SemaphoreType.DMA
    wide_links, momenta_vmem, plaquette = pl.pallas_call(
        functools.partial(kernel, sizes, volume, groups),
        out_shape=(
            vm(4, 2, 3, 3, 3, 8, 128),
            vm(*block),
            vm(8, 128),
        ),
        in_specs=[pl.BlockSpec(memory_space=pl.ANY)] * 2,
        out_specs=(
            pl.BlockSpec(memory_space=pltpu.VMEM),
            pl.BlockSpec(memory_space=pltpu.VMEM),
            pl.BlockSpec(memory_space=pltpu.VMEM),
        ),
        scratch_shapes=[
            vm(4, 2, 3, 3, 3, 8, 128),
            vm(*block),
            vm(4, 8, 3, 8, 128),
            vm(6, 8, 2, 8, 128),
            vm(2, 4, 4, 8, 3, 8, 128),
            vm(4, CODED, 8, 128),
            vm(4, CODED, 8, 128),
            vm(2, 3, 3, 8, 128),
            vm(2, 3, 3, 8, 128),
            vm(4, 8, 2, 1, 128),
            vm(2, 3, 3, 8, 128),
            vm(2, 3, 3, 8, 128),
            vm(2, 3, 3, 8, 128),
            vm(8, 8, 128),
            vm(2, 3, 8, 8, 128),
            vm(4, CODED, 8, 128),
            vm(4, CODED, 8, 128),
            vm(4, 8, 8, 128),
            vm(4, 8, 8, 128),
            vm(2, 4, 2, 3, 3, 8, 128),
            vm(2, 4, 8, 2, 1, 128),
            vm(2, 4, 8, 8, 128),
            vm(2, 4, 8, 8, 128),
            vm(2, 8, 128),
            dma((5,)),
            dma((1,)),
            dma((LANES,)),
            dma((LANES,)),
            dma((len(groups),)),
            vm(8192, 1, 128),
            *[vm(count, 1, 128) for count in counts],
        ],
        compiler_params=pltpu.CompilerParams(collective_id=0, has_side_effects=True),
        name="md_step",
    )(gauge_links, momenta)
    anywhere = pl.BlockSpec(memory_space=pl.ANY)
    in_vmem = pl.BlockSpec(memory_space=pltpu.VMEM)
    new_links, new_momenta, plaquette = pl.pallas_call(
        store_kernel,
        out_shape=(
            jax.ShapeDtypeStruct(block, f32),
            jax.ShapeDtypeStruct(block, f32),
            jax.ShapeDtypeStruct((1, 128), f32),
        ),
        in_specs=[in_vmem] * 3,
        out_specs=(anywhere,) * 3,
        scratch_shapes=[dma((3,))],
        name="store",
    )(
        pltpu.with_memory_space_constraint(wide_links, pltpu.VMEM),
        pltpu.with_memory_space_constraint(momenta_vmem, pltpu.VMEM),
        pltpu.with_memory_space_constraint(plaquette, pltpu.VMEM),
    )
    return new_links, new_momenta, plaquette[0, 0]


def solution(mesh):
    spec = P(None, None, None, None, "gx", "gy", "zt")
    return jax.shard_map(
        per_device,
        mesh=mesh,
        in_specs=(spec, spec),
        out_specs=(spec, spec, P()),
        check_vma=False,
    )
```

```python
import functools

import jax
import jax.numpy as jnp
from jax import lax
from jax.experimental import pallas as pl
from jax.experimental.pallas import tpu as pltpu
from jax.sharding import PartitionSpec as P

LT = 64
AXES = ("gx", "gy", "zt")
PAIRS = ((1, 3), (0, 3), (0, 1), (2, 3), (0, 2), (1, 2))
ORDERS = (
    ((1, 3), (0, 3), (0, 1), (2, 3), (1, 2), (0, 2)),
    ((1, 3), (2, 3), (0, 3), (0, 2), (0, 1), (1, 2)),
)
EARLY = 2
EDGE = (3, 0, 2)
LOADS = (3, 1, 0, 2)
Z_LINKS = (3, 0, 1)
SENDS = ((0, 3), (1, 3), (2, 3), (1, 0), (1, 2), (2, 1), (0, 1), (2, 0), (0, 2))
UPDATES = (3, 0, 1, 2)
MESH_ID = pl.DeviceIdType.MESH

kick_size = 0.25
step_size = 0.2


def mul(a, b):
    return a[0] * b[0] - a[1] * b[1], a[0] * b[1] + a[1] * b[0]


def mul_conj_second(a, b):
    return a[0] * b[0] + a[1] * b[1], a[1] * b[0] - a[0] * b[1]


def mul_conj_first(a, b):
    return a[0] * b[0] + a[1] * b[1], a[0] * b[1] - a[1] * b[0]


def add(a, b):
    return a[0] + b[0], a[1] + b[1]


def total(terms):
    result = terms[0]
    for term in terms[1:]:
        result = add(result, term)
    return result


def conj(a):
    return a[0], -a[1]


def pick(a, index):
    return a[0][index], a[1][index]


TINY = 1e-30
FAR = 1e15
CODED = 11
LANES = 15
CODED_X = (1, 2)


def project(first, rest):
    square = rest[0] * rest[0]
    for value in rest[1:]:
        square = square + value * value
    near = first >= 0.0
    low = jnp.where(near, 1.0 + first, square)
    factor = jnp.where(near, 1.0, 1.0 - first) / jnp.maximum(low, TINY)
    result = [value * factor for value in rest]
    result[0] = jnp.where(low < TINY, FAR, result[0])
    return result


def lift(values):
    square = values[0] * values[0]
    for value in values[1:]:
        square = square + value * value
    inverse = 1.0 / (1.0 + square)
    double = 2.0 * inverse
    return [(1.0 - square) * inverse] + [value * double for value in values]


def cross(a, b):
    result = []
    for i in range(3):
        j, k = (i + 1) % 3, (i + 2) % 3
        p, q = mul(a[j], b[k]), mul(a[k], b[j])
        result.append((p[0] - q[0], p[1] - q[1]))
    return result


def encode(rows):
    rows = [[pick(row, l) for l in range(3)] for row in rows]
    normal = cross(rows[0], rows[1])
    det = total([mul(rows[2][l], normal[l]) for l in range(3)])
    values = []
    for row in rows[:2]:
        flat = [part for entry in row for part in entry]
        values += project(flat[0], flat[1:])
    return values + project(det[0], [det[1]])


def decode(values):
    rows = []
    for start in (0, 5):
        flat = lift(values[start : start + 5])
        rows.append([(flat[2 * l], flat[2 * l + 1]) for l in range(3)])
    det = lift(values[10:])
    rows.append([mul_conj_second(det, entry) for entry in cross(rows[0], rows[1])])
    return rows


def kernel(
    sizes,
    volume,
    groups,
    links_in,
    mom_in,
    W,
    NM,
    plaq_out,
    V,
    MB,
    HB,
    TB,
    LB,
    XS,
    XR,
    EM,
    EN,
    YHS,
    EX,
    EP,
    EH,
    EK,
    ET,
    ZS,
    ZR,
    ZHS,
    ZHR,
    ZL,
    YBR,
    ZBS,
    ZBR,
    TR,
    load_sem,
    send_sem,
    frecv,
    brecv,
    trecv,
    lines,
    *slots,
):
    coords = [lax.axis_index(axis) for axis in AXES]

    def device(offset):
        return tuple(
            lax.rem(coords[axis] + (offset[axis] % sizes[axis]), sizes[axis]) for axis in range(3)
        )

    def along(axis, distance):
        return tuple(distance if other == axis else 0 for other in range(3))

    loads = []
    for m in LOADS:
        copy = pltpu.make_async_copy(links_in.at[m], V.at[m, :, :, :, 0:2], load_sem.at[m])
        copy.start()
        loads.append(copy)
    mom_load = pltpu.make_async_copy(mom_in, MB, load_sem.at[4])
    mom_load.start()

    barrier = pltpu.get_barrier_semaphore()
    partners = 0
    for axis in range(3):
        for k in range(1, sizes[axis]):
            pl.semaphore_signal(barrier, inc=1, device_id=device(along(axis, k)), device_id_type=MESH_ID)
            partners += 1

    shape3 = (1, 8, 128)
    lane = lax.broadcasted_iota(jnp.int32, shape3, 2)
    sub = lax.broadcasted_iota(jnp.int32, shape3, 1)
    sub2 = lax.broadcasted_iota(jnp.int32, shape3[1:], 0)
    t_index = lax.rem(lane, LT)
    half_lanes = lane.shape[-1] // 2
    low = lane < half_lanes
    low_row = lax.broadcasted_iota(jnp.int32, (1, 1, 128), 2) < half_lanes
    t_last = t_index == LT - 1
    t_first = t_index == 0
    y_first = sub == 0

    def choose(mask, a, b):
        return jnp.where(jnp.broadcast_to(mask, b.shape), jnp.broadcast_to(a, b.shape), b)

    pending = []

    def send(src, dst, offset, recv_sem):
        copy = pltpu.make_async_remote_copy(
            src_ref=src,
            dst_ref=dst,
            send_sem=send_sem.at[0],
            recv_sem=recv_sem,
            device_id=device(offset),
            device_id_type=MESH_ID,
        )
        copy.start()
        pending.append(rows_of(src))
        return copy

    def rows_of(ref):
        size = 1
        for extent in ref.shape:
            size *= extent
        return size // 128

    def wait_rows(count, sem):
        part = lines.at[0:count]
        pltpu.make_async_copy(part, part, sem).wait()

    lane_of = {}
    for d in range(3):
        for m in range(4):
            if d != m:
                lane_of[0, d, m] = len(set(lane_of.values()))
                lane_of[1, d, m] = lane_of[0, d, m] + (d > 0)
    forward = {}
    backward = {}

    def forward_send(stage, d, m, src, dst):
        send(src, dst, along(d, -1), frecv.at[lane_of[stage, d, m]])
        forward[stage, d, m] = forward.get((stage, d, m), 0) + rows_of(src)

    def wait_forward(stage, d, m):
        with jax.named_scope(f"wf{stage}_d{d}m{m}"):
            wait_rows(forward[stage, d, m], frecv.at[lane_of[stage, d, m]])

    def edge_row(m, x):
        row = 2 * EDGE.index(m) + x
        return slice(row, row + 1)

    def store_code(buf, m, rows):
        for c, value in enumerate(encode(rows)):
            buf[m, c] = value

    def pack_z(m):
        rows = []
        for i in range(3):
            parts = []
            for r in range(2):
                first = V[m, r, i, :, 0]
                second = V[m, r, i, :, 1]
                parts.append(choose(low, first, pltpu.roll(second, half_lanes, 2)))
            rows.append(tuple(parts))
        store_code(ZS, m, rows)

    def send_link(d, m):
        if d == 1:
            for x in range(2):
                forward_send(0, 1, m, V.at[m, :, :, :, x, 0:1], EH.at[:, :, :, edge_row(m, x)])
        elif d == 2:
            pack_z(m)
            forward_send(0, 2, m, ZS.at[m], ZR.at[m])
        elif m in CODED_X:
            store_code(XS, m, [(V[m, 0, k, :, 0], V[m, 1, k, :, 0]) for k in range(3)])
            forward_send(0, 0, m, XS.at[m], XR.at[m])
        else:
            forward_send(0, 0, m, V.at[m, :, :, :, 0], V.at[m, :, :, :, 2])

    def share(d, m):
        return (0.5 * kick_size) if m < d else (-0.5 * kick_size)

    def add_x(m):
        if m != 0:
            wait_back(0, m, (0,))
            HB[m, :, 0] = HB[m, :, 0] + share(0, m) * LB[0, 0, m, :, 0]

    def add_y(m):
        if m != 1:
            if m == 2:
                wait_back(0, m, (1,))
            for x in range(2):
                HB[m, :, x, 0:1] = HB[m, :, x, 0:1] + share(1, m) * YBR[0, m, :, x]

    def add_z(m):
        if m == 2:
            return
        wait_back(0, m, (2,))
        for x in range(2):
            halo = pltpu.roll(ZBR[0, m], half_lanes * x, 2) if x else ZBR[0, m]
            HB[m, :, x] = HB[m, :, x] + choose(low, share(2, m) * halo, jnp.zeros_like(halo))

    def send_half_z(m):
        ZHS[m] = choose(low, HB[m, :, 0], pltpu.roll(HB[m, :, 1], half_lanes, 2))
        if m != 1:
            wait_back(0, m, (1,))
            first, second = YBR[0, m, :, 0], YBR[0, m, :, 1]
            row = choose(low_row, first, pltpu.roll(second, half_lanes, 2))
            ZHS[m, :, 0:1] = ZHS[m, :, 0:1] + share(1, m) * row
        forward_send(1, 2, m, ZHS.at[m], ZHR.at[m])

    def send_half_y(m):
        if m != 1:
            for x in range(2):
                YHS[m, :, x] = HB[m, :, x, 0:1]
                forward_send(1, 1, m, YHS.at[m, :, x], EK.at[:, edge_row(m, x)])

    def send_half_x(m):
        if m != 0:
            forward_send(1, 0, m, HB.at[m, :, 0], HB.at[m, :, 2])

    def send_back(stage, d, m):
        if d == 3:
            return
        if d == 0:
            copies = [(LB.at[stage, 0, m, :, 2], LB.at[stage, 0, m, :, 0])]
        elif d == 1:
            copies = [(ET.at[stage, 1, :, edge_row(m, x)], YBR.at[stage, m, :, x]) for x in range(2)]
        else:
            first = LB[stage, 2, m, :, 1]
            second = LB[stage, 2, m, :, 2]
            ZBS[stage, m] = choose(low, pltpu.roll(first, half_lanes, 2), second)
            copies = [(ZBS.at[stage, m], ZBR.at[stage, m])]
        for src, dst in copies:
            send(src, dst, along(d, 1), brecv.at[lane_of[stage, d, m]])
            backward[stage, d, m] = backward.get((stage, d, m), 0) + rows_of(src)

    def ahead(stage, buf, n, d, x):
        rows = []
        for k in range(3):
            parts = []
            for r in range(2):
                if d == 0:
                    parts.append(buf[n, r, k, :, x + 1])
                    continue
                value = buf[n, r, k, :, x]
                if d == 3:
                    parts.append(
                        choose(t_last, pltpu.roll(value, LT - 1, 2), pltpu.roll(value, 127, 2))
                    )
                elif d == 1:
                    parts.append(pltpu.roll(value, 7, 1))
                else:
                    halo = pltpu.roll(ZL[stage, n, r, k], half_lanes * (1 - x), 2)
                    parts.append(choose(low, pltpu.roll(value, half_lanes, 2), halo))
            rows.append(tuple(parts))
        return rows

    def behind(stage, d, m, x):
        if d == 0:
            return LB[stage, 0, m, :, x]
        value = LB[stage, d, m, :, x + 1]
        if d == 1:
            return choose(y_first, YBR[stage, m, :, x], pltpu.roll(value, 1, 1))
        if d == 2:
            halo = pltpu.roll(ZBR[stage, m], half_lanes * x, 2)
            return choose(low, halo, pltpu.roll(value, half_lanes, 2))
        return choose(t_first, pltpu.roll(value, 128 - (LT - 1), 2), pltpu.roll(value, 1, 2))

    def conjugate(T, rows):
        d0, d1, d2, h01, h02, h12 = T
        full = [
            [d0, h01, h02],
            [(-h01[0], h01[1]), d1, h12],
            [(-h02[0], h02[1]), (-h12[0], h12[1]), d2],
        ]
        M = []
        for i in range(3):
            terms = []
            for k in range(3):
                if i == k:
                    terms.append((-(full[i][i] * rows[k][1]), full[i][i] * rows[k][0]))
                else:
                    terms.append(mul(full[i][k], rows[k]))
            M.append(total(terms))
        r0 = 0.0
        r1 = 0.0
        for k in range(3):
            r0 = r0 + (rows[k][0][0] * M[k][1][0] - rows[k][1][0] * M[k][0][0])
            r1 = r1 + (rows[k][0][1] * M[k][1][1] - rows[k][1][1] * M[k][0][1])
        tail = slice(1, 3)
        row0 = total(
            [mul_conj_first(pick(rows[k], 0), (M[k][0][tail], M[k][1][tail])) for k in range(3)]
        )
        r12 = total([mul_conj_first(pick(rows[k], 1), pick(M[k], 2)) for k in range(3)])
        return [r0, r1, row0[0][0], row0[1][0], row0[0][1], row0[1][1], r12[0], r12[1]]

    def close(A, m_ahead, columns):
        Bt = []
        for k in range(3):
            Bt.append(total([mul(pick(m_ahead[l], k), columns[l]) for l in range(3)]))
        loop = []
        for i in range(3):
            loop.append(total([mul_conj_second(pick(A[i], k), Bt[k]) for k in range(3)]))
        i0, i1, i2 = loop[0][1][0], loop[1][1][1], loop[2][1][2]
        mean = (i0 + i1 + i2) * (2.0 / 3.0)
        d0 = 2.0 * i0 - mean
        d1 = 2.0 * i1 - mean

        def off(i, j):
            a = pick(loop[i], j)
            b = pick(loop[j], i)
            return a[0] - b[0], a[1] + b[1]

        h01, h02, h12 = off(0, 1), off(0, 2), off(1, 2)
        values = [d0, d1, h01[0], h01[1], h02[0], h02[1], h12[0], h12[1]]
        return values, loop[0][0][0] + loop[1][0][1] + loop[2][0][2]

    def loop_task(stage, buf, m, n, x):
        index = PAIRS.index((m, n))
        n_ahead = ahead(stage, buf, n, m, x)
        A = []
        for i in range(3):
            A.append(
                total(
                    [mul((buf[m, 0, i, k, x], buf[m, 1, i, k, x]), n_ahead[k]) for k in range(3)]
                )
            )
        m_ahead = ahead(stage, buf, m, n, x)
        columns = [(buf[n, 0, :, l, x], buf[n, 1, :, l, x]) for l in range(3)]
        values, trace = close(A, m_ahead, columns)
        for c in range(8):
            TB[index, c, x] = values[c]
        if stage == 1:
            if 1 in (m, n):
                trace = jnp.where(sub2 == 7, 0.0, trace)
            TR[x] = trace if (m, n) == ORDERS[1][0] else TR[x] + trace
        return values

    def algebra(values):
        d0, d1 = values[0], values[1]
        return (d0, d1, -(d0 + d1), tuple(values[2:4]), tuple(values[4:6]), tuple(values[6:8]))

    def edge_rows(stage, buf):
        for r in range(2):
            for k in range(3):
                for s, m in enumerate(EDGE):
                    for x in range(2):
                        row = slice(2 * s + x, 2 * s + x + 1)
                        EM[r, k, :, row] = buf[m, r, k, :, x, 7:8, :]
                        EN[r, k, :, row] = buf[1, r, k, :, x, 7:8, :]
                for x in range(2):
                    EX[r, k, :, 2 + x : 3 + x] = buf[1, r, k, :, x + 1, 7:8, :]
                    EX[r, k, :, 4 + x : 5 + x] = ZL[stage, 1, r, k, :, 7:8]
        n_ahead = []
        for k in range(3):
            parts = []
            for r in range(2):
                own, other = EN[r, k], EX[r, k]
                t_ahead = choose(t_last, pltpu.roll(own, LT - 1, 2), pltpu.roll(own, 127, 2))
                halo = choose(sub == 4, pltpu.roll(other, half_lanes, 2), other)
                z_ahead = choose(low, pltpu.roll(own, half_lanes, 2), halo)
                parts.append(choose(sub < 2, t_ahead, choose(sub < 4, other, z_ahead)))
            n_ahead.append(tuple(parts))
        for i in range(3):
            value = total([mul((EM[0, i, k], EM[1, i, k]), n_ahead[k]) for k in range(3)])
            EP[0, i], EP[1, i] = value

    def edge_loops(stage):
        for m in EDGE:
            wait_forward(stage, 1, m)
        m_ahead = [(EH[0, k], EH[1, k]) for k in range(3)]
        if stage == 1:
            scale = jnp.where((sub2 < 2) | (sub2 > 3), share(1, 3), share(1, 0))
            m_ahead = cayley([EK[c] + scale * ET[0, 1, c] for c in range(8)], m_ahead)
        A = [(EP[0, i], EP[1, i]) for i in range(3)]
        columns = [(EN[0, :, l], EN[1, :, l]) for l in range(3)]
        values, trace = close(A, m_ahead, columns)
        if stage == 1:
            TR[0] = TR[0] + jnp.where(sub2 < 6, trace, 0.0)
        sign = jnp.where((sub2 < 2) | (sub2 > 3), -1.0, 1.0)
        for c in range(8):
            ET[stage, 0, c] = sign * values[c]

    def edge_staples(stage):
        T = algebra([ET[stage, 0, c] for c in range(8)])
        for slot, buf in ((1, EN), (2, EM)):
            result = conjugate(T, [(buf[0, k], buf[1, k]) for k in range(3)])
            for c in range(8):
                ET[stage, slot, c] = result[c]
        for m in EDGE:
            send_back(stage, 1, m)

    def edge_merge(stage):
        for m in EDGE:
            index = PAIRS.index((min(m, 1), max(m, 1)))
            for x in range(2):
                TB[index, :, x, 7:8] = ET[stage, 0, :, edge_row(m, x)]
                LB[stage, m, 1, :, x + 1, 7:8] = ET[stage, 2, :, edge_row(m, x)]
        for d in (2, 0):
            send_back(stage, d, 1)

    def staple_task(stage, buf, m, n, x, values=None):
        if values is None:
            index = PAIRS.index((m, n))
            values = [TB[index, c, x] for c in range(8)]
        T = algebra(values)
        for link, d in ((m, n), (n, m)):
            rows = [(buf[d, 0, k, :, x], buf[d, 1, k, :, x]) for k in range(3)]
            result = conjugate(T, rows)
            for c in range(8):
                LB[stage, d, link, c, x + 1] = result[c]

    def force(stage, m, x, directions=(0, 1, 2, 3)):
        result = None
        for n in range(4):
            if n == m:
                continue
            index = PAIRS.index((min(m, n), max(m, n)))
            term = TB[index, :, x]
            if n in directions:
                term = term - behind(stage, n, m, x)
            if result is None:
                result = term if m < n else -term
            else:
                result = result + term if m < n else result - term
        return result

    places = ((1, 0, 0), (1, 1, 1), (0, 0, 1), (1, 0, 1), (0, 0, 2), (1, 0, 2), (0, 1, 2), (1, 1, 2))

    def half_update(m, x):
        F = None
        for n in range(4):
            if n == m:
                continue
            term = TB[PAIRS.index((min(m, n), max(m, n))), :, x]
            if n == 0 and x:
                term = term - LB[0, 0, m, :, x]
            elif n != 0:
                value = LB[0, n, m, :, x + 1]
                if n == 1:
                    back = choose(y_first, jnp.zeros_like(value), pltpu.roll(value, 1, 1))
                elif n == 2:
                    back = choose(low, jnp.zeros_like(value), pltpu.roll(value, half_lanes, 2))
                else:
                    back = behind(0, 3, m, x)
                term = term - back
            term = term if m < n else -term
            F = term if F is None else F + term
        for c, (r, i, j) in enumerate(places):
            HB[m, c, x] = MB[m, r, i, j, x] - (0.5 * kick_size) * F[c]

    def cayley(momentum, rows):
        half = [(0.5 * step_size) * value for value in momentum]
        d0, d1 = half[0], half[1]
        d2 = -(d0 + d1)
        h01, h02, h12 = (half[2], half[3]), (half[4], half[5]), (half[6], half[7])
        n01 = h01[0] * h01[0] + h01[1] * h01[1]
        n02 = h02[0] * h02[0] + h02[1] * h02[1]
        n12 = h12[0] * h12[0] + h12[1] * h12[1]
        k00 = d0 * d0 + n01 + n02
        k11 = d1 * d1 + n01 + n12
        k22 = d2 * d2 + n02 + n12
        one_c = 1.0 + 0.5 * (k00 + k11 + k22)
        h01h12 = mul(h01, h12)
        z_imag = h01h12[1] * h02[0] - h01h12[0] * h02[1]
        h = d0 * n12 + d2 * n01 + d1 * n02 - d0 * d1 * d2 - 2.0 * z_imag
        factor = 2.0 / (one_c * one_c + h * h)
        f = (one_c * factor, h * factor)
        s01 = mul_conj_second(h02, h12)
        k01 = (-(d0 + d1) * h01[1] - s01[0], (d0 + d1) * h01[0] - s01[1])
        k02 = (h01h12[0] - (d0 + d2) * h02[1], h01h12[1] + (d0 + d2) * h02[0])
        s12 = mul_conj_first(h01, h02)
        k12 = (-s12[0] - (d1 + d2) * h12[1], (d1 + d2) * h12[0] - s12[1])
        G = [[None] * 3 for _ in range(3)]
        for i, (k, d) in enumerate(((k00, d0), (k11, d1), (k22, d2))):
            G[i][i] = (one_c - k, d)
        for i, j, hh, kk in ((0, 1, h01, k01), (0, 2, h02, k02), (1, 2, h12, k12)):
            G[i][j] = add(hh, kk)
            G[j][i] = (kk[0] - hh[0], hh[1] - kk[1])
        result = []
        for i in range(3):
            E = []
            for k in range(3):
                value = mul(f, G[i][k])
                E.append((value[0] - 1.0, value[1]) if i == k else value)
            result.append(total([mul(E[k], rows[k]) for k in range(3)]))
        return result

    def link_update(m, x):
        rows = [(V[m, 0, k, :, x], V[m, 1, k, :, x]) for k in range(3)]
        new = cayley([HB[m, c, x] for c in range(8)], rows)
        for i in range(3):
            W[m, 0, i, :, x] = new[i][0]
            W[m, 1, i, :, x] = new[i][1]

    def halo_update(d, m):
        if d == 0:
            link_update(m, 2)
            return
        rows = [(ZL[0, m, 0, k], ZL[0, m, 1, k]) for k in range(3)]
        scale = share(2, m)
        new = cayley([ZHR[m, c] + scale * ZBS[0, m, c] for c in range(8)], rows)
        for i in range(3):
            ZL[1, m, 0, i] = new[i][0]
            ZL[1, m, 1, i] = new[i][1]

    def halo_decode(m):
        rows = decode([ZR[m, c] for c in range(CODED)])
        for k in range(3):
            for r in range(2):
                for l in range(3):
                    ZL[0, m, r, k, l] = rows[k][l][r]

    def last_update(m, x):
        F = force(1, m, x)
        v = [HB[m, c, x] - (0.5 * kick_size) * F[c] for c in range(8)]
        zero = jnp.zeros_like(v[0])
        for i in range(3):
            NM[m, 0, i, i, x] = zero
        NM[m, 1, 0, 0, x] = v[0]
        NM[m, 1, 1, 1, x] = v[1]
        NM[m, 1, 2, 2, x] = -(v[0] + v[1])
        for i, j, c in ((0, 1, 2), (0, 2, 4), (1, 2, 6)):
            NM[m, 0, i, j, x] = v[c]
            NM[m, 0, j, i, x] = -v[c]
            NM[m, 1, i, j, x] = v[c + 1]
            NM[m, 1, j, i, x] = v[c + 1]

    def for_x(body):
        for x in range(2):
            body(x)

    def wait_ahead(stage, m, n):
        for link, d in ((n, m), (m, n)):
            if d in (1, 3):
                continue
            wait_forward(stage, d, link)
            if stage == 1:
                halo_update(d, link)
            elif d == 2:
                halo_decode(link)
            elif link in CODED_X:
                rows = decode([XR[link, c] for c in range(CODED)])
                for k in range(3):
                    for r in range(2):
                        for l in range(3):
                            V[link, r, k, l, 2] = rows[k][l][r]

    def send_pair(stage, m, n):
        if 1 in (m, n):
            return
        for link, d in ((m, n), (n, m)):
            send_back(stage, d, link)

    def whole_pair(stage, buf, m, n):
        wait_ahead(stage, m, n)
        for_x(lambda x: staple_task(stage, buf, m, n, x, loop_task(stage, buf, m, n, x)))
        send_pair(stage, m, n)

    def wait_back(stage, m, directions=(0, 1, 2)):
        for d in directions:
            if d != m:
                with jax.named_scope(f"wb{stage}_d{d}m{m}"):
                    wait_rows(backward[stage, d, m], brecv.at[lane_of[stage, d, m]])

    waits = {m: position for position, m in enumerate(LOADS)}
    loads[waits.pop(3)].wait()
    with jax.named_scope("bar"):
        pl.semaphore_wait(barrier, partners)
    send_link(*SENDS[0])
    for d, m in SENDS[1:]:
        if m in waits:
            loads[waits.pop(m)].wait()
        send_link(d, m)
    for m, n in ORDERS[0]:
        whole_pair(0, V, m, n)
        if (m, n) == (1, 2):
            edge_rows(0, V)
            edge_loops(0)
            edge_staples(0)
            edge_merge(0)
    mom_load.wait()
    for m in UPDATES:
        for_x(lambda x: half_update(m, x))

    for m in Z_LINKS:
        add_x(m)
        send_half_z(m)
    for m in UPDATES:
        if m == 2:
            add_x(m)
        add_z(m)
        send_half_y(m)
        add_y(m)
        send_half_x(m)
    for m in UPDATES:
        for_x(lambda x: link_update(m, x))
    for m, n in ORDERS[1][:EARLY]:
        whole_pair(1, W, m, n)
    for m, n in ORDERS[1][EARLY:]:
        wait_ahead(1, m, n)
        for_x(lambda x: loop_task(1, W, m, n, x))
    edge_rows(1, W)
    edge_loops(1)

    def offsets(group):
        result = [()]
        for axis in range(3):
            span = range(sizes[axis]) if axis in group else (0,)
            result = [head + (k,) for head in result for k in span]
        weight = lambda item: sum(min(k, size - k) + (k % 2) for k, size in zip(item, sizes))
        return sorted([item for item in result if any(item)], key=weight, reverse=True)

    def spread(index, value):
        buf = slots[index]
        position = 0
        for axis in groups[index]:
            position = position * sizes[axis] + coords[axis]
        buf[position] = jnp.sum(value, axis=0, keepdims=True)
        for offset in offsets(groups[index]):
            send(buf.at[position], buf.at[position], offset, trecv.at[index])

    def gathered(index):
        wait_rows(slots[index].shape[0] - 1, trecv.at[index])
        value = slots[index][0]
        for k in range(1, slots[index].shape[0]):
            value = value + slots[index][k]
        return value

    def finish(m):
        wait_back(1, m)
        for_x(lambda x: last_update(m, x))

    value = TR[0] + TR[1]
    spread(0, value)
    edge_staples(1)
    for m, n in ORDERS[1][EARLY:]:
        for_x(lambda x: staple_task(1, W, m, n, x))
        send_pair(1, m, n)
    edge_merge(1)
    for position, m in enumerate(UPDATES):
        finish(m)
        if position + 1 < len(groups):
            value = gathered(position)
            spread(position + 1, value)
    with jax.named_scope("plaq"):
        lanes = gathered(len(groups) - 1) * (4.0 / (72.0 * volume))
        plaq_out[...] = jnp.broadcast_to(jnp.sum(lanes, axis=1, keepdims=True), (8, 128))
    wait_rows(sum(pending), send_sem.at[0])


def store_kernel(links, mom, plaq, links_out, mom_out, plaq_out, sem):
    copies = [
        pltpu.make_async_copy(links.at[:, :, :, :, 0:2], links_out, sem.at[0]),
        pltpu.make_async_copy(mom, mom_out, sem.at[1]),
        pltpu.make_async_copy(plaq.at[0:1], plaq_out, sem.at[2]),
    ]
    for copy in copies:
        copy.start()
    for copy in copies:
        copy.wait()


def per_device(gauge_links, momenta):
    block = gauge_links.shape
    assert block[-3:] == (2, 8, 2 * LT)
    sizes = tuple(lax.axis_size(axis) for axis in AXES)
    sites = block[-3] * block[-2] * block[-1]
    volume = sites * sizes[0] * sizes[1] * sizes[2]
    f32 = jnp.float32
    vm = lambda *shape: pltpu.VMEM(shape, f32)
    groups = ((0, 1, 2),) if sizes[0] * sizes[1] * sizes[2] <= 32 else ((0,), (1,), (2,))
    counts = []
    for group in groups:
        count = 1
        for axis in group:
            count *= sizes[axis]
        counts.append(count)
    dma = pltpu.SemaphoreType.DMA
    wide_links, momenta_vmem, plaquette = pl.pallas_call(
        functools.partial(kernel, sizes, volume, groups),
        out_shape=(
            vm(4, 2, 3, 3, 3, 8, 128),
            vm(*block),
            vm(8, 128),
        ),
        in_specs=[pl.BlockSpec(memory_space=pl.ANY)] * 2,
        out_specs=(
            pl.BlockSpec(memory_space=pltpu.VMEM),
            pl.BlockSpec(memory_space=pltpu.VMEM),
            pl.BlockSpec(memory_space=pltpu.VMEM),
        ),
        scratch_shapes=[
            vm(4, 2, 3, 3, 3, 8, 128),
            vm(*block),
            vm(4, 8, 3, 8, 128),
            vm(6, 8, 2, 8, 128),
            vm(2, 4, 4, 8, 3, 8, 128),
            vm(4, CODED, 8, 128),
            vm(4, CODED, 8, 128),
            vm(2, 3, 3, 8, 128),
            vm(2, 3, 3, 8, 128),
            vm(4, 8, 2, 1, 128),
            vm(2, 3, 3, 8, 128),
            vm(2, 3, 3, 8, 128),
            vm(2, 3, 3, 8, 128),
            vm(8, 8, 128),
            vm(2, 3, 8, 8, 128),
            vm(4, CODED, 8, 128),
            vm(4, CODED, 8, 128),
            vm(4, 8, 8, 128),
            vm(4, 8, 8, 128),
            vm(2, 4, 2, 3, 3, 8, 128),
            vm(2, 4, 8, 2, 1, 128),
            vm(2, 4, 8, 8, 128),
            vm(2, 4, 8, 8, 128),
            vm(2, 8, 128),
            dma((5,)),
            dma((1,)),
            dma((LANES,)),
            dma((LANES,)),
            dma((len(groups),)),
            vm(8192, 1, 128),
            *[vm(count, 1, 128) for count in counts],
        ],
        compiler_params=pltpu.CompilerParams(collective_id=0, has_side_effects=True),
        name="md_step",
    )(gauge_links, momenta)
    anywhere = pl.BlockSpec(memory_space=pl.ANY)
    in_vmem = pl.BlockSpec(memory_space=pltpu.VMEM)
    new_links, new_momenta, plaquette = pl.pallas_call(
        store_kernel,
        out_shape=(
            jax.ShapeDtypeStruct(block, f32),
            jax.ShapeDtypeStruct(block, f32),
            jax.ShapeDtypeStruct((1, 128), f32),
        ),
        in_specs=[in_vmem] * 3,
        out_specs=(anywhere,) * 3,
        scratch_shapes=[dma((3,))],
        name="store",
    )(
        pltpu.with_memory_space_constraint(wide_links, pltpu.VMEM),
        pltpu.with_memory_space_constraint(momenta_vmem, pltpu.VMEM),
        pltpu.with_memory_space_constraint(plaquette, pltpu.VMEM),
    )
    return new_links, new_momenta, plaquette[0, 0]


def solution(mesh):
    spec = P(None, None, None, None, "gx", "gy", "zt")
    return jax.shard_map(
        per_device,
        mesh=mesh,
        in_specs=(spec, spec),
        out_specs=(spec, spec, P()),
        check_vma=False,
    )
```

```python
import functools

import jax
import jax.numpy as jnp
from jax import lax
from jax.experimental import pallas as pl
from jax.experimental.pallas import tpu as pltpu
from jax.sharding import PartitionSpec as P

LT = 64
AXES = ("gx", "gy", "zt")
PAIRS = ((1, 3), (0, 3), (0, 1), (2, 3), (0, 2), (1, 2))
ORDERS = (
    ((1, 3), (0, 3), (0, 1), (2, 3), (1, 2), (0, 2)),
    ((1, 3), (2, 3), (0, 3), (0, 2), (0, 1), (1, 2)),
)
EARLY = 3
EDGE = (3, 0, 2)
LOADS = (3, 1, 0, 2)
Z_LINKS = (3, 0, 1)
SENDS = ((0, 3), (1, 3), (2, 3), (1, 0), (1, 2), (2, 1), (0, 1), (2, 0), (0, 2))
UPDATES = (3, 2, 0, 1)
MESH_ID = pl.DeviceIdType.MESH

kick_size = 0.25
step_size = 0.2


def mul(a, b):
    return a[0] * b[0] - a[1] * b[1], a[0] * b[1] + a[1] * b[0]


def mul_conj_second(a, b):
    return a[0] * b[0] + a[1] * b[1], a[1] * b[0] - a[0] * b[1]


def mul_conj_first(a, b):
    return a[0] * b[0] + a[1] * b[1], a[0] * b[1] - a[1] * b[0]


def add(a, b):
    return a[0] + b[0], a[1] + b[1]


def total(terms):
    result = terms[0]
    for term in terms[1:]:
        result = add(result, term)
    return result


def conj(a):
    return a[0], -a[1]


def pick(a, index):
    return a[0][index], a[1][index]


TINY = 1e-30
FAR = 1e15
CODED = 11
LANES = 15
CODED_X = (1, 2)


def project(first, rest):
    square = rest[0] * rest[0]
    for value in rest[1:]:
        square = square + value * value
    near = first >= 0.0
    low = jnp.where(near, 1.0 + first, square)
    factor = jnp.where(near, 1.0, 1.0 - first) / jnp.maximum(low, TINY)
    result = [value * factor for value in rest]
    result[0] = jnp.where(low < TINY, FAR, result[0])
    return result


def lift(values):
    square = values[0] * values[0]
    for value in values[1:]:
        square = square + value * value
    inverse = 1.0 / (1.0 + square)
    double = 2.0 * inverse
    return [(1.0 - square) * inverse] + [value * double for value in values]


def cross(a, b):
    result = []
    for i in range(3):
        j, k = (i + 1) % 3, (i + 2) % 3
        p, q = mul(a[j], b[k]), mul(a[k], b[j])
        result.append((p[0] - q[0], p[1] - q[1]))
    return result


def encode(rows):
    rows = [[pick(row, l) for l in range(3)] for row in rows]
    normal = cross(rows[0], rows[1])
    det = total([mul(rows[2][l], normal[l]) for l in range(3)])
    values = []
    for row in rows[:2]:
        flat = [part for entry in row for part in entry]
        values += project(flat[0], flat[1:])
    return values + project(det[0], [det[1]])


def decode(values):
    rows = []
    for start in (0, 5):
        flat = lift(values[start : start + 5])
        rows.append([(flat[2 * l], flat[2 * l + 1]) for l in range(3)])
    det = lift(values[10:])
    rows.append([mul_conj_second(det, entry) for entry in cross(rows[0], rows[1])])
    return rows


def kernel(
    sizes,
    volume,
    groups,
    links_in,
    mom_in,
    W,
    NM,
    plaq_out,
    V,
    MB,
    HB,
    TB,
    LB,
    XS,
    XR,
    EM,
    EN,
    YHS,
    EX,
    EP,
    EH,
    EK,
    ET,
    ZS,
    ZR,
    ZHS,
    ZHR,
    ZL,
    YBR,
    ZBS,
    ZBR,
    TR,
    load_sem,
    send_sem,
    frecv,
    brecv,
    trecv,
    lines,
    *slots,
):
    coords = [lax.axis_index(axis) for axis in AXES]

    def device(offset):
        return tuple(
            lax.rem(coords[axis] + (offset[axis] % sizes[axis]), sizes[axis]) for axis in range(3)
        )

    def along(axis, distance):
        return tuple(distance if other == axis else 0 for other in range(3))

    loads = []
    for m in LOADS:
        copy = pltpu.make_async_copy(links_in.at[m], V.at[m, :, :, :, 0:2], load_sem.at[m])
        copy.start()
        loads.append(copy)
    mom_load = pltpu.make_async_copy(mom_in, MB, load_sem.at[4])
    mom_load.start()

    barrier = pltpu.get_barrier_semaphore()
    partners = 0
    for axis in range(3):
        for k in range(1, sizes[axis]):
            pl.semaphore_signal(barrier, inc=1, device_id=device(along(axis, k)), device_id_type=MESH_ID)
            partners += 1

    shape3 = (1, 8, 128)
    lane = lax.broadcasted_iota(jnp.int32, shape3, 2)
    sub = lax.broadcasted_iota(jnp.int32, shape3, 1)
    sub2 = lax.broadcasted_iota(jnp.int32, shape3[1:], 0)
    t_index = lax.rem(lane, LT)
    half_lanes = lane.shape[-1] // 2
    low = lane < half_lanes
    low_row = lax.broadcasted_iota(jnp.int32, (1, 1, 128), 2) < half_lanes
    t_last = t_index == LT - 1
    t_first = t_index == 0
    y_first = sub == 0

    def choose(mask, a, b):
        return jnp.where(jnp.broadcast_to(mask, b.shape), jnp.broadcast_to(a, b.shape), b)

    pending = []

    def send(src, dst, offset, recv_sem):
        copy = pltpu.make_async_remote_copy(
            src_ref=src,
            dst_ref=dst,
            send_sem=send_sem.at[0],
            recv_sem=recv_sem,
            device_id=device(offset),
            device_id_type=MESH_ID,
        )
        copy.start()
        pending.append(rows_of(src))
        return copy

    def rows_of(ref):
        size = 1
        for extent in ref.shape:
            size *= extent
        return size // 128

    def wait_rows(count, sem):
        part = lines.at[0:count]
        pltpu.make_async_copy(part, part, sem).wait()

    lane_of = {}
    for d in range(3):
        for m in range(4):
            if d != m:
                lane_of[0, d, m] = len(set(lane_of.values()))
                lane_of[1, d, m] = lane_of[0, d, m] + (d > 0)
    forward = {}
    backward = {}

    def forward_send(stage, d, m, src, dst):
        send(src, dst, along(d, -1), frecv.at[lane_of[stage, d, m]])
        forward[stage, d, m] = forward.get((stage, d, m), 0) + rows_of(src)

    def wait_forward(stage, d, m):
        with jax.named_scope(f"wf{stage}_d{d}m{m}"):
            wait_rows(forward[stage, d, m], frecv.at[lane_of[stage, d, m]])

    def edge_row(m, x):
        row = 2 * EDGE.index(m) + x
        return slice(row, row + 1)

    def store_code(buf, m, rows):
        for c, value in enumerate(encode(rows)):
            buf[m, c] = value

    def pack_z(m):
        rows = []
        for i in range(3):
            parts = []
            for r in range(2):
                first = V[m, r, i, :, 0]
                second = V[m, r, i, :, 1]
                parts.append(choose(low, first, pltpu.roll(second, half_lanes, 2)))
            rows.append(tuple(parts))
        store_code(ZS, m, rows)

    def send_link(d, m):
        if d == 1:
            for x in range(2):
                forward_send(0, 1, m, V.at[m, :, :, :, x, 0:1], EH.at[:, :, :, edge_row(m, x)])
        elif d == 2:
            pack_z(m)
            forward_send(0, 2, m, ZS.at[m], ZR.at[m])
        elif m in CODED_X:
            store_code(XS, m, [(V[m, 0, k, :, 0], V[m, 1, k, :, 0]) for k in range(3)])
            forward_send(0, 0, m, XS.at[m], XR.at[m])
        else:
            forward_send(0, 0, m, V.at[m, :, :, :, 0], V.at[m, :, :, :, 2])

    def share(d, m):
        return (0.5 * kick_size) if m < d else (-0.5 * kick_size)

    def add_x(m):
        if m != 0:
            wait_back(0, m, (0,))
            HB[m, :, 0] = HB[m, :, 0] + share(0, m) * LB[0, 0, m, :, 0]

    def add_y(m):
        if m != 1:
            if m == 2:
                wait_back(0, m, (1,))
            for x in range(2):
                HB[m, :, x, 0:1] = HB[m, :, x, 0:1] + share(1, m) * YBR[0, m, :, x]

    def add_z(m):
        if m == 2:
            return
        wait_back(0, m, (2,))
        for x in range(2):
            halo = pltpu.roll(ZBR[0, m], half_lanes * x, 2) if x else ZBR[0, m]
            HB[m, :, x] = HB[m, :, x] + choose(low, share(2, m) * halo, jnp.zeros_like(halo))

    def send_half_z(m):
        ZHS[m] = choose(low, HB[m, :, 0], pltpu.roll(HB[m, :, 1], half_lanes, 2))
        if m != 1:
            wait_back(0, m, (1,))
            first, second = YBR[0, m, :, 0], YBR[0, m, :, 1]
            row = choose(low_row, first, pltpu.roll(second, half_lanes, 2))
            ZHS[m, :, 0:1] = ZHS[m, :, 0:1] + share(1, m) * row
        forward_send(1, 2, m, ZHS.at[m], ZHR.at[m])

    def send_half_y(m):
        if m != 1:
            for x in range(2):
                YHS[m, :, x] = HB[m, :, x, 0:1]
                forward_send(1, 1, m, YHS.at[m, :, x], EK.at[:, edge_row(m, x)])

    def send_half_x(m):
        if m != 0:
            forward_send(1, 0, m, HB.at[m, :, 0], HB.at[m, :, 2])

    def send_back(stage, d, m):
        if d == 3:
            return
        if d == 0:
            copies = [(LB.at[stage, 0, m, :, 2], LB.at[stage, 0, m, :, 0])]
        elif d == 1:
            copies = [(ET.at[stage, 1, :, edge_row(m, x)], YBR.at[stage, m, :, x]) for x in range(2)]
        else:
            first = LB[stage, 2, m, :, 1]
            second = LB[stage, 2, m, :, 2]
            ZBS[stage, m] = choose(low, pltpu.roll(first, half_lanes, 2), second)
            copies = [(ZBS.at[stage, m], ZBR.at[stage, m])]
        for src, dst in copies:
            send(src, dst, along(d, 1), brecv.at[lane_of[stage, d, m]])
            backward[stage, d, m] = backward.get((stage, d, m), 0) + rows_of(src)

    def ahead(stage, buf, n, d, x):
        rows = []
        for k in range(3):
            parts = []
            for r in range(2):
                if d == 0:
                    parts.append(buf[n, r, k, :, x + 1])
                    continue
                value = buf[n, r, k, :, x]
                if d == 3:
                    parts.append(
                        choose(t_last, pltpu.roll(value, LT - 1, 2), pltpu.roll(value, 127, 2))
                    )
                elif d == 1:
                    parts.append(pltpu.roll(value, 7, 1))
                else:
                    halo = pltpu.roll(ZL[stage, n, r, k], half_lanes * (1 - x), 2)
                    parts.append(choose(low, pltpu.roll(value, half_lanes, 2), halo))
            rows.append(tuple(parts))
        return rows

    def behind(stage, d, m, x):
        if d == 0:
            return LB[stage, 0, m, :, x]
        value = LB[stage, d, m, :, x + 1]
        if d == 1:
            return choose(y_first, YBR[stage, m, :, x], pltpu.roll(value, 1, 1))
        if d == 2:
            halo = pltpu.roll(ZBR[stage, m], half_lanes * x, 2)
            return choose(low, halo, pltpu.roll(value, half_lanes, 2))
        return choose(t_first, pltpu.roll(value, 128 - (LT - 1), 2), pltpu.roll(value, 1, 2))

    def conjugate(T, rows):
        d0, d1, d2, h01, h02, h12 = T
        full = [
            [d0, h01, h02],
            [(-h01[0], h01[1]), d1, h12],
            [(-h02[0], h02[1]), (-h12[0], h12[1]), d2],
        ]
        M = []
        for i in range(3):
            terms = []
            for k in range(3):
                if i == k:
                    terms.append((-(full[i][i] * rows[k][1]), full[i][i] * rows[k][0]))
                else:
                    terms.append(mul(full[i][k], rows[k]))
            M.append(total(terms))
        r0 = 0.0
        r1 = 0.0
        for k in range(3):
            r0 = r0 + (rows[k][0][0] * M[k][1][0] - rows[k][1][0] * M[k][0][0])
            r1 = r1 + (rows[k][0][1] * M[k][1][1] - rows[k][1][1] * M[k][0][1])
        tail = slice(1, 3)
        row0 = total(
            [mul_conj_first(pick(rows[k], 0), (M[k][0][tail], M[k][1][tail])) for k in range(3)]
        )
        r12 = total([mul_conj_first(pick(rows[k], 1), pick(M[k], 2)) for k in range(3)])
        return [r0, r1, row0[0][0], row0[1][0], row0[0][1], row0[1][1], r12[0], r12[1]]

    def close(A, m_ahead, columns):
        Bt = []
        for k in range(3):
            Bt.append(total([mul(pick(m_ahead[l], k), columns[l]) for l in range(3)]))
        loop = []
        for i in range(3):
            loop.append(total([mul_conj_second(pick(A[i], k), Bt[k]) for k in range(3)]))
        i0, i1, i2 = loop[0][1][0], loop[1][1][1], loop[2][1][2]
        mean = (i0 + i1 + i2) * (2.0 / 3.0)
        d0 = 2.0 * i0 - mean
        d1 = 2.0 * i1 - mean

        def off(i, j):
            a = pick(loop[i], j)
            b = pick(loop[j], i)
            return a[0] - b[0], a[1] + b[1]

        h01, h02, h12 = off(0, 1), off(0, 2), off(1, 2)
        values = [d0, d1, h01[0], h01[1], h02[0], h02[1], h12[0], h12[1]]
        return values, loop[0][0][0] + loop[1][0][1] + loop[2][0][2]

    def loop_task(stage, buf, m, n, x):
        index = PAIRS.index((m, n))
        n_ahead = ahead(stage, buf, n, m, x)
        A = []
        for i in range(3):
            A.append(
                total(
                    [mul((buf[m, 0, i, k, x], buf[m, 1, i, k, x]), n_ahead[k]) for k in range(3)]
                )
            )
        m_ahead = ahead(stage, buf, m, n, x)
        columns = [(buf[n, 0, :, l, x], buf[n, 1, :, l, x]) for l in range(3)]
        values, trace = close(A, m_ahead, columns)
        for c in range(8):
            TB[index, c, x] = values[c]
        if stage == 1:
            if 1 in (m, n):
                trace = jnp.where(sub2 == 7, 0.0, trace)
            TR[x] = trace if (m, n) == ORDERS[1][0] else TR[x] + trace
        return values

    def algebra(values):
        d0, d1 = values[0], values[1]
        return (d0, d1, -(d0 + d1), tuple(values[2:4]), tuple(values[4:6]), tuple(values[6:8]))

    def edge_rows(stage, buf):
        for r in range(2):
            for k in range(3):
                for s, m in enumerate(EDGE):
                    for x in range(2):
                        row = slice(2 * s + x, 2 * s + x + 1)
                        EM[r, k, :, row] = buf[m, r, k, :, x, 7:8, :]
                        EN[r, k, :, row] = buf[1, r, k, :, x, 7:8, :]
                for x in range(2):
                    EX[r, k, :, 2 + x : 3 + x] = buf[1, r, k, :, x + 1, 7:8, :]
                    EX[r, k, :, 4 + x : 5 + x] = ZL[stage, 1, r, k, :, 7:8]
        n_ahead = []
        for k in range(3):
            parts = []
            for r in range(2):
                own, other = EN[r, k], EX[r, k]
                t_ahead = choose(t_last, pltpu.roll(own, LT - 1, 2), pltpu.roll(own, 127, 2))
                halo = choose(sub == 4, pltpu.roll(other, half_lanes, 2), other)
                z_ahead = choose(low, pltpu.roll(own, half_lanes, 2), halo)
                parts.append(choose(sub < 2, t_ahead, choose(sub < 4, other, z_ahead)))
            n_ahead.append(tuple(parts))
        for i in range(3):
            value = total([mul((EM[0, i, k], EM[1, i, k]), n_ahead[k]) for k in range(3)])
            EP[0, i], EP[1, i] = value

    def edge_loops(stage):
        for m in EDGE:
            wait_forward(stage, 1, m)
        m_ahead = [(EH[0, k], EH[1, k]) for k in range(3)]
        if stage == 1:
            scale = jnp.where((sub2 < 2) | (sub2 > 3), share(1, 3), share(1, 0))
            m_ahead = cayley([EK[c] + scale * ET[0, 1, c] for c in range(8)], m_ahead)
        A = [(EP[0, i], EP[1, i]) for i in range(3)]
        columns = [(EN[0, :, l], EN[1, :, l]) for l in range(3)]
        values, trace = close(A, m_ahead, columns)
        if stage == 1:
            TR[0] = TR[0] + jnp.where(sub2 < 6, trace, 0.0)
        sign = jnp.where((sub2 < 2) | (sub2 > 3), -1.0, 1.0)
        for c in range(8):
            ET[stage, 0, c] = sign * values[c]

    def edge_staples(stage):
        T = algebra([ET[stage, 0, c] for c in range(8)])
        for slot, buf in ((1, EN), (2, EM)):
            result = conjugate(T, [(buf[0, k], buf[1, k]) for k in range(3)])
            for c in range(8):
                ET[stage, slot, c] = result[c]
        for m in EDGE:
            send_back(stage, 1, m)

    def edge_merge(stage):
        for m in EDGE:
            index = PAIRS.index((min(m, 1), max(m, 1)))
            for x in range(2):
                TB[index, :, x, 7:8] = ET[stage, 0, :, edge_row(m, x)]
                LB[stage, m, 1, :, x + 1, 7:8] = ET[stage, 2, :, edge_row(m, x)]
        for d in (2, 0):
            send_back(stage, d, 1)

    def staple_task(stage, buf, m, n, x, values=None):
        if values is None:
            index = PAIRS.index((m, n))
            values = [TB[index, c, x] for c in range(8)]
        T = algebra(values)
        for link, d in ((m, n), (n, m)):
            rows = [(buf[d, 0, k, :, x], buf[d, 1, k, :, x]) for k in range(3)]
            result = conjugate(T, rows)
            for c in range(8):
                LB[stage, d, link, c, x + 1] = result[c]

    def force(stage, m, x, directions=(0, 1, 2, 3)):
        result = None
        for n in range(4):
            if n == m:
                continue
            index = PAIRS.index((min(m, n), max(m, n)))
            term = TB[index, :, x]
            if n in directions:
                term = term - behind(stage, n, m, x)
            if result is None:
                result = term if m < n else -term
            else:
                result = result + term if m < n else result - term
        return result

    places = ((1, 0, 0), (1, 1, 1), (0, 0, 1), (1, 0, 1), (0, 0, 2), (1, 0, 2), (0, 1, 2), (1, 1, 2))

    def half_update(m, x):
        F = None
        for n in range(4):
            if n == m:
                continue
            term = TB[PAIRS.index((min(m, n), max(m, n))), :, x]
            if n == 0 and x:
                term = term - LB[0, 0, m, :, x]
            elif n != 0:
                value = LB[0, n, m, :, x + 1]
                if n == 1:
                    back = choose(y_first, jnp.zeros_like(value), pltpu.roll(value, 1, 1))
                elif n == 2:
                    back = choose(low, jnp.zeros_like(value), pltpu.roll(value, half_lanes, 2))
                else:
                    back = behind(0, 3, m, x)
                term = term - back
            term = term if m < n else -term
            F = term if F is None else F + term
        for c, (r, i, j) in enumerate(places):
            HB[m, c, x] = MB[m, r, i, j, x] - (0.5 * kick_size) * F[c]

    def cayley(momentum, rows):
        half = [(0.5 * step_size) * value for value in momentum]
        d0, d1 = half[0], half[1]
        d2 = -(d0 + d1)
        h01, h02, h12 = (half[2], half[3]), (half[4], half[5]), (half[6], half[7])
        n01 = h01[0] * h01[0] + h01[1] * h01[1]
        n02 = h02[0] * h02[0] + h02[1] * h02[1]
        n12 = h12[0] * h12[0] + h12[1] * h12[1]
        k00 = d0 * d0 + n01 + n02
        k11 = d1 * d1 + n01 + n12
        k22 = d2 * d2 + n02 + n12
        one_c = 1.0 + 0.5 * (k00 + k11 + k22)
        h01h12 = mul(h01, h12)
        z_imag = h01h12[1] * h02[0] - h01h12[0] * h02[1]
        h = d0 * n12 + d2 * n01 + d1 * n02 - d0 * d1 * d2 - 2.0 * z_imag
        factor = 2.0 / (one_c * one_c + h * h)
        f = (one_c * factor, h * factor)
        s01 = mul_conj_second(h02, h12)
        k01 = (-(d0 + d1) * h01[1] - s01[0], (d0 + d1) * h01[0] - s01[1])
        k02 = (h01h12[0] - (d0 + d2) * h02[1], h01h12[1] + (d0 + d2) * h02[0])
        s12 = mul_conj_first(h01, h02)
        k12 = (-s12[0] - (d1 + d2) * h12[1], (d1 + d2) * h12[0] - s12[1])
        G = [[None] * 3 for _ in range(3)]
        for i, (k, d) in enumerate(((k00, d0), (k11, d1), (k22, d2))):
            G[i][i] = (one_c - k, d)
        for i, j, hh, kk in ((0, 1, h01, k01), (0, 2, h02, k02), (1, 2, h12, k12)):
            G[i][j] = add(hh, kk)
            G[j][i] = (kk[0] - hh[0], hh[1] - kk[1])
        result = []
        for i in range(3):
            E = []
            for k in range(3):
                value = mul(f, G[i][k])
                E.append((value[0] - 1.0, value[1]) if i == k else value)
            result.append(total([mul(E[k], rows[k]) for k in range(3)]))
        return result

    def link_update(m, x):
        rows = [(V[m, 0, k, :, x], V[m, 1, k, :, x]) for k in range(3)]
        new = cayley([HB[m, c, x] for c in range(8)], rows)
        for i in range(3):
            W[m, 0, i, :, x] = new[i][0]
            W[m, 1, i, :, x] = new[i][1]

    def halo_update(d, m):
        if d == 0:
            link_update(m, 2)
            return
        rows = [(ZL[0, m, 0, k], ZL[0, m, 1, k]) for k in range(3)]
        scale = share(2, m)
        new = cayley([ZHR[m, c] + scale * ZBS[0, m, c] for c in range(8)], rows)
        for i in range(3):
            ZL[1, m, 0, i] = new[i][0]
            ZL[1, m, 1, i] = new[i][1]

    def halo_decode(m):
        rows = decode([ZR[m, c] for c in range(CODED)])
        for k in range(3):
            for r in range(2):
                for l in range(3):
                    ZL[0, m, r, k, l] = rows[k][l][r]

    def last_update(m, x):
        F = force(1, m, x)
        v = [HB[m, c, x] - (0.5 * kick_size) * F[c] for c in range(8)]
        zero = jnp.zeros_like(v[0])
        for i in range(3):
            NM[m, 0, i, i, x] = zero
        NM[m, 1, 0, 0, x] = v[0]
        NM[m, 1, 1, 1, x] = v[1]
        NM[m, 1, 2, 2, x] = -(v[0] + v[1])
        for i, j, c in ((0, 1, 2), (0, 2, 4), (1, 2, 6)):
            NM[m, 0, i, j, x] = v[c]
            NM[m, 0, j, i, x] = -v[c]
            NM[m, 1, i, j, x] = v[c + 1]
            NM[m, 1, j, i, x] = v[c + 1]

    def for_x(body):
        for x in range(2):
            body(x)

    def wait_ahead(stage, m, n):
        for link, d in ((n, m), (m, n)):
            if d in (1, 3):
                continue
            wait_forward(stage, d, link)
            if stage == 1:
                halo_update(d, link)
            elif d == 2:
                halo_decode(link)
            elif link in CODED_X:
                rows = decode([XR[link, c] for c in range(CODED)])
                for k in range(3):
                    for r in range(2):
                        for l in range(3):
                            V[link, r, k, l, 2] = rows[k][l][r]

    def send_pair(stage, m, n):
        if 1 in (m, n):
            return
        for link, d in ((m, n), (n, m)):
            send_back(stage, d, link)

    def whole_pair(stage, buf, m, n):
        wait_ahead(stage, m, n)
        for_x(lambda x: staple_task(stage, buf, m, n, x, loop_task(stage, buf, m, n, x)))
        send_pair(stage, m, n)

    def wait_back(stage, m, directions=(0, 1, 2)):
        for d in directions:
            if d != m:
                with jax.named_scope(f"wb{stage}_d{d}m{m}"):
                    wait_rows(backward[stage, d, m], brecv.at[lane_of[stage, d, m]])

    waits = {m: position for position, m in enumerate(LOADS)}
    loads[waits.pop(3)].wait()
    with jax.named_scope("bar"):
        pl.semaphore_wait(barrier, partners)
    send_link(*SENDS[0])
    for d, m in SENDS[1:]:
        if m in waits:
            loads[waits.pop(m)].wait()
        send_link(d, m)
    for m, n in ORDERS[0]:
        whole_pair(0, V, m, n)
        if (m, n) == (1, 2):
            edge_rows(0, V)
            edge_loops(0)
            edge_staples(0)
            edge_merge(0)
    mom_load.wait()
    for m in UPDATES:
        for_x(lambda x: half_update(m, x))

    for m in Z_LINKS:
        add_x(m)
        send_half_z(m)
    for m in UPDATES:
        if m == 2:
            add_x(m)
        add_z(m)
        send_half_y(m)
        add_y(m)
        send_half_x(m)
    for m in UPDATES:
        for_x(lambda x: link_update(m, x))
    for m, n in ORDERS[1][:EARLY]:
        whole_pair(1, W, m, n)
    for m, n in ORDERS[1][EARLY:]:
        wait_ahead(1, m, n)
        for_x(lambda x: loop_task(1, W, m, n, x))
    edge_rows(1, W)
    edge_loops(1)

    def offsets(group):
        result = [()]
        for axis in range(3):
            span = range(sizes[axis]) if axis in group else (0,)
            result = [head + (k,) for head in result for k in span]
        weight = lambda item: sum(min(k, size - k) + (k % 2) for k, size in zip(item, sizes))
        return sorted([item for item in result if any(item)], key=weight, reverse=True)

    def spread(index, value):
        buf = slots[index]
        position = 0
        for axis in groups[index]:
            position = position * sizes[axis] + coords[axis]
        buf[position] = jnp.sum(value, axis=0, keepdims=True)
        for offset in offsets(groups[index]):
            send(buf.at[position], buf.at[position], offset, trecv.at[index])

    def gathered(index):
        wait_rows(slots[index].shape[0] - 1, trecv.at[index])
        value = slots[index][0]
        for k in range(1, slots[index].shape[0]):
            value = value + slots[index][k]
        return value

    def finish(m):
        wait_back(1, m)
        for_x(lambda x: last_update(m, x))

    value = TR[0] + TR[1]
    spread(0, value)
    edge_staples(1)
    for m, n in ORDERS[1][EARLY:]:
        for_x(lambda x: staple_task(1, W, m, n, x))
        send_pair(1, m, n)
    edge_merge(1)
    for position, m in enumerate(UPDATES):
        finish(m)
        if position + 1 < len(groups):
            value = gathered(position)
            spread(position + 1, value)
    with jax.named_scope("plaq"):
        lanes = gathered(len(groups) - 1) * (4.0 / (72.0 * volume))
        plaq_out[...] = jnp.broadcast_to(jnp.sum(lanes, axis=1, keepdims=True), (8, 128))
    wait_rows(sum(pending), send_sem.at[0])


def store_kernel(links, mom, plaq, links_out, mom_out, plaq_out, sem):
    copies = [
        pltpu.make_async_copy(links.at[:, :, :, :, 0:2], links_out, sem.at[0]),
        pltpu.make_async_copy(mom, mom_out, sem.at[1]),
        pltpu.make_async_copy(plaq.at[0:1], plaq_out, sem.at[2]),
    ]
    for copy in copies:
        copy.start()
    for copy in copies:
        copy.wait()


def per_device(gauge_links, momenta):
    block = gauge_links.shape
    assert block[-3:] == (2, 8, 2 * LT)
    sizes = tuple(lax.axis_size(axis) for axis in AXES)
    sites = block[-3] * block[-2] * block[-1]
    volume = sites * sizes[0] * sizes[1] * sizes[2]
    f32 = jnp.float32
    vm = lambda *shape: pltpu.VMEM(shape, f32)
    groups = ((0, 1, 2),) if sizes[0] * sizes[1] * sizes[2] <= 32 else ((0,), (1,), (2,))
    counts = []
    for group in groups:
        count = 1
        for axis in group:
            count *= sizes[axis]
        counts.append(count)
    dma = pltpu.SemaphoreType.DMA
    wide_links, momenta_vmem, plaquette = pl.pallas_call(
        functools.partial(kernel, sizes, volume, groups),
        out_shape=(
            vm(4, 2, 3, 3, 3, 8, 128),
            vm(*block),
            vm(8, 128),
        ),
        in_specs=[pl.BlockSpec(memory_space=pl.ANY)] * 2,
        out_specs=(
            pl.BlockSpec(memory_space=pltpu.VMEM),
            pl.BlockSpec(memory_space=pltpu.VMEM),
            pl.BlockSpec(memory_space=pltpu.VMEM),
        ),
        scratch_shapes=[
            vm(4, 2, 3, 3, 3, 8, 128),
            vm(*block),
            vm(4, 8, 3, 8, 128),
            vm(6, 8, 2, 8, 128),
            vm(2, 4, 4, 8, 3, 8, 128),
            vm(4, CODED, 8, 128),
            vm(4, CODED, 8, 128),
            vm(2, 3, 3, 8, 128),
            vm(2, 3, 3, 8, 128),
            vm(4, 8, 2, 1, 128),
            vm(2, 3, 3, 8, 128),
            vm(2, 3, 3, 8, 128),
            vm(2, 3, 3, 8, 128),
            vm(8, 8, 128),
            vm(2, 3, 8, 8, 128),
            vm(4, CODED, 8, 128),
            vm(4, CODED, 8, 128),
            vm(4, 8, 8, 128),
            vm(4, 8, 8, 128),
            vm(2, 4, 2, 3, 3, 8, 128),
            vm(2, 4, 8, 2, 1, 128),
            vm(2, 4, 8, 8, 128),
            vm(2, 4, 8, 8, 128),
            vm(2, 8, 128),
            dma((5,)),
            dma((1,)),
            dma((LANES,)),
            dma((LANES,)),
            dma((len(groups),)),
            vm(8192, 1, 128),
            *[vm(count, 1, 128) for count in counts],
        ],
        compiler_params=pltpu.CompilerParams(collective_id=0, has_side_effects=True),
        name="md_step",
    )(gauge_links, momenta)
    anywhere = pl.BlockSpec(memory_space=pl.ANY)
    in_vmem = pl.BlockSpec(memory_space=pltpu.VMEM)
    new_links, new_momenta, plaquette = pl.pallas_call(
        store_kernel,
        out_shape=(
            jax.ShapeDtypeStruct(block, f32),
            jax.ShapeDtypeStruct(block, f32),
            jax.ShapeDtypeStruct((1, 128), f32),
        ),
        in_specs=[in_vmem] * 3,
        out_specs=(anywhere,) * 3,
        scratch_shapes=[dma((3,))],
        name="store",
    )(
        pltpu.with_memory_space_constraint(wide_links, pltpu.VMEM),
        pltpu.with_memory_space_constraint(momenta_vmem, pltpu.VMEM),
        pltpu.with_memory_space_constraint(plaquette, pltpu.VMEM),
    )
    return new_links, new_momenta, plaquette[0, 0]


def solution(mesh):
    spec = P(None, None, None, None, "gx", "gy", "zt")
    return jax.shard_map(
        per_device,
        mesh=mesh,
        in_specs=(spec, spec),
        out_specs=(spec, spec, P()),
        check_vma=False,
    )
```

```python
import functools

import jax
import jax.numpy as jnp
from jax import lax
from jax.experimental import pallas as pl
from jax.experimental.pallas import tpu as pltpu
from jax.sharding import PartitionSpec as P

LT = 64
AXES = ("gx", "gy", "zt")
PAIRS = ((1, 3), (0, 3), (0, 1), (2, 3), (0, 2), (1, 2))
ORDERS = (
    ((1, 3), (0, 3), (0, 1), (2, 3), (1, 2), (0, 2)),
    ((1, 3), (2, 3), (0, 3), (0, 2), (0, 1), (1, 2)),
)
EARLY = 3
EDGE = (3, 0, 2)
LOADS = (3, 1, 0, 2)
Z_LINKS = (3, 1, 0)
SENDS = ((0, 3), (1, 3), (2, 3), (1, 0), (1, 2), (2, 1), (0, 1), (2, 0), (0, 2))
UPDATES = (3, 2, 0, 1)
MESH_ID = pl.DeviceIdType.MESH

kick_size = 0.25
step_size = 0.2


def mul(a, b):
    return a[0] * b[0] - a[1] * b[1], a[0] * b[1] + a[1] * b[0]


def mul_conj_second(a, b):
    return a[0] * b[0] + a[1] * b[1], a[1] * b[0] - a[0] * b[1]


def mul_conj_first(a, b):
    return a[0] * b[0] + a[1] * b[1], a[0] * b[1] - a[1] * b[0]


def add(a, b):
    return a[0] + b[0], a[1] + b[1]


def total(terms):
    result = terms[0]
    for term in terms[1:]:
        result = add(result, term)
    return result


def conj(a):
    return a[0], -a[1]


def pick(a, index):
    return a[0][index], a[1][index]


TINY = 1e-30
FAR = 1e15
CODED = 11
LANES = 15
CODED_X = (1, 2)


def project(first, rest):
    square = rest[0] * rest[0]
    for value in rest[1:]:
        square = square + value * value
    near = first >= 0.0
    low = jnp.where(near, 1.0 + first, square)
    factor = jnp.where(near, 1.0, 1.0 - first) / jnp.maximum(low, TINY)
    result = [value * factor for value in rest]
    result[0] = jnp.where(low < TINY, FAR, result[0])
    return result


def lift(values):
    square = values[0] * values[0]
    for value in values[1:]:
        square = square + value * value
    inverse = 1.0 / (1.0 + square)
    double = 2.0 * inverse
    return [(1.0 - square) * inverse] + [value * double for value in values]


def cross(a, b):
    result = []
    for i in range(3):
        j, k = (i + 1) % 3, (i + 2) % 3
        p, q = mul(a[j], b[k]), mul(a[k], b[j])
        result.append((p[0] - q[0], p[1] - q[1]))
    return result


def encode(rows):
    rows = [[pick(row, l) for l in range(3)] for row in rows]
    normal = cross(rows[0], rows[1])
    det = total([mul(rows[2][l], normal[l]) for l in range(3)])
    values = []
    for row in rows[:2]:
        flat = [part for entry in row for part in entry]
        values += project(flat[0], flat[1:])
    return values + project(det[0], [det[1]])


def decode(values):
    rows = []
    for start in (0, 5):
        flat = lift(values[start : start + 5])
        rows.append([(flat[2 * l], flat[2 * l + 1]) for l in range(3)])
    det = lift(values[10:])
    rows.append([mul_conj_second(det, entry) for entry in cross(rows[0], rows[1])])
    return rows


def kernel(
    sizes,
    volume,
    groups,
    links_in,
    mom_in,
    W,
    NM,
    plaq_out,
    V,
    MB,
    HB,
    TB,
    LB,
    XS,
    XR,
    EM,
    EN,
    YHS,
    EX,
    EP,
    EH,
    EK,
    ET,
    ZS,
    ZR,
    ZHS,
    ZHR,
    ZL,
    YBR,
    ZBS,
    ZBR,
    TR,
    load_sem,
    send_sem,
    frecv,
    brecv,
    trecv,
    lines,
    *slots,
):
    coords = [lax.axis_index(axis) for axis in AXES]

    def device(offset):
        return tuple(
            lax.rem(coords[axis] + (offset[axis] % sizes[axis]), sizes[axis]) for axis in range(3)
        )

    def along(axis, distance):
        return tuple(distance if other == axis else 0 for other in range(3))

    loads = []
    for m in LOADS:
        copy = pltpu.make_async_copy(links_in.at[m], V.at[m, :, :, :, 0:2], load_sem.at[m])
        copy.start()
        loads.append(copy)
    mom_load = pltpu.make_async_copy(mom_in, MB, load_sem.at[4])
    mom_load.start()

    barrier = pltpu.get_barrier_semaphore()
    partners = 0
    for axis in range(3):
        for k in range(1, sizes[axis]):
            pl.semaphore_signal(barrier, inc=1, device_id=device(along(axis, k)), device_id_type=MESH_ID)
            partners += 1

    shape3 = (1, 8, 128)
    lane = lax.broadcasted_iota(jnp.int32, shape3, 2)
    sub = lax.broadcasted_iota(jnp.int32, shape3, 1)
    sub2 = lax.broadcasted_iota(jnp.int32, shape3[1:], 0)
    t_index = lax.rem(lane, LT)
    half_lanes = lane.shape[-1] // 2
    low = lane < half_lanes
    low_row = lax.broadcasted_iota(jnp.int32, (1, 1, 128), 2) < half_lanes
    t_last = t_index == LT - 1
    t_first = t_index == 0
    y_first = sub == 0

    def choose(mask, a, b):
        return jnp.where(jnp.broadcast_to(mask, b.shape), jnp.broadcast_to(a, b.shape), b)

    pending = []

    def send(src, dst, offset, recv_sem):
        copy = pltpu.make_async_remote_copy(
            src_ref=src,
            dst_ref=dst,
            send_sem=send_sem.at[0],
            recv_sem=recv_sem,
            device_id=device(offset),
            device_id_type=MESH_ID,
        )
        copy.start()
        pending.append(rows_of(src))
        return copy

    def rows_of(ref):
        size = 1
        for extent in ref.shape:
            size *= extent
        return size // 128

    def wait_rows(count, sem):
        part = lines.at[0:count]
        pltpu.make_async_copy(part, part, sem).wait()

    lane_of = {}
    for d in range(3):
        for m in range(4):
            if d != m:
                lane_of[0, d, m] = len(set(lane_of.values()))
                lane_of[1, d, m] = lane_of[0, d, m] + (d > 0)
    forward = {}
    backward = {}

    def forward_send(stage, d, m, src, dst):
        send(src, dst, along(d, -1), frecv.at[lane_of[stage, d, m]])
        forward[stage, d, m] = forward.get((stage, d, m), 0) + rows_of(src)

    def wait_forward(stage, d, m):
        with jax.named_scope(f"wf{stage}_d{d}m{m}"):
            wait_rows(forward[stage, d, m], frecv.at[lane_of[stage, d, m]])

    def edge_row(m, x):
        row = 2 * EDGE.index(m) + x
        return slice(row, row + 1)

    def store_code(buf, m, rows):
        for c, value in enumerate(encode(rows)):
            buf[m, c] = value

    def pack_z(m):
        rows = []
        for i in range(3):
            parts = []
            for r in range(2):
                first = V[m, r, i, :, 0]
                second = V[m, r, i, :, 1]
                parts.append(choose(low, first, pltpu.roll(second, half_lanes, 2)))
            rows.append(tuple(parts))
        store_code(ZS, m, rows)

    def send_link(d, m):
        if d == 1:
            for x in range(2):
                forward_send(0, 1, m, V.at[m, :, :, :, x, 0:1], EH.at[:, :, :, edge_row(m, x)])
        elif d == 2:
            pack_z(m)
            forward_send(0, 2, m, ZS.at[m], ZR.at[m])
        elif m in CODED_X:
            store_code(XS, m, [(V[m, 0, k, :, 0], V[m, 1, k, :, 0]) for k in range(3)])
            forward_send(0, 0, m, XS.at[m], XR.at[m])
        else:
            forward_send(0, 0, m, V.at[m, :, :, :, 0], V.at[m, :, :, :, 2])

    def share(d, m):
        return (0.5 * kick_size) if m < d else (-0.5 * kick_size)

    def add_x(m):
        if m != 0:
            wait_back(0, m, (0,))
            HB[m, :, 0] = HB[m, :, 0] + share(0, m) * LB[0, 0, m, :, 0]

    def add_y(m):
        if m != 1:
            if m == 2:
                wait_back(0, m, (1,))
            for x in range(2):
                HB[m, :, x, 0:1] = HB[m, :, x, 0:1] + share(1, m) * YBR[0, m, :, x]

    def add_z(m):
        if m == 2:
            return
        wait_back(0, m, (2,))
        for x in range(2):
            halo = pltpu.roll(ZBR[0, m], half_lanes * x, 2) if x else ZBR[0, m]
            HB[m, :, x] = HB[m, :, x] + choose(low, share(2, m) * halo, jnp.zeros_like(halo))

    def send_half_z(m):
        ZHS[m] = choose(low, HB[m, :, 0], pltpu.roll(HB[m, :, 1], half_lanes, 2))
        if m != 1:
            wait_back(0, m, (1,))
            first, second = YBR[0, m, :, 0], YBR[0, m, :, 1]
            row = choose(low_row, first, pltpu.roll(second, half_lanes, 2))
            ZHS[m, :, 0:1] = ZHS[m, :, 0:1] + share(1, m) * row
        forward_send(1, 2, m, ZHS.at[m], ZHR.at[m])

    def send_half_y(m):
        if m != 1:
            for x in range(2):
                YHS[m, :, x] = HB[m, :, x, 0:1]
                forward_send(1, 1, m, YHS.at[m, :, x], EK.at[:, edge_row(m, x)])

    def send_half_x(m):
        if m != 0:
            forward_send(1, 0, m, HB.at[m, :, 0], HB.at[m, :, 2])

    def send_back(stage, d, m):
        if d == 3:
            return
        if d == 0:
            copies = [(LB.at[stage, 0, m, :, 2], LB.at[stage, 0, m, :, 0])]
        elif d == 1:
            copies = [(ET.at[stage, 1, :, edge_row(m, x)], YBR.at[stage, m, :, x]) for x in range(2)]
        else:
            first = LB[stage, 2, m, :, 1]
            second = LB[stage, 2, m, :, 2]
            ZBS[stage, m] = choose(low, pltpu.roll(first, half_lanes, 2), second)
            copies = [(ZBS.at[stage, m], ZBR.at[stage, m])]
        for src, dst in copies:
            send(src, dst, along(d, 1), brecv.at[lane_of[stage, d, m]])
            backward[stage, d, m] = backward.get((stage, d, m), 0) + rows_of(src)

    def ahead(stage, buf, n, d, x):
        rows = []
        for k in range(3):
            parts = []
            for r in range(2):
                if d == 0:
                    parts.append(buf[n, r, k, :, x + 1])
                    continue
                value = buf[n, r, k, :, x]
                if d == 3:
                    parts.append(
                        choose(t_last, pltpu.roll(value, LT - 1, 2), pltpu.roll(value, 127, 2))
                    )
                elif d == 1:
                    parts.append(pltpu.roll(value, 7, 1))
                else:
                    halo = pltpu.roll(ZL[stage, n, r, k], half_lanes * (1 - x), 2)
                    parts.append(choose(low, pltpu.roll(value, half_lanes, 2), halo))
            rows.append(tuple(parts))
        return rows

    def behind(stage, d, m, x):
        if d == 0:
            return LB[stage, 0, m, :, x]
        value = LB[stage, d, m, :, x + 1]
        if d == 1:
            return choose(y_first, YBR[stage, m, :, x], pltpu.roll(value, 1, 1))
        if d == 2:
            halo = pltpu.roll(ZBR[stage, m], half_lanes * x, 2)
            return choose(low, halo, pltpu.roll(value, half_lanes, 2))
        return choose(t_first, pltpu.roll(value, 128 - (LT - 1), 2), pltpu.roll(value, 1, 2))

    def conjugate(T, rows):
        d0, d1, d2, h01, h02, h12 = T
        full = [
            [d0, h01, h02],
            [(-h01[0], h01[1]), d1, h12],
            [(-h02[0], h02[1]), (-h12[0], h12[1]), d2],
        ]
        M = []
        for i in range(3):
            terms = []
            for k in range(3):
                if i == k:
                    terms.append((-(full[i][i] * rows[k][1]), full[i][i] * rows[k][0]))
                else:
                    terms.append(mul(full[i][k], rows[k]))
            M.append(total(terms))
        r0 = 0.0
        r1 = 0.0
        for k in range(3):
            r0 = r0 + (rows[k][0][0] * M[k][1][0] - rows[k][1][0] * M[k][0][0])
            r1 = r1 + (rows[k][0][1] * M[k][1][1] - rows[k][1][1] * M[k][0][1])
        tail = slice(1, 3)
        row0 = total(
            [mul_conj_first(pick(rows[k], 0), (M[k][0][tail], M[k][1][tail])) for k in range(3)]
        )
        r12 = total([mul_conj_first(pick(rows[k], 1), pick(M[k], 2)) for k in range(3)])
        return [r0, r1, row0[0][0], row0[1][0], row0[0][1], row0[1][1], r12[0], r12[1]]

    def close(A, m_ahead, columns):
        Bt = []
        for k in range(3):
            Bt.append(total([mul(pick(m_ahead[l], k), columns[l]) for l in range(3)]))
        loop = []
        for i in range(3):
            loop.append(total([mul_conj_second(pick(A[i], k), Bt[k]) for k in range(3)]))
        i0, i1, i2 = loop[0][1][0], loop[1][1][1], loop[2][1][2]
        mean = (i0 + i1 + i2) * (2.0 / 3.0)
        d0 = 2.0 * i0 - mean
        d1 = 2.0 * i1 - mean

        def off(i, j):
            a = pick(loop[i], j)
            b = pick(loop[j], i)
            return a[0] - b[0], a[1] + b[1]

        h01, h02, h12 = off(0, 1), off(0, 2), off(1, 2)
        values = [d0, d1, h01[0], h01[1], h02[0], h02[1], h12[0], h12[1]]
        return values, loop[0][0][0] + loop[1][0][1] + loop[2][0][2]

    def loop_task(stage, buf, m, n, x):
        index = PAIRS.index((m, n))
        n_ahead = ahead(stage, buf, n, m, x)
        A = []
        for i in range(3):
            A.append(
                total(
                    [mul((buf[m, 0, i, k, x], buf[m, 1, i, k, x]), n_ahead[k]) for k in range(3)]
                )
            )
        m_ahead = ahead(stage, buf, m, n, x)
        columns = [(buf[n, 0, :, l, x], buf[n, 1, :, l, x]) for l in range(3)]
        values, trace = close(A, m_ahead, columns)
        for c in range(8):
            TB[index, c, x] = values[c]
        if stage == 1:
            if 1 in (m, n):
                trace = jnp.where(sub2 == 7, 0.0, trace)
            TR[x] = trace if (m, n) == ORDERS[1][0] else TR[x] + trace
        return values

    def algebra(values):
        d0, d1 = values[0], values[1]
        return (d0, d1, -(d0 + d1), tuple(values[2:4]), tuple(values[4:6]), tuple(values[6:8]))

    def edge_rows(stage, buf):
        for r in range(2):
            for k in range(3):
                for s, m in enumerate(EDGE):
                    for x in range(2):
                        row = slice(2 * s + x, 2 * s + x + 1)
                        EM[r, k, :, row] = buf[m, r, k, :, x, 7:8, :]
                        EN[r, k, :, row] = buf[1, r, k, :, x, 7:8, :]
                for x in range(2):
                    EX[r, k, :, 2 + x : 3 + x] = buf[1, r, k, :, x + 1, 7:8, :]
                    EX[r, k, :, 4 + x : 5 + x] = ZL[stage, 1, r, k, :, 7:8]
        n_ahead = []
        for k in range(3):
            parts = []
            for r in range(2):
                own, other = EN[r, k], EX[r, k]
                t_ahead = choose(t_last, pltpu.roll(own, LT - 1, 2), pltpu.roll(own, 127, 2))
                halo = choose(sub == 4, pltpu.roll(other, half_lanes, 2), other)
                z_ahead = choose(low, pltpu.roll(own, half_lanes, 2), halo)
                parts.append(choose(sub < 2, t_ahead, choose(sub < 4, other, z_ahead)))
            n_ahead.append(tuple(parts))
        for i in range(3):
            value = total([mul((EM[0, i, k], EM[1, i, k]), n_ahead[k]) for k in range(3)])
            EP[0, i], EP[1, i] = value

    def edge_loops(stage):
        for m in EDGE:
            wait_forward(stage, 1, m)
        m_ahead = [(EH[0, k], EH[1, k]) for k in range(3)]
        if stage == 1:
            scale = jnp.where((sub2 < 2) | (sub2 > 3), share(1, 3), share(1, 0))
            m_ahead = cayley([EK[c] + scale * ET[0, 1, c] for c in range(8)], m_ahead)
        A = [(EP[0, i], EP[1, i]) for i in range(3)]
        columns = [(EN[0, :, l], EN[1, :, l]) for l in range(3)]
        values, trace = close(A, m_ahead, columns)
        if stage == 1:
            TR[0] = TR[0] + jnp.where(sub2 < 6, trace, 0.0)
        sign = jnp.where((sub2 < 2) | (sub2 > 3), -1.0, 1.0)
        for c in range(8):
            ET[stage, 0, c] = sign * values[c]

    def edge_staples(stage):
        T = algebra([ET[stage, 0, c] for c in range(8)])
        for slot, buf in ((1, EN), (2, EM)):
            result = conjugate(T, [(buf[0, k], buf[1, k]) for k in range(3)])
            for c in range(8):
                ET[stage, slot, c] = result[c]
        for m in EDGE:
            send_back(stage, 1, m)

    def edge_merge(stage):
        for m in EDGE:
            index = PAIRS.index((min(m, 1), max(m, 1)))
            for x in range(2):
                TB[index, :, x, 7:8] = ET[stage, 0, :, edge_row(m, x)]
                LB[stage, m, 1, :, x + 1, 7:8] = ET[stage, 2, :, edge_row(m, x)]
        for d in (2, 0):
            send_back(stage, d, 1)

    def staple_task(stage, buf, m, n, x, values=None):
        if values is None:
            index = PAIRS.index((m, n))
            values = [TB[index, c, x] for c in range(8)]
        T = algebra(values)
        for link, d in ((m, n), (n, m)):
            rows = [(buf[d, 0, k, :, x], buf[d, 1, k, :, x]) for k in range(3)]
            result = conjugate(T, rows)
            for c in range(8):
                LB[stage, d, link, c, x + 1] = result[c]

    def force(stage, m, x, directions=(0, 1, 2, 3)):
        result = None
        for n in range(4):
            if n == m:
                continue
            index = PAIRS.index((min(m, n), max(m, n)))
            term = TB[index, :, x]
            if n in directions:
                term = term - behind(stage, n, m, x)
            if result is None:
                result = term if m < n else -term
            else:
                result = result + term if m < n else result - term
        return result

    places = ((1, 0, 0), (1, 1, 1), (0, 0, 1), (1, 0, 1), (0, 0, 2), (1, 0, 2), (0, 1, 2), (1, 1, 2))

    def half_update(m, x):
        F = None
        for n in range(4):
            if n == m:
                continue
            term = TB[PAIRS.index((min(m, n), max(m, n))), :, x]
            if n == 0 and x:
                term = term - LB[0, 0, m, :, x]
            elif n != 0:
                value = LB[0, n, m, :, x + 1]
                if n == 1:
                    back = choose(y_first, jnp.zeros_like(value), pltpu.roll(value, 1, 1))
                elif n == 2:
                    back = choose(low, jnp.zeros_like(value), pltpu.roll(value, half_lanes, 2))
                else:
                    back = behind(0, 3, m, x)
                term = term - back
            term = term if m < n else -term
            F = term if F is None else F + term
        for c, (r, i, j) in enumerate(places):
            HB[m, c, x] = MB[m, r, i, j, x] - (0.5 * kick_size) * F[c]

    def cayley(momentum, rows):
        half = [(0.5 * step_size) * value for value in momentum]
        d0, d1 = half[0], half[1]
        d2 = -(d0 + d1)
        h01, h02, h12 = (half[2], half[3]), (half[4], half[5]), (half[6], half[7])
        n01 = h01[0] * h01[0] + h01[1] * h01[1]
        n02 = h02[0] * h02[0] + h02[1] * h02[1]
        n12 = h12[0] * h12[0] + h12[1] * h12[1]
        k00 = d0 * d0 + n01 + n02
        k11 = d1 * d1 + n01 + n12
        k22 = d2 * d2 + n02 + n12
        one_c = 1.0 + 0.5 * (k00 + k11 + k22)
        h01h12 = mul(h01, h12)
        z_imag = h01h12[1] * h02[0] - h01h12[0] * h02[1]
        h = d0 * n12 + d2 * n01 + d1 * n02 - d0 * d1 * d2 - 2.0 * z_imag
        factor = 2.0 / (one_c * one_c + h * h)
        f = (one_c * factor, h * factor)
        s01 = mul_conj_second(h02, h12)
        k01 = (-(d0 + d1) * h01[1] - s01[0], (d0 + d1) * h01[0] - s01[1])
        k02 = (h01h12[0] - (d0 + d2) * h02[1], h01h12[1] + (d0 + d2) * h02[0])
        s12 = mul_conj_first(h01, h02)
        k12 = (-s12[0] - (d1 + d2) * h12[1], (d1 + d2) * h12[0] - s12[1])
        G = [[None] * 3 for _ in range(3)]
        for i, (k, d) in enumerate(((k00, d0), (k11, d1), (k22, d2))):
            G[i][i] = (one_c - k, d)
        for i, j, hh, kk in ((0, 1, h01, k01), (0, 2, h02, k02), (1, 2, h12, k12)):
            G[i][j] = add(hh, kk)
            G[j][i] = (kk[0] - hh[0], hh[1] - kk[1])
        result = []
        for i in range(3):
            E = []
            for k in range(3):
                value = mul(f, G[i][k])
                E.append((value[0] - 1.0, value[1]) if i == k else value)
            result.append(total([mul(E[k], rows[k]) for k in range(3)]))
        return result

    def link_update(m, x):
        rows = [(V[m, 0, k, :, x], V[m, 1, k, :, x]) for k in range(3)]
        new = cayley([HB[m, c, x] for c in range(8)], rows)
        for i in range(3):
            W[m, 0, i, :, x] = new[i][0]
            W[m, 1, i, :, x] = new[i][1]

    def halo_update(d, m):
        if d == 0:
            link_update(m, 2)
            return
        rows = [(ZL[0, m, 0, k], ZL[0, m, 1, k]) for k in range(3)]
        scale = share(2, m)
        new = cayley([ZHR[m, c] + scale * ZBS[0, m, c] for c in range(8)], rows)
        for i in range(3):
            ZL[1, m, 0, i] = new[i][0]
            ZL[1, m, 1, i] = new[i][1]

    def halo_decode(m):
        rows = decode([ZR[m, c] for c in range(CODED)])
        for k in range(3):
            for r in range(2):
                for l in range(3):
                    ZL[0, m, r, k, l] = rows[k][l][r]

    def last_update(m, x):
        F = force(1, m, x)
        v = [HB[m, c, x] - (0.5 * kick_size) * F[c] for c in range(8)]
        zero = jnp.zeros_like(v[0])
        for i in range(3):
            NM[m, 0, i, i, x] = zero
        NM[m, 1, 0, 0, x] = v[0]
        NM[m, 1, 1, 1, x] = v[1]
        NM[m, 1, 2, 2, x] = -(v[0] + v[1])
        for i, j, c in ((0, 1, 2), (0, 2, 4), (1, 2, 6)):
            NM[m, 0, i, j, x] = v[c]
            NM[m, 0, j, i, x] = -v[c]
            NM[m, 1, i, j, x] = v[c + 1]
            NM[m, 1, j, i, x] = v[c + 1]

    def for_x(body):
        for x in range(2):
            body(x)

    def wait_ahead(stage, m, n):
        for link, d in ((n, m), (m, n)):
            if d in (1, 3):
                continue
            wait_forward(stage, d, link)
            if stage == 1:
                halo_update(d, link)
            elif d == 2:
                halo_decode(link)
            elif link in CODED_X:
                rows = decode([XR[link, c] for c in range(CODED)])
                for k in range(3):
                    for r in range(2):
                        for l in range(3):
                            V[link, r, k, l, 2] = rows[k][l][r]

    def send_pair(stage, m, n):
        if 1 in (m, n):
            return
        for link, d in ((m, n), (n, m)):
            send_back(stage, d, link)

    def whole_pair(stage, buf, m, n):
        wait_ahead(stage, m, n)
        for_x(lambda x: staple_task(stage, buf, m, n, x, loop_task(stage, buf, m, n, x)))
        send_pair(stage, m, n)

    def wait_back(stage, m, directions=(0, 1, 2)):
        for d in directions:
            if d != m:
                with jax.named_scope(f"wb{stage}_d{d}m{m}"):
                    wait_rows(backward[stage, d, m], brecv.at[lane_of[stage, d, m]])

    waits = {m: position for position, m in enumerate(LOADS)}
    loads[waits.pop(3)].wait()
    with jax.named_scope("bar"):
        pl.semaphore_wait(barrier, partners)
    send_link(*SENDS[0])
    for d, m in SENDS[1:]:
        if m in waits:
            loads[waits.pop(m)].wait()
        send_link(d, m)
    for m, n in ORDERS[0]:
        whole_pair(0, V, m, n)
        if (m, n) == (1, 2):
            edge_rows(0, V)
            edge_loops(0)
            edge_staples(0)
            edge_merge(0)
    mom_load.wait()
    for m in UPDATES:
        for_x(lambda x: half_update(m, x))

    for m in Z_LINKS:
        add_x(m)
        send_half_z(m)
    for m in UPDATES:
        if m == 2:
            add_x(m)
        add_z(m)
        send_half_y(m)
        add_y(m)
        send_half_x(m)
    for m in UPDATES:
        for_x(lambda x: link_update(m, x))
    for m, n in ORDERS[1][:EARLY]:
        whole_pair(1, W, m, n)
    for m, n in ORDERS[1][EARLY:]:
        wait_ahead(1, m, n)
        for_x(lambda x: loop_task(1, W, m, n, x))
    edge_rows(1, W)
    edge_loops(1)

    def offsets(group):
        result = [()]
        for axis in range(3):
            span = range(sizes[axis]) if axis in group else (0,)
            result = [head + (k,) for head in result for k in span]
        weight = lambda item: sum(min(k, size - k) + (k % 2) for k, size in zip(item, sizes))
        return sorted([item for item in result if any(item)], key=weight, reverse=True)

    def spread(index, value):
        buf = slots[index]
        position = 0
        for axis in groups[index]:
            position = position * sizes[axis] + coords[axis]
        buf[position] = jnp.sum(value, axis=0, keepdims=True)
        for offset in offsets(groups[index]):
            send(buf.at[position], buf.at[position], offset, trecv.at[index])

    def gathered(index):
        wait_rows(slots[index].shape[0] - 1, trecv.at[index])
        value = slots[index][0]
        for k in range(1, slots[index].shape[0]):
            value = value + slots[index][k]
        return value

    def finish(m):
        wait_back(1, m)
        for_x(lambda x: last_update(m, x))

    value = TR[0] + TR[1]
    spread(0, value)
    edge_staples(1)
    for m, n in ORDERS[1][EARLY:]:
        for_x(lambda x: staple_task(1, W, m, n, x))
        send_pair(1, m, n)
    edge_merge(1)
    for position, m in enumerate(UPDATES):
        finish(m)
        if position + 1 < len(groups):
            value = gathered(position)
            spread(position + 1, value)
    with jax.named_scope("plaq"):
        lanes = gathered(len(groups) - 1) * (4.0 / (72.0 * volume))
        plaq_out[...] = jnp.broadcast_to(jnp.sum(lanes, axis=1, keepdims=True), (8, 128))
    wait_rows(sum(pending), send_sem.at[0])


def store_kernel(links, mom, plaq, links_out, mom_out, plaq_out, sem):
    copies = [
        pltpu.make_async_copy(links.at[:, :, :, :, 0:2], links_out, sem.at[0]),
        pltpu.make_async_copy(mom, mom_out, sem.at[1]),
        pltpu.make_async_copy(plaq.at[0:1], plaq_out, sem.at[2]),
    ]
    for copy in copies:
        copy.start()
    for copy in copies:
        copy.wait()


def per_device(gauge_links, momenta):
    block = gauge_links.shape
    assert block[-3:] == (2, 8, 2 * LT)
    sizes = tuple(lax.axis_size(axis) for axis in AXES)
    sites = block[-3] * block[-2] * block[-1]
    volume = sites * sizes[0] * sizes[1] * sizes[2]
    f32 = jnp.float32
    vm = lambda *shape: pltpu.VMEM(shape, f32)
    groups = ((0, 1, 2),) if sizes[0] * sizes[1] * sizes[2] <= 32 else ((0,), (1,), (2,))
    counts = []
    for group in groups:
        count = 1
        for axis in group:
            count *= sizes[axis]
        counts.append(count)
    dma = pltpu.SemaphoreType.DMA
    wide_links, momenta_vmem, plaquette = pl.pallas_call(
        functools.partial(kernel, sizes, volume, groups),
        out_shape=(
            vm(4, 2, 3, 3, 3, 8, 128),
            vm(*block),
            vm(8, 128),
        ),
        in_specs=[pl.BlockSpec(memory_space=pl.ANY)] * 2,
        out_specs=(
            pl.BlockSpec(memory_space=pltpu.VMEM),
            pl.BlockSpec(memory_space=pltpu.VMEM),
            pl.BlockSpec(memory_space=pltpu.VMEM),
        ),
        scratch_shapes=[
            vm(4, 2, 3, 3, 3, 8, 128),
            vm(*block),
            vm(4, 8, 3, 8, 128),
            vm(6, 8, 2, 8, 128),
            vm(2, 4, 4, 8, 3, 8, 128),
            vm(4, CODED, 8, 128),
            vm(4, CODED, 8, 128),
            vm(2, 3, 3, 8, 128),
            vm(2, 3, 3, 8, 128),
            vm(4, 8, 2, 1, 128),
            vm(2, 3, 3, 8, 128),
            vm(2, 3, 3, 8, 128),
            vm(2, 3, 3, 8, 128),
            vm(8, 8, 128),
            vm(2, 3, 8, 8, 128),
            vm(4, CODED, 8, 128),
            vm(4, CODED, 8, 128),
            vm(4, 8, 8, 128),
            vm(4, 8, 8, 128),
            vm(2, 4, 2, 3, 3, 8, 128),
            vm(2, 4, 8, 2, 1, 128),
            vm(2, 4, 8, 8, 128),
            vm(2, 4, 8, 8, 128),
            vm(2, 8, 128),
            dma((5,)),
            dma((1,)),
            dma((LANES,)),
            dma((LANES,)),
            dma((len(groups),)),
            vm(8192, 1, 128),
            *[vm(count, 1, 128) for count in counts],
        ],
        compiler_params=pltpu.CompilerParams(collective_id=0, has_side_effects=True),
        name="md_step",
    )(gauge_links, momenta)
    anywhere = pl.BlockSpec(memory_space=pl.ANY)
    in_vmem = pl.BlockSpec(memory_space=pltpu.VMEM)
    new_links, new_momenta, plaquette = pl.pallas_call(
        store_kernel,
        out_shape=(
            jax.ShapeDtypeStruct(block, f32),
            jax.ShapeDtypeStruct(block, f32),
            jax.ShapeDtypeStruct((1, 128), f32),
        ),
        in_specs=[in_vmem] * 3,
        out_specs=(anywhere,) * 3,
        scratch_shapes=[dma((3,))],
        name="store",
    )(
        pltpu.with_memory_space_constraint(wide_links, pltpu.VMEM),
        pltpu.with_memory_space_constraint(momenta_vmem, pltpu.VMEM),
        pltpu.with_memory_space_constraint(plaquette, pltpu.VMEM),
    )
    return new_links, new_momenta, plaquette[0, 0]


def solution(mesh):
    spec = P(None, None, None, None, "gx", "gy", "zt")
    return jax.shard_map(
        per_device,
        mesh=mesh,
        in_specs=(spec, spec),
        out_specs=(spec, spec, P()),
        check_vma=False,
    )
```
